32 devices in a mesh: row: 8 (over z, core), col: 4 (over y, x).
Axes of the slice: x: 2, y: 2, z: 4, core: 2. Of those that a mesh axis runs over, the one named last changes fastest.
Arguments:
- factor: bfloat16 [8192, 8192], P('row', 'col'), as said below
- sel_tiles: int32 [32], replicated, may hold values from 0 to 63, as said below
- coupling: bfloat16 [8192, 2048], P('col', 'row')
Outputs:
- root_inverse: float32 [8192, 8192], P('row', 'col')
- child_inverse: float32 [2048, 8192], P('col', 'row')
The draws below stay inside these ranges and needn't reach their ends.
Inputs may be any that keep to these rules, and one draw needn't show every extreme that they name: sel_tiles holds 32 distinct tile indices in increasing order; rows of coupling outside the listed tiles are zero. factor is lower triangular with a diagonal between 1 and 1.5.
All inputs are finite; a program needn't handle non-finite values.
Results may differ from the reference program's by a relative error of at most 0.003.
Values may be sent and summed in bfloat16 or wider, within the bound.
A program may use at most 128 MiB of HBM per device.

```python
import jax
import jax.numpy as jnp

S = 8192
TILE = 128
NCH = 2048
R = 32


def chosen_tiles(key):
    order = jax.random.permutation(jax.random.fold_in(key, 7), S // TILE)
    return jnp.sort(order[:R]).astype(jnp.int32)


def draw_sel_tiles(key, part):
    return chosen_tiles(key)


def draw_factor(key, part):
    first = jax.random.fold_in(key, 11)
    second = jax.random.fold_in(key, 13)
    rows = jnp.arange(S)[:, None]
    cols = jnp.arange(S)[None, :]
    lower = jax.random.normal(first, (S, S), jnp.float32)
    lower = lower * S ** (-0.5)
    diag = 1.0 + 0.5 * jax.random.uniform(second, (S,), jnp.float32)
    full = jnp.where(rows > cols, lower, 0.0) + jnp.where(rows == cols, diag[None, :], 0.0)
    return full.astype(jnp.bfloat16)


def draw_coupling(key, part):
    tiles = chosen_tiles(key)
    tile_of = (jnp.arange(S) // TILE).astype(jnp.int32)
    member = jnp.any(tile_of[:, None] == tiles[None, :], axis=1)
    values = 0.5 * jax.random.normal(jax.random.fold_in(key, 5), (S, NCH), jnp.float32)
    return jnp.where(member[:, None], values, 0.0).astype(jnp.bfloat16)


def setup_inputs(seed: int = 0) -> dict:
    key_of = jax.random.split(jax.random.key(seed), 4)
    factor = draw_factor(jax.random.fold_in(key_of[3], 71), 0)
    sel_tiles = draw_sel_tiles(jax.random.fold_in(key_of[3], 71), 0)
    coupling = draw_coupling(jax.random.fold_in(key_of[3], 71), 0)
    return {"factor": factor, "sel_tiles": sel_tiles, "coupling": coupling}


def reference(factor, sel_tiles, coupling):
    gram = jnp.dot(factor.T, factor, preferred_element_type=jnp.float32)
    rounded = gram.astype(jnp.bfloat16)
    tile_of = (jnp.arange(S) // TILE).astype(jnp.int32)
    member = jnp.any(tile_of[:, None] == sel_tiles[None, :], axis=1)
    product = jnp.dot(coupling.T, rounded.T, preferred_element_type=jnp.float32)
    child = jnp.where(member[None, :], -product, jnp.float32(0.0))
    return gram, child
```

```python
import functools
import math

import jax
import jax.numpy as jnp
from jax import lax
from jax.experimental import pallas as pl
from jax.experimental.pallas import tpu as pltpu
from jax.sharding import PartitionSpec as P

TILE = 128
MESH = pl.DeviceIdType.MESH
SKEW = 2


def gather_kernel(dims, f_ref, a_ref, b_ref, recv_a, recv_b, send_z, send_p, send_b, send_f, local_a, stage):
    levels, wide, high, cores, chunks = dims
    rows, width = f_ref.shape
    narrow = width // cores
    h = rows // chunks
    r, c = lax.axis_index("row"), lax.axis_index("col")
    k, z = lax.rem(r, cores), r // cores
    x, y = lax.rem(c, wide), c // wide
    x0, y0 = lax.rem(z, wide), z // wide
    source = c == z

    def chunk_rows(block, j):
        return pl.ds(pl.multiple_of(block * rows + j * h, h), h)

    def remote(src, dst, send, recv, row, col):
        return pltpu.make_async_remote_copy(
            src_ref=src, dst_ref=dst, send_sem=send, recv_sem=recv,
            device_id=(row, col), device_id_type=MESH,
        )

    def copies(t, j):
        m = z + t
        inside = m < levels
        has = inside & (m >= c)
        block = m * cores + k
        at = chunk_rows(block, j)
        if t == 0:
            def src(cols):
                return f_ref.at[pl.ds(j * h, h), cols]
        else:
            def src(cols):
                return a_ref.at[at, cols]
        everything = pl.ds(0, width)
        found = []
        for kk in range(cores):
            piece = src(pl.ds(kk * narrow, narrow))
            into = b_ref.at[at, :]
            for dx in range(1, wide):
                xt = lax.rem(x + dx, wide)
                found.append((
                    source & inside & (m >= y * wide + xt),
                    remote(piece, into, send_b.at[kk, dx, t, j], recv_b.at[block, j],
                           z * cores + kk, y * wide + xt),
                    False,
                ))
            for dy in range(1, high):
                yt = lax.rem(y + dy, high)
                found.append((
                    source & inside & (m >= yt * wide),
                    remote(piece, into, send_b.at[kk, wide - 1 + dy, t, j], recv_b.at[block, j],
                           z * cores + kk, yt * wide + x),
                    False,
                ))
        found.append((
            has & (z > 0),
            remote(src(everything), a_ref.at[at, :], send_z.at[t, j], recv_a.at[block, j],
                   r - cores, c),
            False,
        ))
        for dk in range(1, cores):
            other = z * cores + lax.rem(k + dk, cores)
            found.append((
                has,
                remote(src(everything), a_ref.at[at, :], send_p.at[dk, t, j], recv_a.at[block, j], other, c),
                False,
            ))
        for kk in range(cores):
            piece = src(pl.ds(kk * narrow, narrow))
            into = b_ref.at[at, :]
            found.append((
                source & inside & (k != kk),
                remote(piece, into, send_b.at[kk, 0, t, j], recv_b.at[block, j], z * cores + kk, c),
                False,
            ))
        return found

    def keep(t, j):
        m = z + t
        at = chunk_rows(m * cores + k, j)
        here = f_ref.at[pl.ds(j * h, h), :] if t == 0 else a_ref.at[at, :]
        inside = (m < levels) & (m >= c)

        @pl.when(inside if t == 0 else inside & source)
        def _():
            load = pltpu.make_async_copy(here, stage, local_a.at[0])
            load.start()
            load.wait()
            if t == 0:
                pltpu.make_async_copy(stage, a_ref.at[at, :], local_a.at[1]).start()
            for kk in range(cores):
                @pl.when(source & (k == kk))
                def _():
                    store = pltpu.make_async_copy(
                        stage.at[:, pl.ds(kk * narrow, narrow)], b_ref.at[at, :], local_a.at[2]
                    )
                    store.start()
                    store.wait()
            if t == 0:
                pltpu.make_async_copy(stage, a_ref.at[at, :], local_a.at[1]).wait()

    def forwards(t, j, p):
        m = z + t
        block = m * cores + p
        part = b_ref.at[chunk_rows(block, j), :]
        mine = (x == x0) & (y != y0) & (m < levels)
        found = []
        for dx in range(1, wide):
            xt = lax.rem(x + dx, wide)
            found.append((
                mine & (m >= y * wide + xt),
                remote(part, part, send_f.at[dx, p, t, j], recv_b.at[block, j], r, y * wide + xt),
            ))
        return mine & (m >= y * wide), found

    def arrived(ref, sem):
        remote(ref, ref, send_z.at[0, 0], sem, r, c).wait_recv()

    def step(t, j):
        m = z + t
        block = m * cores + k
        if t > 0:
            @pl.when((m < levels) & (m >= c))
            def _():
                arrived(a_ref.at[chunk_rows(block, j), :], recv_a.at[block, j])
        for condition, copy, _ in copies(t, j):
            pl.when(condition)(copy.start)
        keep(t, j)

    def forward(t, j):
        for p in range(cores):
            due, found = forwards(t, j, p)
            block = (z + t) * cores + p

            @pl.when(due)
            def _():
                arrived(b_ref.at[chunk_rows(block, j), :], recv_b.at[block, j])
            for condition, copy in found:
                pl.when(condition)(copy.start)

    order = [(t, j) for t in range(levels) for j in range(chunks)]
    for n, (t, j) in enumerate(order):
        step(t, j)
        if n >= SKEW:
            forward(*order[n - SKEW])
    for t, j in order[len(order) - SKEW:]:
        forward(t, j)

    for t, j in order:
        m = z + t
        inside = m < levels
        for dk in range(1, cores):
            block = m * cores + lax.rem(k + dk, cores)

            @pl.when(inside & (m >= c))
            def _():
                arrived(a_ref.at[chunk_rows(block, j), :], recv_a.at[block, j])

            @pl.when(inside & source)
            def _():
                arrived(b_ref.at[chunk_rows(block, j), :], recv_b.at[block, j])
        for p in range(cores):
            block = m * cores + p

            @pl.when(inside & (x != x0) & (m >= c))
            def _():
                arrived(b_ref.at[chunk_rows(block, j), :], recv_b.at[block, j])
        for condition, copy, local in copies(t, j):
            pl.when(condition)(copy.wait if local else copy.wait_send)
        for p in range(cores):
            for condition, copy in forwards(t, j, p)[1]:
                pl.when(condition)(copy.wait_send)


def gather(factor, n_row, n_col):
    rows, width = factor.shape
    cores = n_row // n_col
    wide = next(w for w in range(math.isqrt(n_col), 0, -1) if n_col % w == 0)
    high = n_col // wide
    levels = n_col
    chunks = max(1, 32 // n_row)
    dma = pltpu.SemaphoreType.DMA
    whole = rows * n_row
    return pl.pallas_call(
        functools.partial(gather_kernel, (levels, wide, high, cores, chunks)),
        out_shape=(
            jax.ShapeDtypeStruct((whole, width), factor.dtype),
            jax.ShapeDtypeStruct((whole, width // cores), factor.dtype),
        ),
        in_specs=[pl.BlockSpec(memory_space=pl.ANY)],
        out_specs=(pl.BlockSpec(memory_space=pl.ANY), pl.BlockSpec(memory_space=pl.ANY)),
        scratch_shapes=[
            dma((n_row, chunks)),
            dma((n_row, chunks)),
            dma((levels, chunks)),
            dma((cores, levels, chunks)),
            dma((cores, wide + high, levels, chunks)),
            dma((wide, cores, levels, chunks)),
            dma((3,)),
            pltpu.VMEM((rows // chunks, width), factor.dtype),
        ],
        compiler_params=pltpu.CompilerParams(has_side_effects=True),
        cost_estimate=pl.CostEstimate(flops=0, bytes_accessed=whole * width * 32, transcendentals=0),
    )(factor)


LAG = 2


def block_flows(pieces):
    half = pieces // 2
    found = []

    def add(block, hops, first=0, last=pieces):
        found.append((block, block, hops, first, last))

    side = [((3, 1), (2, 1)), ((2, 1), (1, 1)), ((1, 1), (1, 3)), ((1, 3), (1, 2)), ((1, 2), (1, 0))]
    add((3, 3), [((3, 3), (2, 3)), ((2, 3), (1, 3)), ((1, 3), (0, 3)), ((3, 3), (3, 1)), ((3, 3), (3, 2)),
                 ((3, 2), (3, 0))])
    add((3, 2), [((3, 2), (2, 2)), ((2, 2), (2, 3)), ((2, 3), (2, 1)), ((2, 2), (2, 0)), ((2, 2), (1, 2)),
                 ((1, 2), (0, 2))])
    add((3, 1), side + [((1, 1), (0, 1))], 0, half)
    add((3, 1), side + [((1, 3), (0, 3)), ((0, 3), (0, 1))], half, pieces)
    add((3, 0), [((3, 0), (2, 0)), ((2, 0), (2, 1)), ((2, 1), (2, 3)), ((2, 3), (1, 3)), ((1, 3), (0, 3)),
                 ((0, 3), (0, 1)), ((0, 1), (0, 0)), ((0, 3), (0, 2)), ((2, 0), (1, 0))])
    add((2, 0), [((2, 0), (1, 0)), ((1, 0), (0, 0)), ((0, 0), (0, 1)), ((0, 0), (0, 2))])
    add((1, 0), [((1, 0), (0, 0)), ((0, 0), (0, 1))])
    add((2, 1), [((2, 1), (1, 1)), ((1, 1), (0, 1)), ((1, 1), (1, 0)), ((1, 0), (1, 2))])
    add((1, 1), [((1, 1), (0, 1)), ((1, 1), (1, 0))])
    add((2, 2), [((2, 2), (2, 3)), ((2, 3), (2, 1)), ((2, 2), (2, 0)), ((2, 2), (1, 2)), ((1, 2), (0, 2))])
    return found


def coupling_flows(pieces):
    found = []
    for c in range(4):
        for z in range(4):
            hops = [((a, c), (a - 1, c)) for a in range(z, 0, -1)] + [((a, c), (a + 1, c)) for a in range(z, 3)]
            found.append((("u", z, c), (z, c), hops, 0, pieces))
    return found


ORDER = [6, 8, 5, 2, 23, 9, 4, 11, 25, 18, 1, 3, 10, 20, 12, 13, 19, 0, 7, 17, 15, 16, 14, 22, 24, 21]


@functools.cache
def plan(pieces, coupling_pieces):
    flows = block_flows(pieces) + coupling_flows(coupling_pieces)
    busy, hops = {}, []
    for index in ORDER:
        block, source, route, first, last = flows[index]
        n, at = last - first, {source: 0}
        for p, q in route:
            t, used = at[p], busy.setdefault((p, q), [])
            while any(t < e and s < t + n for s, e in used):
                t += 1
            used.append((t, t + n))
            at[q] = t + LAG
            hops.append((block, p, q, first, last, t))
    chips = [(z, c) for z in range(4) for c in range(4)]
    slots = {chip: {} for chip in chips}
    needs = {chip: set() for chip in chips}
    for z, c in chips:
        for m in range(max(z, c), 4):
            slots[z, c][m, c] = m
            needs[z, c].add((m, c))
            if c != z:
                slots[z, c][m, z] = 4 + m
                needs[z, c].add((m, z))
    for block, p, q, first, last, t in hops:
        if block[0] != "u" and block not in slots[q]:
            slots[q][block] = min(set(range(8)) - set(slots[q].values()))
    due = {}
    for chip in chips:
        z, c = chip
        ready = {(z, c): [1] * pieces}
        for block, p, q, first, last, t in hops:
            if q == chip:
                for j in range(first, last):
                    ready.setdefault(block, [None] * pieces)[j] = t + LAG + j - first
        for m in range(max(z, c), 4):
            both = [ready[m, c], ready[m, z]]
            due[chip, m] = 1 + max(max(b[2 * j], b[2 * j + 1]) - 2 * j for b in both for j in range(pieces // 2))
    steps = max([t + last - first + LAG for block, p, q, first, last, t in hops] + [d + pieces for d in due.values()])
    return hops, slots, needs, due, steps


def stream_kernel(pieces, coupling_pieces, f_ref, u_ref, x_ref, ub_ref, g_ref, send, send_u, near, near_u, recv,
                  recv_u, recv_near, recv_near_u, local, acc, a_buf, b_buf, stage, stage_u, zeros):
    hops, slots, needs, due, steps = plan(pieces, coupling_pieces)
    rows, width = f_ref.shape
    depth, narrow = u_ref.shape
    h, hu, quarter = rows // pieces, depth // coupling_pieces, width // 4
    tall = acc.shape[0]
    r, c = lax.axis_index("row"), lax.axis_index("col")
    k, z = lax.rem(r, 2), r // 2
    chip = z * 4 + c
    owner = z >= c

    def at_rows(slot, core, j):
        return pl.ds(pl.multiple_of((slot * 2 + core) * rows + j * h, h), h)

    def remote(src, dst, send_sem, recv_sem, row, col):
        return pltpu.make_async_remote_copy(
            src_ref=src, dst_ref=dst, send_sem=send_sem, recv_sem=recv_sem,
            device_id=(row, col), device_id_type=MESH,
        )

    def shapes(block, j):
        if block[0] != block[1]:
            return [(None, width)]
        part = (k * pieces + j) // (pieces // 2)
        return [(part == q, (q + 1) * quarter) for q in range(4)]

    def each(block, j, act):
        if block[0] == "u":
            act(None)
            return
        for condition, columns in shapes(block, j):
            if condition is None:
                act(columns)
            else:
                pl.when(condition)(functools.partial(act, columns))

    def hop_copy(hop, number, j, columns):
        block, p, q, first, last, t = hop
        if block[0] == "u":
            at = pl.ds(pl.multiple_of(j * hu, hu), hu)
            src = u_ref.at[at, :] if p == block[1:] else ub_ref.at[block[1] * 2 + k, at, :]
            return remote(src, ub_ref.at[block[1] * 2 + k, at, :], send_u.at[number, j], recv_u.at[block[1], j],
                          q[0] * 2 + k, q[1])
        cols = pl.ds(0, columns)
        if p == block:
            src = f_ref.at[pl.ds(pl.multiple_of(j * h, h), h), cols]
        else:
            src = x_ref.at[at_rows(slots[p][block], k, j), cols]
        slot = slots[q][block]
        return remote(src, x_ref.at[at_rows(slot, k, j), cols], send.at[number, j], recv.at[slot, j],
                      q[0] * 2 + k, q[1])

    def near_copy(slot, j, src=None):
        at = at_rows(slot, k, j)
        return remote(x_ref.at[at, :] if src is None else src, x_ref.at[at, :], near.at[slot, j],
                      recv_near.at[slot, j], z * 2 + 1 - k, c)

    def near_arrival(slot, j):
        ref = x_ref.at[at_rows(slot, 1 - k, j), :]
        return remote(ref, ref, near.at[slot, j], recv_near.at[slot, j], r, c)

    def near_copy_u(level, j, src=None):
        at = pl.ds(pl.multiple_of(j * hu, hu), hu)
        ref = ub_ref.at[level * 2 + k, at, :]
        return remote(ref if src is None else src, ref, near_u.at[level, j], recv_near_u.at[level, j],
                      z * 2 + 1 - k, c)

    def own_rows(j):
        return f_ref.at[pl.ds(pl.multiple_of(j * h, h), h), :]

    def own_rows_u(j):
        return u_ref.at[pl.ds(pl.multiple_of(j * hu, hu), hu), :]

    chips = [(a, b) for a in range(4) for b in range(4)]
    incoming = {chip_: [hop for hop in hops if hop[2] == chip_] for chip_ in chips}
    outgoing = {chip_: [] for chip_ in chips}
    count, count_u = {}, {}
    for hop in hops:
        counts = count_u if hop[0][0] == "u" else count
        number = counts.get(hop[1], 0)
        counts[hop[1]] = number + 1
        outgoing[hop[1]].append((hop, number))

    zeros[...] = jnp.zeros_like(zeros)

    def fill(slot, begin):
        def one(j, carry):
            for condition, columns in shapes((0, 0), j):
                if columns < width:
                    copy = pltpu.make_async_copy(
                        zeros.at[:, pl.ds(0, width - columns)],
                        x_ref.at[at_rows(slot, k, j), pl.ds(columns, width - columns)], local.at[1])

                    @pl.when(condition)
                    def _():
                        copy.start()
                        copy.wait()
            return carry
        lax.fori_loop(0, pieces, one, 0)

    def spread(j, carry):
        @pl.when(owner)
        def _():
            near_copy(z, j, own_rows(j)).start()
        return carry

    def spread_u(j, carry):
        near_copy_u(z, j, own_rows_u(j)).start()
        return carry

    def step(t, carry):
        for place in chips:
            @pl.when(chip == place[0] * 4 + place[1])
            def _():
                for hop in incoming[place]:
                    block, p, q, first, last, t0 = hop

                    @pl.when((t >= t0 + LAG) & (t < t0 + LAG + last - first))
                    def _():
                        j = t - (t0 + LAG) + first
                        each(block, j, lambda columns: hop_copy(hop, 0, j, columns).wait_recv())
                        if block[0] == "u":
                            near_copy_u(block[1], j).start()
                        elif block in needs[place]:
                            near_copy(slots[place][block], j).start()
                for hop, number in outgoing[place]:
                    block, p, q, first, last, t0 = hop

                    @pl.when((t >= t0) & (t < t0 + last - first))
                    def _():
                        j = t - t0 + first
                        each(block, j, lambda columns: hop_copy(hop, number, j, columns).start())

        def consume(m, carry):
            begin = jnp.int32(-1000)
            for level in range(4):
                begin = jnp.where(m == level, begins[level], begin)
            ago = t - begin

            @pl.when((ago >= 0) & (ago < pieces) & (lax.rem(ago, 2) == 0))
            def _():
                slot_b = jnp.where(c == z, m, 4 + m)
                for i in range(2):
                    near_arrival(m, ago + i).wait_recv()

                    @pl.when(c != z)
                    def _():
                        near_arrival(slot_b, ago + i).wait_recv()
                loads = []
                cols = pl.ds(pl.multiple_of(k * tall, tall), tall)
                for core in range(2):
                    at_a = pl.ds(pl.multiple_of((m * 2 + core) * rows + ago * h, 2 * h), 2 * h)
                    at_b = pl.ds(pl.multiple_of((slot_b * 2 + core) * rows + ago * h, 2 * h), 2 * h)
                    into = pl.ds(core * 2 * h, 2 * h)
                    loads.append(pltpu.make_async_copy(x_ref.at[at_a, :], a_buf.at[into, :], local.at[2 + core]))
                    loads.append(pltpu.make_async_copy(x_ref.at[at_b, cols], b_buf.at[into, :], local.at[4 + core]))
                for copy in loads:
                    copy.start()
                for copy in loads:
                    copy.wait()
                tile = min(256, tall)

                def rows_of(i, carry):
                    at = pl.ds(pl.multiple_of(i * tile, tile), tile)
                    acc[at, :] += lax.dot_general(
                        b_buf[:, at], a_buf[...], (((0,), (0,)), ((), ())), preferred_element_type=jnp.float32)
                    return carry
                lax.fori_loop(0, tall // tile, rows_of, 0)
            return carry
        lax.fori_loop(0, 4, consume, 0)
        return carry

    begins = []
    for m in range(4):
        begin = jnp.int32(-1000)
        for place in chips:
            if (place, m) in due:
                begin = jnp.where(chip == place[0] * 4 + place[1], due[place, m], begin)
        begins.append(begin)

    lax.fori_loop(0, pieces, spread, 0)
    lax.fori_loop(0, coupling_pieces, spread_u, 0)
    own = pltpu.make_async_copy(f_ref, stage, local.at[0])
    keep = pltpu.make_async_copy(stage, x_ref.at[pl.ds(pl.multiple_of((z * 2 + k) * rows, rows), rows), :], local.at[0])

    own_u = pltpu.make_async_copy(u_ref, stage_u, local.at[1])
    keep_u = pltpu.make_async_copy(stage_u, ub_ref.at[r], local.at[1])

    @pl.when(owner)
    def _():
        own.start()
    acc[...] = jnp.zeros_like(acc)
    for place in chips:
        filled = [slots[place][b] for b in needs[place] if b[0] == b[1] and b != place]
        for slot in filled:
            @pl.when(chip == place[0] * 4 + place[1])
            def _():
                fill(slot, 0)

    @pl.when(owner)
    def _():
        own.wait()
        keep.start()
        keep.wait()
    own_u.start()
    own_u.wait()
    keep_u.start()
    keep_u.wait()
    lax.fori_loop(0, steps, step, 0)
    out = pltpu.make_async_copy(acc, g_ref, local.at[0])
    out.start()

    def settle(j, carry):
        @pl.when(owner)
        def _():
            near_copy(z, j, own_rows(j)).wait_send()
        return carry
    lax.fori_loop(0, pieces, settle, 0)

    def settle_u(j, carry):
        for level in range(4):
            near_copy_u(level, j).wait_send()
            at = pl.ds(pl.multiple_of(j * hu, hu), hu)
            ref = ub_ref.at[level * 2 + 1 - k, at, :]
            remote(ref, ref, near_u.at[level, j], recv_near_u.at[level, j], r, c).wait_recv()
        return carry
    lax.fori_loop(0, coupling_pieces, settle_u, 0)
    for place in chips:
        @pl.when(chip == place[0] * 4 + place[1])
        def _():
            for hop, number in outgoing[place]:
                def sent(j, carry):
                    each(hop[0], j, lambda columns: hop_copy(hop, number, j, columns).wait_send())
                    return carry
                lax.fori_loop(hop[3], hop[4], sent, 0)
            for hop in incoming[place]:
                if hop[0][0] != "u" and hop[0] in needs[place]:
                    def passed(j, carry):
                        near_copy(slots[place][hop[0]], j).wait_send()
                        return carry
                    lax.fori_loop(hop[3], hop[4], passed, 0)
    out.wait()


def stream(factor, coupling, n_row, n_col):
    rows, width = factor.shape
    depth, narrow = coupling.shape
    pieces, coupling_pieces = 16, 4
    hops = plan(pieces, coupling_pieces)[0]
    out_count = max(sum(hop[1] == chip and hop[0][0] != "u" for hop in hops) for chip in {h[1] for h in hops})
    out_count_u = max(sum(hop[1] == chip and hop[0][0] == "u" for hop in hops) for chip in {h[1] for h in hops})
    tall = width // 2
    h = rows // pieces
    dma = pltpu.SemaphoreType.DMA
    return pl.pallas_call(
        functools.partial(stream_kernel, pieces, coupling_pieces),
        out_shape=(
            jax.ShapeDtypeStruct((8 * 2 * rows, width), factor.dtype),
            jax.ShapeDtypeStruct((n_row, depth, narrow), coupling.dtype),
            jax.ShapeDtypeStruct((tall, width), jnp.float32),
        ),
        in_specs=[pl.BlockSpec(memory_space=pl.ANY)] * 2,
        out_specs=[pl.BlockSpec(memory_space=pl.ANY)] * 3,
        scratch_shapes=[
            dma((out_count, pieces)),
            dma((out_count_u, coupling_pieces)),
            dma((8, pieces)),
            dma((4, coupling_pieces)),
            dma((8, pieces)),
            dma((4, coupling_pieces)),
            dma((8, pieces)),
            dma((4, coupling_pieces)),
            dma((6,)),
            pltpu.VMEM((tall, width), jnp.float32),
            pltpu.VMEM((4 * h, width), factor.dtype),
            pltpu.VMEM((4 * h, tall), factor.dtype),
            pltpu.VMEM((rows, width), factor.dtype),
            pltpu.VMEM((depth, narrow), coupling.dtype),
            pltpu.VMEM((h, width), factor.dtype),
        ],
        compiler_params=pltpu.CompilerParams(has_side_effects=True, vmem_limit_bytes=48 * 1024 * 1024),
        cost_estimate=pl.CostEstimate(flops=0, bytes_accessed=rows * width * 64, transcendentals=0),
    )(factor, coupling)


def exchange_kernel(n_col, part_ref, out_ref, send, recv):
    r, c = lax.axis_index("row"), lax.axis_index("col")
    depth = out_ref.shape[1]
    started = []
    for d in range(1, n_col):
        ct = lax.rem(c + d, n_col)
        copy = pltpu.make_async_remote_copy(
            src_ref=part_ref.at[pl.ds(pl.multiple_of(ct * depth, depth), depth), :],
            dst_ref=out_ref.at[d - 1],
            send_sem=send.at[d - 1],
            recv_sem=recv.at[d - 1],
            device_id=(r, ct),
            device_id_type=MESH,
        )
        copy.start()
        started.append(copy)
    for copy in started:
        copy.wait()


def exchange(part, n_col):
    total, width = part.shape
    dma = pltpu.SemaphoreType.DMA
    return pl.pallas_call(
        functools.partial(exchange_kernel, n_col),
        out_shape=jax.ShapeDtypeStruct((n_col - 1, total // n_col, width), part.dtype),
        in_specs=[pl.BlockSpec(memory_space=pl.ANY)],
        out_specs=pl.BlockSpec(memory_space=pl.ANY),
        scratch_shapes=[dma((n_col - 1,)), dma((n_col - 1,))],
        compiler_params=pltpu.CompilerParams(has_side_effects=True),
    )(part)


def general(n_row, n_col, factor, coupling):
    rows_here = factor.shape[0]
    row_index, col_index = lax.axis_index("row"), lax.axis_index("col")
    cores = n_row // n_col
    below, partner = gather(factor, n_row, n_col)
    coupling_full = lax.all_gather(coupling, "row", axis=1, tiled=True)

    def product(level, below, partner):
        first = level * rows_here * cores
        return lax.dot_general(
            partner[first:], below[first:], (((0,), (0,)), ((), ())), preferred_element_type=jnp.float32
        )

    gram = lax.switch(
        jnp.maximum(row_index // cores, col_index),
        [functools.partial(product, level) for level in range(n_col)],
        below,
        partner,
    )
    rounded = gram.astype(jnp.bfloat16)
    part = lax.dot_general(
        coupling_full, rounded, (((0,), (1,)), ((), ())), preferred_element_type=jnp.float32
    ).astype(jnp.bfloat16)
    return gram, part


def body(n_row, n_col, factor, sel_tiles, coupling):
    rows_here = factor.shape[0]
    row_index, col_index = lax.axis_index("row"), lax.axis_index("col")
    cores = n_row // n_col
    if (n_row, n_col) == (8, 4):
        _, pieces, gram = stream(factor, coupling, n_row, n_col)
        rounded = gram.astype(jnp.bfloat16)
        part = lax.dot_general(
            pieces, rounded, (((1,), (1,)), ((), ())), preferred_element_type=jnp.float32
        ).astype(jnp.bfloat16)
        part = part.reshape(-1, part.shape[-1])
    else:
        gram, part = general(n_row, n_col, factor, coupling)
    global_rows = row_index * rows_here + jnp.arange(rows_here, dtype=jnp.int32)
    member = jnp.any((global_rows // TILE)[:, None] == sel_tiles[None, :], axis=1)
    depth = part.shape[0] // n_col
    arrived = exchange(part, n_col)
    summed = lax.dynamic_slice_in_dim(part, col_index * depth, depth, 0).astype(jnp.float32)
    for d in range(n_col - 1):
        summed = summed + arrived[d].astype(jnp.float32)
    child = jnp.where(member[None, :], -summed, jnp.float32(0.0))
    return (gram, child)


def solution(mesh):
    placed = (P("row", "col"), P(), P("col", "row"))
    return jax.shard_map(
        functools.partial(body, mesh.shape["row"], mesh.shape["col"]),
        mesh=mesh,
        in_specs=placed,
        out_specs=(P("row", "col"), P("col", "row")),
        check_vma=False,
    )
```

```python
import functools
import math

import jax
import jax.numpy as jnp
from jax import lax
from jax.experimental import pallas as pl
from jax.experimental.pallas import tpu as pltpu
from jax.sharding import PartitionSpec as P

TILE = 128
MESH = pl.DeviceIdType.MESH
SKEW = 2


def gather_kernel(dims, f_ref, a_ref, b_ref, recv_a, recv_b, send_z, send_p, send_b, send_f, local_a, stage):
    levels, wide, high, cores, chunks = dims
    rows, width = f_ref.shape
    narrow = width // cores
    h = rows // chunks
    r, c = lax.axis_index("row"), lax.axis_index("col")
    k, z = lax.rem(r, cores), r // cores
    x, y = lax.rem(c, wide), c // wide
    x0, y0 = lax.rem(z, wide), z // wide
    source = c == z

    def chunk_rows(block, j):
        return pl.ds(pl.multiple_of(block * rows + j * h, h), h)

    def remote(src, dst, send, recv, row, col):
        return pltpu.make_async_remote_copy(
            src_ref=src, dst_ref=dst, send_sem=send, recv_sem=recv,
            device_id=(row, col), device_id_type=MESH,
        )

    def copies(t, j):
        m = z + t
        inside = m < levels
        has = inside & (m >= c)
        block = m * cores + k
        at = chunk_rows(block, j)
        if t == 0:
            def src(cols):
                return f_ref.at[pl.ds(j * h, h), cols]
        else:
            def src(cols):
                return a_ref.at[at, cols]
        everything = pl.ds(0, width)
        found = []
        for kk in range(cores):
            piece = src(pl.ds(kk * narrow, narrow))
            into = b_ref.at[at, :]
            for dx in range(1, wide):
                xt = lax.rem(x + dx, wide)
                found.append((
                    source & inside & (m >= y * wide + xt),
                    remote(piece, into, send_b.at[kk, dx, t, j], recv_b.at[block, j],
                           z * cores + kk, y * wide + xt),
                    False,
                ))
            for dy in range(1, high):
                yt = lax.rem(y + dy, high)
                found.append((
                    source & inside & (m >= yt * wide),
                    remote(piece, into, send_b.at[kk, wide - 1 + dy, t, j], recv_b.at[block, j],
                           z * cores + kk, yt * wide + x),
                    False,
                ))
        found.append((
            has & (z > 0),
            remote(src(everything), a_ref.at[at, :], send_z.at[t, j], recv_a.at[block, j],
                   r - cores, c),
            False,
        ))
        for dk in range(1, cores):
            other = z * cores + lax.rem(k + dk, cores)
            found.append((
                has,
                remote(src(everything), a_ref.at[at, :], send_p.at[dk, t, j], recv_a.at[block, j], other, c),
                False,
            ))
        for kk in range(cores):
            piece = src(pl.ds(kk * narrow, narrow))
            into = b_ref.at[at, :]
            found.append((
                source & inside & (k != kk),
                remote(piece, into, send_b.at[kk, 0, t, j], recv_b.at[block, j], z * cores + kk, c),
                False,
            ))
        return found

    def keep(t, j):
        m = z + t
        at = chunk_rows(m * cores + k, j)
        here = f_ref.at[pl.ds(j * h, h), :] if t == 0 else a_ref.at[at, :]
        inside = (m < levels) & (m >= c)

        @pl.when(inside if t == 0 else inside & source)
        def _():
            load = pltpu.make_async_copy(here, stage, local_a.at[0])
            load.start()
            load.wait()
            if t == 0:
                pltpu.make_async_copy(stage, a_ref.at[at, :], local_a.at[1]).start()
            for kk in range(cores):
                @pl.when(source & (k == kk))
                def _():
                    store = pltpu.make_async_copy(
                        stage.at[:, pl.ds(kk * narrow, narrow)], b_ref.at[at, :], local_a.at[2]
                    )
                    store.start()
                    store.wait()
            if t == 0:
                pltpu.make_async_copy(stage, a_ref.at[at, :], local_a.at[1]).wait()

    def forwards(t, j, p):
        m = z + t
        block = m * cores + p
        part = b_ref.at[chunk_rows(block, j), :]
        mine = (x == x0) & (y != y0) & (m < levels)
        found = []
        for dx in range(1, wide):
            xt = lax.rem(x + dx, wide)
            found.append((
                mine & (m >= y * wide + xt),
                remote(part, part, send_f.at[dx, p, t, j], recv_b.at[block, j], r, y * wide + xt),
            ))
        return mine & (m >= y * wide), found

    def arrived(ref, sem):
        remote(ref, ref, send_z.at[0, 0], sem, r, c).wait_recv()

    def step(t, j):
        m = z + t
        block = m * cores + k
        if t > 0:
            @pl.when((m < levels) & (m >= c))
            def _():
                arrived(a_ref.at[chunk_rows(block, j), :], recv_a.at[block, j])
        for condition, copy, _ in copies(t, j):
            pl.when(condition)(copy.start)
        keep(t, j)

    def forward(t, j):
        for p in range(cores):
            due, found = forwards(t, j, p)
            block = (z + t) * cores + p

            @pl.when(due)
            def _():
                arrived(b_ref.at[chunk_rows(block, j), :], recv_b.at[block, j])
            for condition, copy in found:
                pl.when(condition)(copy.start)

    order = [(t, j) for t in range(levels) for j in range(chunks)]
    for n, (t, j) in enumerate(order):
        step(t, j)
        if n >= SKEW:
            forward(*order[n - SKEW])
    for t, j in order[len(order) - SKEW:]:
        forward(t, j)

    for t, j in order:
        m = z + t
        inside = m < levels
        for dk in range(1, cores):
            block = m * cores + lax.rem(k + dk, cores)

            @pl.when(inside & (m >= c))
            def _():
                arrived(a_ref.at[chunk_rows(block, j), :], recv_a.at[block, j])

            @pl.when(inside & source)
            def _():
                arrived(b_ref.at[chunk_rows(block, j), :], recv_b.at[block, j])
        for p in range(cores):
            block = m * cores + p

            @pl.when(inside & (x != x0) & (m >= c))
            def _():
                arrived(b_ref.at[chunk_rows(block, j), :], recv_b.at[block, j])
        for condition, copy, local in copies(t, j):
            pl.when(condition)(copy.wait if local else copy.wait_send)
        for p in range(cores):
            for condition, copy in forwards(t, j, p)[1]:
                pl.when(condition)(copy.wait_send)


def gather(factor, n_row, n_col):
    rows, width = factor.shape
    cores = n_row // n_col
    wide = next(w for w in range(math.isqrt(n_col), 0, -1) if n_col % w == 0)
    high = n_col // wide
    levels = n_col
    chunks = max(1, 32 // n_row)
    dma = pltpu.SemaphoreType.DMA
    whole = rows * n_row
    return pl.pallas_call(
        functools.partial(gather_kernel, (levels, wide, high, cores, chunks)),
        out_shape=(
            jax.ShapeDtypeStruct((whole, width), factor.dtype),
            jax.ShapeDtypeStruct((whole, width // cores), factor.dtype),
        ),
        in_specs=[pl.BlockSpec(memory_space=pl.ANY)],
        out_specs=(pl.BlockSpec(memory_space=pl.ANY), pl.BlockSpec(memory_space=pl.ANY)),
        scratch_shapes=[
            dma((n_row, chunks)),
            dma((n_row, chunks)),
            dma((levels, chunks)),
            dma((cores, levels, chunks)),
            dma((cores, wide + high, levels, chunks)),
            dma((wide, cores, levels, chunks)),
            dma((3,)),
            pltpu.VMEM((rows // chunks, width), factor.dtype),
        ],
        compiler_params=pltpu.CompilerParams(has_side_effects=True),
        cost_estimate=pl.CostEstimate(flops=0, bytes_accessed=whole * width * 32, transcendentals=0),
    )(factor)


LAG = 2
G = ("g", 1, 0)


def block_flows(pieces):
    half = pieces // 2
    found = []

    def add(block, source, hops, first=0, last=pieces):
        found.append((block, source, hops, first, last))

    add((3, 3), (3, 3), [((3, 3), (2, 3)), ((2, 3), (1, 3)), ((1, 3), (0, 3)), ((3, 3), (3, 1)), ((3, 3), (3, 2)),
                         ((3, 2), (3, 0))])
    add((3, 2), (3, 2), [((3, 2), (2, 2)), ((2, 2), (2, 3)), ((2, 3), (2, 1)), ((2, 2), (2, 0)), ((2, 2), (1, 2)),
                         ((1, 2), (0, 2))])
    add((3, 1), (3, 1), [((3, 1), (2, 1)), ((2, 1), (2, 0)), ((2, 0), (1, 0)), ((1, 0), (1, 1)), ((1, 1), (1, 3)),
                         ((1, 3), (1, 2))], 0, half)
    add((3, 1), (3, 1), [((3, 1), (2, 1)), ((2, 1), (1, 1)), ((1, 1), (1, 3)), ((1, 3), (1, 2)), ((1, 2), (1, 0))],
        half, pieces)
    add((3, 0), (3, 0), [((3, 0), (2, 0)), ((2, 0), (2, 1)), ((2, 1), (2, 3)), ((2, 3), (1, 3)), ((1, 3), (1, 2)),
                         ((1, 2), (1, 0)), ((1, 3), (0, 3)), ((0, 3), (0, 2)), ((0, 2), (0, 0))])
    add((2, 0), (2, 0), [((2, 0), (1, 0)), ((1, 0), (1, 1)), ((1, 1), (0, 1)), ((0, 1), (0, 0)), ((0, 0), (0, 2))])
    add((1, 0), (1, 0), [((1, 0), (0, 0))])
    add((2, 1), (2, 1), [((2, 1), (1, 1)), ((1, 1), (1, 0)), ((1, 0), (1, 2))])
    add((1, 1), (1, 1), [((1, 1), (1, 0))])
    add((2, 2), (2, 2), [((2, 2), (2, 3)), ((2, 3), (2, 1)), ((2, 2), (2, 0)), ((2, 2), (1, 2)), ((1, 2), (0, 2))])
    add(G, (1, 0), [((1, 0), (0, 0)), ((0, 0), (0, 1))], 0, half)
    add(G, (1, 0), [((1, 0), (1, 1)), ((1, 1), (0, 1))], half, pieces)
    return found


def coupling_flows(pieces):
    found = []
    for c in range(4):
        for z in range(4):
            hops = [((a, c), (a - 1, c)) for a in range(z, 0, -1)] + [((a, c), (a + 1, c)) for a in range(z, 3)]
            found.append((("u", z, c), (z, c), hops, 0, pieces))
    return found


ORDER = [3, 4, 19, 12, 0, 20, 23, 22, 21, 5, 25, 2, 13, 6, 16, 26, 27, 24, 1, 7, 18, 15, 17, 8, 9, 14, 10, 11]


@functools.cache
def plan(pieces, coupling_pieces):
    flows = block_flows(pieces) + coupling_flows(coupling_pieces)
    chips = [(z, c) for z in range(4) for c in range(4)]
    pairs = [(chip, m) for chip in chips if chip != (0, 1) for m in range(max(chip), 4)]
    busy, hops, due = {}, [], {}
    final = None
    for index in ORDER:
        block, source, route, first, last = flows[index]
        if block == G and final is None:
            due = ready_steps(pieces, hops, pairs)
            final = max(d for key, d in due.items() if key[0] == (1, 0)) + pieces // 4
        n, at = last - first, {source: final + 1 if block == G else 0}
        for p, q in route:
            t, used = at[p], busy.setdefault((p, q), [])
            while any(t < e and s < t + n for s, e in used):
                t += 1
            used.append((t, t + n))
            at[q] = t + LAG
            hops.append((block, p, q, first, last, t))
    slots = {chip: {} for chip in chips}
    needs = {chip: set() for chip in chips}
    for chip, m in pairs:
        z, c = chip
        slots[chip][m, c] = m
        needs[chip].add((m, c))
        if c != z:
            slots[chip][m, z] = 4 + m
            needs[chip].add((m, z))
    for block, p, q, first, last, t in hops:
        for chip in (p, q):
            if block[0] != "u" and block not in slots[chip] and block != chip:
                slots[chip][block] = min(set(range(8)) - set(slots[chip].values()))
    steps = max([t + last - first + LAG for block, p, q, first, last, t in hops] + [d + pieces // 4 for d in due.values()] + [final + 1])
    return hops, slots, needs, due, steps, final


def ready_steps(pieces, hops, pairs):
    due, group = {}, pieces // 8
    for chip, m in pairs:
        z, c = chip
        ready = {(z, c): [1] * pieces}
        for block, p, q, first, last, t in hops:
            if q == chip:
                for j in range(first, last):
                    ready.setdefault(block, [None] * pieces)[j] = t + LAG + j - first
        both = [ready[m, c], ready[m, z]]
        for part in range(4):
            begin = part * (pieces // 4)
            due[chip, m, part] = 1 + max(b[begin + j] - j // group * group for b in both for j in range(pieces // 4))
    return due


def stream_kernel(pieces, coupling_pieces, f_ref, u_ref, x_ref, ub_ref, g_ref, send, send_u, near, near_u, recv,
                  recv_u, recv_near, recv_near_u, turn, local, acc, a_buf, b_buf, stage, stage_u, zeros, flipped):
    hops, slots, needs, due, steps, final = plan(pieces, coupling_pieces)
    rows, width = f_ref.shape
    depth, narrow = u_ref.shape
    h, hu, quarter = rows // pieces, depth // coupling_pieces, width // 4
    tall = acc.shape[0]
    r, c = lax.axis_index("row"), lax.axis_index("col")
    k, z = lax.rem(r, 2), r // 2
    chip = z * 4 + c
    owner = z >= c

    def at_rows(slot, core, j):
        return pl.ds(pl.multiple_of((slot * 2 + core) * rows + j * h, h), h)

    def remote(src, dst, send_sem, recv_sem, row, col):
        return pltpu.make_async_remote_copy(
            src_ref=src, dst_ref=dst, send_sem=send_sem, recv_sem=recv_sem,
            device_id=(row, col), device_id_type=MESH,
        )

    def shapes(block, j):
        if block[0] != block[1]:
            return [(None, width)]
        part = (k * pieces + j) // (pieces // 2)
        return [(part == q, (q + 1) * quarter) for q in range(4)]

    def each(block, j, act):
        if block[0] == "u":
            act(None)
            return
        for condition, columns in shapes(block, j):
            if condition is None:
                act(columns)
            else:
                pl.when(condition)(functools.partial(act, columns))

    def hop_copy(hop, number, j, columns):
        block, p, q, first, last, t = hop
        if block[0] == "u":
            at = pl.ds(pl.multiple_of(j * hu, hu), hu)
            src = u_ref.at[at, :] if p == block[1:] else ub_ref.at[block[1] * 2 + k, at, :]
            return remote(src, ub_ref.at[block[1] * 2 + k, at, :], send_u.at[number, j], recv_u.at[block[1], j],
                          q[0] * 2 + k, q[1])
        cols = pl.ds(0, columns)
        if p == block:
            src = f_ref.at[pl.ds(pl.multiple_of(j * h, h), h), cols]
        else:
            src = x_ref.at[at_rows(slots[p][block], k, j), cols]
        slot = slots[q][block]
        return remote(src, x_ref.at[at_rows(slot, k, j), cols], send.at[number, j], recv.at[slot, j],
                      q[0] * 2 + k, q[1])

    def near_copy(slot, j, src=None):
        at = at_rows(slot, k, j)
        return remote(x_ref.at[at, :] if src is None else src, x_ref.at[at, :], near.at[slot, j],
                      recv_near.at[slot, j], z * 2 + 1 - k, c)

    def near_arrival(slot, j):
        ref = x_ref.at[at_rows(slot, 1 - k, j), :]
        return remote(ref, ref, near.at[slot, j], recv_near.at[slot, j], r, c)

    def near_copy_u(level, j, src=None):
        at = pl.ds(pl.multiple_of(j * hu, hu), hu)
        ref = ub_ref.at[level * 2 + k, at, :]
        return remote(ref if src is None else src, ref, near_u.at[level, j], recv_near_u.at[level, j],
                      z * 2 + 1 - k, c)

    def own_rows(j):
        return f_ref.at[pl.ds(pl.multiple_of(j * h, h), h), :]

    def own_rows_u(j):
        return u_ref.at[pl.ds(pl.multiple_of(j * hu, hu), hu), :]

    chips = [(a, b) for a in range(4) for b in range(4)]
    incoming = {chip_: [hop for hop in hops if hop[2] == chip_] for chip_ in chips}
    outgoing = {chip_: [] for chip_ in chips}
    count, count_u = {}, {}
    for hop in hops:
        counts = count_u if hop[0][0] == "u" else count
        number = counts.get(hop[1], 0)
        counts[hop[1]] = number + 1
        outgoing[hop[1]].append((hop, number))

    zeros[...] = jnp.zeros_like(zeros)

    def fill(slot, begin):
        def one(j, carry):
            for condition, columns in shapes((0, 0), j):
                if columns < width:
                    copy = pltpu.make_async_copy(
                        zeros.at[:, pl.ds(0, width - columns)],
                        x_ref.at[at_rows(slot, k, j), pl.ds(columns, width - columns)], local.at[1])

                    @pl.when(condition)
                    def _():
                        copy.start()
                        copy.wait()
            return carry
        lax.fori_loop(0, pieces, one, 0)

    def spread(j, carry):
        @pl.when(owner)
        def _():
            near_copy(z, j, own_rows(j)).start()
        return carry

    def spread_u(j, carry):
        near_copy_u(z, j, own_rows_u(j)).start()
        return carry

    def flip():
        slot = slots[1, 0][G]
        tile = min(256, width)

        def turned(i, carry):
            at = pl.ds(pl.multiple_of(i * tile, tile), tile)
            flipped[at, :] = acc[:, at].T.astype(flipped.dtype)
            return carry
        lax.fori_loop(0, width // tile, turned, 0)
        cols = pl.ds(pl.multiple_of(k * tall, tall), tall)
        kept = []
        for half in range(2):
            at = pl.ds((slot * 2 + half) * rows, rows)
            kept.append(pltpu.make_async_copy(flipped.at[pl.ds(half * rows, rows), :], x_ref.at[at, cols],
                                              local.at[half]))
        for copy in kept:
            copy.start()
        for copy in kept:
            copy.wait()
        at = pl.ds(pl.multiple_of((slot * 2 + 1 - k) * rows, rows), rows)
        pass_on = remote(x_ref.at[at, cols], x_ref.at[at, cols], turn.at[0], turn.at[1], z * 2 + 1 - k, c)
        pass_on.start()
        pass_on.wait_send()
        at = pl.ds(pl.multiple_of((slot * 2 + k) * rows, rows), rows)
        cols = pl.ds(pl.multiple_of((1 - k) * tall, tall), tall)
        remote(x_ref.at[at, cols], x_ref.at[at, cols], turn.at[0], turn.at[1], r, c).wait_recv()

    def step(t, carry):
        for place in chips:
            @pl.when(chip == place[0] * 4 + place[1])
            def _():
                for hop in incoming[place]:
                    block, p, q, first, last, t0 = hop

                    @pl.when((t >= t0 + LAG) & (t < t0 + LAG + last - first))
                    def _():
                        j = t - (t0 + LAG) + first
                        each(block, j, lambda columns: hop_copy(hop, 0, j, columns).wait_recv())
                        if block[0] == "u":
                            near_copy_u(block[1], j).start()
                        elif block in needs[place]:
                            near_copy(slots[place][block], j).start()
                for hop, number in outgoing[place]:
                    block, p, q, first, last, t0 = hop

                    @pl.when((t >= t0) & (t < t0 + last - first))
                    def _():
                        j = t - t0 + first
                        each(block, j, lambda columns: hop_copy(hop, number, j, columns).start())

        def consume(entry, carry):
            begin = jnp.int32(-1000)
            for index in range(16):
                begin = jnp.where(entry == index, begins[index], begin)
            m, part = entry // 4, lax.rem(entry, 4)
            past = t - begin

            @pl.when((past >= 0) & (past < pieces // 4) & (lax.rem(past, 2) == 0))
            def _():
                ago = past + part * (pieces // 4)
                slot_b = jnp.where(c == z, m, 4 + m)
                for i in range(2):
                    near_arrival(m, ago + i).wait_recv()

                    @pl.when(c != z)
                    def _():
                        near_arrival(slot_b, ago + i).wait_recv()
                loads = []
                cols = pl.ds(pl.multiple_of(k * tall, tall), tall)
                for core in range(2):
                    at_a = pl.ds(pl.multiple_of((m * 2 + core) * rows + ago * h, 2 * h), 2 * h)
                    at_b = pl.ds(pl.multiple_of((slot_b * 2 + core) * rows + ago * h, 2 * h), 2 * h)
                    into = pl.ds(core * 2 * h, 2 * h)
                    loads.append(pltpu.make_async_copy(x_ref.at[at_a, :], a_buf.at[into, :], local.at[2 + core]))
                    loads.append(pltpu.make_async_copy(x_ref.at[at_b, cols], b_buf.at[into, :], local.at[4 + core]))
                for copy in loads:
                    copy.start()
                for copy in loads:
                    copy.wait()
                tile = min(256, tall)

                def rows_of(i, carry):
                    at = pl.ds(pl.multiple_of(i * tile, tile), tile)
                    acc[at, :] += lax.dot_general(
                        b_buf[:, at], a_buf[...], (((0,), (0,)), ((), ())), preferred_element_type=jnp.float32)
                    return carry
                lax.fori_loop(0, tall // tile, rows_of, 0)
            return carry
        lax.fori_loop(0, 16, consume, 0)

        @pl.when((chip == 4) & (t == final))
        def _():
            flip()
        return carry

    begins = []
    for index in range(16):
        begin = jnp.int32(-1000)
        for place in chips:
            if (place, index // 4, index % 4) in due:
                begin = jnp.where(chip == place[0] * 4 + place[1], due[place, index // 4, index % 4], begin)
        begins.append(begin)

    lax.fori_loop(0, pieces, spread, 0)
    lax.fori_loop(0, coupling_pieces, spread_u, 0)
    own = pltpu.make_async_copy(f_ref, stage, local.at[0])
    keep = pltpu.make_async_copy(stage, x_ref.at[pl.ds(pl.multiple_of((z * 2 + k) * rows, rows), rows), :], local.at[0])

    own_u = pltpu.make_async_copy(u_ref, stage_u, local.at[1])
    keep_u = pltpu.make_async_copy(stage_u, ub_ref.at[r], local.at[1])

    @pl.when(owner)
    def _():
        own.start()
    acc[...] = jnp.zeros_like(acc)
    for place in chips:
        filled = [slots[place][b] for b in needs[place] if b[0] == b[1] and b != place]
        for slot in filled:
            @pl.when(chip == place[0] * 4 + place[1])
            def _():
                fill(slot, 0)

    @pl.when(owner)
    def _():
        own.wait()
        keep.start()
        keep.wait()
    own_u.start()
    own_u.wait()
    keep_u.start()
    keep_u.wait()
    lax.fori_loop(0, steps, step, 0)

    @pl.when(chip == 1)
    def _():
        at = pl.ds(pl.multiple_of((slots[0, 1][G] * 2 + k) * rows, rows), rows)
        load = pltpu.make_async_copy(x_ref.at[at, :], stage, local.at[0])
        load.start()
        load.wait()
        tile = min(128, tall)

        def widen(i, carry):
            at = pl.ds(pl.multiple_of(i * tile, tile), tile)
            acc[at, :] = stage[at, :].astype(jnp.float32)
            return carry
        lax.fori_loop(0, tall // tile, widen, 0)
    out = pltpu.make_async_copy(acc, g_ref, local.at[0])
    out.start()

    def settle(j, carry):
        @pl.when(owner)
        def _():
            near_copy(z, j, own_rows(j)).wait_send()
        return carry
    lax.fori_loop(0, pieces, settle, 0)

    def settle_u(j, carry):
        for level in range(4):
            near_copy_u(level, j).wait_send()
            at = pl.ds(pl.multiple_of(j * hu, hu), hu)
            ref = ub_ref.at[level * 2 + 1 - k, at, :]
            remote(ref, ref, near_u.at[level, j], recv_near_u.at[level, j], r, c).wait_recv()
        return carry
    lax.fori_loop(0, coupling_pieces, settle_u, 0)
    for place in chips:
        @pl.when(chip == place[0] * 4 + place[1])
        def _():
            for hop, number in outgoing[place]:
                def sent(j, carry):
                    each(hop[0], j, lambda columns: hop_copy(hop, number, j, columns).wait_send())
                    return carry
                lax.fori_loop(hop[3], hop[4], sent, 0)
            for hop in incoming[place]:
                if hop[0][0] != "u" and hop[0] in needs[place]:
                    def passed(j, carry):
                        near_copy(slots[place][hop[0]], j).wait_send()
                        return carry
                    lax.fori_loop(hop[3], hop[4], passed, 0)
    out.wait()


def stream(factor, coupling, n_row, n_col):
    rows, width = factor.shape
    depth, narrow = coupling.shape
    pieces, coupling_pieces = 16, 4
    hops = plan(pieces, coupling_pieces)[0]
    out_count = max(sum(hop[1] == chip and hop[0][0] != "u" for hop in hops) for chip in {h[1] for h in hops})
    out_count_u = max(sum(hop[1] == chip and hop[0][0] == "u" for hop in hops) for chip in {h[1] for h in hops})
    tall = width // 2
    h = rows // pieces
    dma = pltpu.SemaphoreType.DMA
    return pl.pallas_call(
        functools.partial(stream_kernel, pieces, coupling_pieces),
        out_shape=(
            jax.ShapeDtypeStruct((8 * 2 * rows, width), factor.dtype),
            jax.ShapeDtypeStruct((n_row, depth, narrow), coupling.dtype),
            jax.ShapeDtypeStruct((tall, width), jnp.float32),
        ),
        in_specs=[pl.BlockSpec(memory_space=pl.ANY)] * 2,
        out_specs=[pl.BlockSpec(memory_space=pl.ANY)] * 3,
        scratch_shapes=[
            dma((out_count, pieces)),
            dma((out_count_u, coupling_pieces)),
            dma((8, pieces)),
            dma((4, coupling_pieces)),
            dma((8, pieces)),
            dma((4, coupling_pieces)),
            dma((8, pieces)),
            dma((4, coupling_pieces)),
            dma((2,)),
            dma((6,)),
            pltpu.VMEM((tall, width), jnp.float32),
            pltpu.VMEM((4 * h, width), factor.dtype),
            pltpu.VMEM((4 * h, tall), factor.dtype),
            pltpu.VMEM((rows, width), factor.dtype),
            pltpu.VMEM((depth, narrow), coupling.dtype),
            pltpu.VMEM((h, width), factor.dtype),
            pltpu.VMEM((width, tall), factor.dtype),
        ],
        compiler_params=pltpu.CompilerParams(has_side_effects=True, vmem_limit_bytes=63 * 1024 * 1024),
        cost_estimate=pl.CostEstimate(flops=0, bytes_accessed=rows * width * 64, transcendentals=0),
    )(factor, coupling)


def finish_kernel(g_ref, u_ref, gram_ref, part_ref):
    gram_ref[...] = g_ref[...]
    rounded = g_ref[...].astype(u_ref.dtype)
    narrow = u_ref.shape[2]

    def one(i, carry):
        product = jnp.dot(rounded, u_ref[i], preferred_element_type=jnp.float32)
        part_ref[pl.ds(pl.multiple_of(i * narrow, narrow), narrow), :] = product.T.astype(part_ref.dtype)
        return carry
    lax.fori_loop(0, u_ref.shape[0], one, 0)


def finish(gram, coupling):
    tall, width = gram.shape
    count, depth, narrow = coupling.shape
    tile = min(256, tall)
    return pl.pallas_call(
        finish_kernel,
        grid=(tall // tile,),
        out_shape=(
            jax.ShapeDtypeStruct((tall, width), jnp.float32),
            jax.ShapeDtypeStruct((count * narrow, tall), coupling.dtype),
        ),
        in_specs=[
            pl.BlockSpec((tile, width), lambda i: (i, 0)),
            pl.BlockSpec((count, depth, narrow), lambda i: (0, 0, 0)),
        ],
        out_specs=(
            pl.BlockSpec((tile, width), lambda i: (i, 0)),
            pl.BlockSpec((count * narrow, tile), lambda i: (0, i)),
        ),
        compiler_params=pltpu.CompilerParams(vmem_limit_bytes=63 * 1024 * 1024),
        cost_estimate=pl.CostEstimate(
            flops=2 * tall * width * count * narrow, bytes_accessed=tall * width * 16, transcendentals=0),
    )(gram, coupling)


def exchange_kernel(n_col, part_ref, out_ref, send, recv):
    r, c = lax.axis_index("row"), lax.axis_index("col")
    depth = out_ref.shape[1]
    started = []
    for d in range(1, n_col):
        ct = lax.rem(c + d, n_col)
        copy = pltpu.make_async_remote_copy(
            src_ref=part_ref.at[pl.ds(pl.multiple_of(ct * depth, depth), depth), :],
            dst_ref=out_ref.at[d - 1],
            send_sem=send.at[d - 1],
            recv_sem=recv.at[d - 1],
            device_id=(r, ct),
            device_id_type=MESH,
        )
        copy.start()
        started.append(copy)
    for copy in started:
        copy.wait()


def exchange(part, n_col):
    total, width = part.shape
    dma = pltpu.SemaphoreType.DMA
    return pl.pallas_call(
        functools.partial(exchange_kernel, n_col),
        out_shape=jax.ShapeDtypeStruct((n_col - 1, total // n_col, width), part.dtype),
        in_specs=[pl.BlockSpec(memory_space=pl.ANY)],
        out_specs=pl.BlockSpec(memory_space=pl.ANY),
        scratch_shapes=[dma((n_col - 1,)), dma((n_col - 1,))],
        compiler_params=pltpu.CompilerParams(has_side_effects=True),
    )(part)


def general(n_row, n_col, factor, coupling):
    rows_here = factor.shape[0]
    row_index, col_index = lax.axis_index("row"), lax.axis_index("col")
    cores = n_row // n_col
    below, partner = gather(factor, n_row, n_col)
    coupling_full = lax.all_gather(coupling, "row", axis=1, tiled=True)

    def product(level, below, partner):
        first = level * rows_here * cores
        return lax.dot_general(
            partner[first:], below[first:], (((0,), (0,)), ((), ())), preferred_element_type=jnp.float32
        )

    gram = lax.switch(
        jnp.maximum(row_index // cores, col_index),
        [functools.partial(product, level) for level in range(n_col)],
        below,
        partner,
    )
    rounded = gram.astype(jnp.bfloat16)
    part = lax.dot_general(
        coupling_full, rounded, (((0,), (1,)), ((), ())), preferred_element_type=jnp.float32
    ).astype(jnp.bfloat16)
    return gram, part


def body(n_row, n_col, factor, sel_tiles, coupling):
    rows_here = factor.shape[0]
    row_index, col_index = lax.axis_index("row"), lax.axis_index("col")
    cores = n_row // n_col
    if (n_row, n_col) == (8, 4):
        _, pieces, gram = stream(factor, coupling, n_row, n_col)
        gram, part = finish(gram, pieces)
    else:
        gram, part = general(n_row, n_col, factor, coupling)
    global_rows = row_index * rows_here + jnp.arange(rows_here, dtype=jnp.int32)
    member = jnp.any((global_rows // TILE)[:, None] == sel_tiles[None, :], axis=1)
    depth = part.shape[0] // n_col
    arrived = exchange(part, n_col)
    summed = lax.dynamic_slice_in_dim(part, col_index * depth, depth, 0).astype(jnp.float32)
    for d in range(n_col - 1):
        summed = summed + arrived[d].astype(jnp.float32)
    child = jnp.where(member[None, :], -summed, jnp.float32(0.0))
    return (gram, child)


def solution(mesh):
    placed = (P("row", "col"), P(), P("col", "row"))
    return jax.shard_map(
        functools.partial(body, mesh.shape["row"], mesh.shape["col"]),
        mesh=mesh,
        in_specs=placed,
        out_specs=(P("row", "col"), P("col", "row")),
        check_vma=False,
    )
```

```python
import functools
import math

import jax
import jax.numpy as jnp
from jax import lax
from jax.experimental import pallas as pl
from jax.experimental.pallas import tpu as pltpu
from jax.sharding import PartitionSpec as P

TILE = 128
MESH = pl.DeviceIdType.MESH
SKEW = 2


def gather_kernel(dims, f_ref, a_ref, b_ref, recv_a, recv_b, send_z, send_p, send_b, send_f, local_a, stage):
    levels, wide, high, cores, chunks = dims
    rows, width = f_ref.shape
    narrow = width // cores
    h = rows // chunks
    r, c = lax.axis_index("row"), lax.axis_index("col")
    k, z = lax.rem(r, cores), r // cores
    x, y = lax.rem(c, wide), c // wide
    x0, y0 = lax.rem(z, wide), z // wide
    source = c == z

    def chunk_rows(block, j):
        return pl.ds(pl.multiple_of(block * rows + j * h, h), h)

    def remote(src, dst, send, recv, row, col):
        return pltpu.make_async_remote_copy(
            src_ref=src, dst_ref=dst, send_sem=send, recv_sem=recv,
            device_id=(row, col), device_id_type=MESH,
        )

    def copies(t, j):
        m = z + t
        inside = m < levels
        has = inside & (m >= c)
        block = m * cores + k
        at = chunk_rows(block, j)
        if t == 0:
            def src(cols):
                return f_ref.at[pl.ds(j * h, h), cols]
        else:
            def src(cols):
                return a_ref.at[at, cols]
        everything = pl.ds(0, width)
        found = []
        for kk in range(cores):
            piece = src(pl.ds(kk * narrow, narrow))
            into = b_ref.at[at, :]
            for dx in range(1, wide):
                xt = lax.rem(x + dx, wide)
                found.append((
                    source & inside & (m >= y * wide + xt),
                    remote(piece, into, send_b.at[kk, dx, t, j], recv_b.at[block, j],
                           z * cores + kk, y * wide + xt),
                    False,
                ))
            for dy in range(1, high):
                yt = lax.rem(y + dy, high)
                found.append((
                    source & inside & (m >= yt * wide),
                    remote(piece, into, send_b.at[kk, wide - 1 + dy, t, j], recv_b.at[block, j],
                           z * cores + kk, yt * wide + x),
                    False,
                ))
        found.append((
            has & (z > 0),
            remote(src(everything), a_ref.at[at, :], send_z.at[t, j], recv_a.at[block, j],
                   r - cores, c),
            False,
        ))
        for dk in range(1, cores):
            other = z * cores + lax.rem(k + dk, cores)
            found.append((
                has,
                remote(src(everything), a_ref.at[at, :], send_p.at[dk, t, j], recv_a.at[block, j], other, c),
                False,
            ))
        for kk in range(cores):
            piece = src(pl.ds(kk * narrow, narrow))
            into = b_ref.at[at, :]
            found.append((
                source & inside & (k != kk),
                remote(piece, into, send_b.at[kk, 0, t, j], recv_b.at[block, j], z * cores + kk, c),
                False,
            ))
        return found

    def keep(t, j):
        m = z + t
        at = chunk_rows(m * cores + k, j)
        here = f_ref.at[pl.ds(j * h, h), :] if t == 0 else a_ref.at[at, :]
        inside = (m < levels) & (m >= c)

        @pl.when(inside if t == 0 else inside & source)
        def _():
            load = pltpu.make_async_copy(here, stage, local_a.at[0])
            load.start()
            load.wait()
            if t == 0:
                pltpu.make_async_copy(stage, a_ref.at[at, :], local_a.at[1]).start()
            for kk in range(cores):
                @pl.when(source & (k == kk))
                def _():
                    store = pltpu.make_async_copy(
                        stage.at[:, pl.ds(kk * narrow, narrow)], b_ref.at[at, :], local_a.at[2]
                    )
                    store.start()
                    store.wait()
            if t == 0:
                pltpu.make_async_copy(stage, a_ref.at[at, :], local_a.at[1]).wait()

    def forwards(t, j, p):
        m = z + t
        block = m * cores + p
        part = b_ref.at[chunk_rows(block, j), :]
        mine = (x == x0) & (y != y0) & (m < levels)
        found = []
        for dx in range(1, wide):
            xt = lax.rem(x + dx, wide)
            found.append((
                mine & (m >= y * wide + xt),
                remote(part, part, send_f.at[dx, p, t, j], recv_b.at[block, j], r, y * wide + xt),
            ))
        return mine & (m >= y * wide), found

    def arrived(ref, sem):
        remote(ref, ref, send_z.at[0, 0], sem, r, c).wait_recv()

    def step(t, j):
        m = z + t
        block = m * cores + k
        if t > 0:
            @pl.when((m < levels) & (m >= c))
            def _():
                arrived(a_ref.at[chunk_rows(block, j), :], recv_a.at[block, j])
        for condition, copy, _ in copies(t, j):
            pl.when(condition)(copy.start)
        keep(t, j)

    def forward(t, j):
        for p in range(cores):
            due, found = forwards(t, j, p)
            block = (z + t) * cores + p

            @pl.when(due)
            def _():
                arrived(b_ref.at[chunk_rows(block, j), :], recv_b.at[block, j])
            for condition, copy in found:
                pl.when(condition)(copy.start)

    order = [(t, j) for t in range(levels) for j in range(chunks)]
    for n, (t, j) in enumerate(order):
        step(t, j)
        if n >= SKEW:
            forward(*order[n - SKEW])
    for t, j in order[len(order) - SKEW:]:
        forward(t, j)

    for t, j in order:
        m = z + t
        inside = m < levels
        for dk in range(1, cores):
            block = m * cores + lax.rem(k + dk, cores)

            @pl.when(inside & (m >= c))
            def _():
                arrived(a_ref.at[chunk_rows(block, j), :], recv_a.at[block, j])

            @pl.when(inside & source)
            def _():
                arrived(b_ref.at[chunk_rows(block, j), :], recv_b.at[block, j])
        for p in range(cores):
            block = m * cores + p

            @pl.when(inside & (x != x0) & (m >= c))
            def _():
                arrived(b_ref.at[chunk_rows(block, j), :], recv_b.at[block, j])
        for condition, copy, local in copies(t, j):
            pl.when(condition)(copy.wait if local else copy.wait_send)
        for p in range(cores):
            for condition, copy in forwards(t, j, p)[1]:
                pl.when(condition)(copy.wait_send)


def gather(factor, n_row, n_col):
    rows, width = factor.shape
    cores = n_row // n_col
    wide = next(w for w in range(math.isqrt(n_col), 0, -1) if n_col % w == 0)
    high = n_col // wide
    levels = n_col
    chunks = max(1, 32 // n_row)
    dma = pltpu.SemaphoreType.DMA
    whole = rows * n_row
    return pl.pallas_call(
        functools.partial(gather_kernel, (levels, wide, high, cores, chunks)),
        out_shape=(
            jax.ShapeDtypeStruct((whole, width), factor.dtype),
            jax.ShapeDtypeStruct((whole, width // cores), factor.dtype),
        ),
        in_specs=[pl.BlockSpec(memory_space=pl.ANY)],
        out_specs=(pl.BlockSpec(memory_space=pl.ANY), pl.BlockSpec(memory_space=pl.ANY)),
        scratch_shapes=[
            dma((n_row, chunks)),
            dma((n_row, chunks)),
            dma((levels, chunks)),
            dma((cores, levels, chunks)),
            dma((cores, wide + high, levels, chunks)),
            dma((wide, cores, levels, chunks)),
            dma((3,)),
            pltpu.VMEM((rows // chunks, width), factor.dtype),
        ],
        compiler_params=pltpu.CompilerParams(has_side_effects=True),
        cost_estimate=pl.CostEstimate(flops=0, bytes_accessed=whole * width * 32, transcendentals=0),
    )(factor)


LAG = 2
G = ("g", 1, 0)


def block_flows(pieces):
    half = pieces // 2
    found = []

    def add(block, source, hops, first=0, last=pieces):
        found.append((block, source, hops, first, last))

    add((3, 3), (3, 3), [((3, 3), (2, 3)), ((2, 3), (1, 3)), ((1, 3), (0, 3)), ((3, 3), (3, 1)), ((3, 3), (3, 2)),
                         ((3, 2), (3, 0))])
    add((3, 2), (3, 2), [((3, 2), (2, 2)), ((2, 2), (2, 3)), ((2, 3), (2, 1)), ((2, 2), (2, 0)), ((2, 2), (1, 2)),
                         ((1, 2), (0, 2))])
    add((3, 1), (3, 1), [((3, 1), (2, 1)), ((2, 1), (2, 0)), ((2, 0), (1, 0)), ((1, 0), (1, 1)), ((1, 1), (1, 3)),
                         ((1, 3), (1, 2))], 0, half)
    add((3, 1), (3, 1), [((3, 1), (2, 1)), ((2, 1), (1, 1)), ((1, 1), (1, 3)), ((1, 3), (1, 2)), ((1, 2), (1, 0))],
        half, pieces)
    add((3, 0), (3, 0), [((3, 0), (2, 0)), ((2, 0), (2, 1)), ((2, 1), (2, 3)), ((2, 3), (1, 3)), ((1, 3), (1, 2)),
                         ((1, 2), (1, 0)), ((1, 3), (0, 3)), ((0, 3), (0, 2)), ((0, 2), (0, 0))])
    add((2, 0), (2, 0), [((2, 0), (1, 0)), ((1, 0), (1, 1)), ((1, 1), (0, 1)), ((0, 1), (0, 0)), ((0, 0), (0, 2))])
    add((1, 0), (1, 0), [((1, 0), (0, 0))])
    add((2, 1), (2, 1), [((2, 1), (1, 1)), ((1, 1), (1, 0)), ((1, 0), (1, 2))])
    add((1, 1), (1, 1), [((1, 1), (1, 0))])
    add((2, 2), (2, 2), [((2, 2), (2, 3)), ((2, 3), (2, 1)), ((2, 2), (2, 0)), ((2, 2), (1, 2)), ((1, 2), (0, 2))])
    add(G, (1, 0), [((1, 0), (0, 0)), ((0, 0), (0, 1))], 0, half)
    add(G, (1, 0), [((1, 0), (1, 1)), ((1, 1), (0, 1))], half, pieces)
    return found


def coupling_flows(pieces):
    found = []
    for c in range(4):
        for z in range(4):
            hops = [((a, c), (a - 1, c)) for a in range(z, 0, -1)] + [((a, c), (a + 1, c)) for a in range(z, 3)]
            found.append((("u", z, c), (z, c), hops, 0, pieces))
    return found


ORDER = [3, 4, 19, 12, 0, 20, 23, 22, 21, 5, 25, 2, 13, 6, 16, 26, 27, 24, 1, 7, 18, 15, 17, 8, 9, 14, 10, 11]


@functools.cache
def plan(pieces, coupling_pieces):
    flows = block_flows(pieces) + coupling_flows(coupling_pieces)
    chips = [(z, c) for z in range(4) for c in range(4)]
    pairs = [(chip, m) for chip in chips if chip != (0, 1) for m in range(max(chip), 4)]
    busy, hops, due = {}, [], {}
    final = None
    for index in ORDER:
        block, source, route, first, last = flows[index]
        if block == G and final is None:
            due = ready_steps(pieces, hops, pairs)
            final = max(d for key, d in due.items() if key[0] == (1, 0)) + pieces // 4
        n, at = last - first, {source: final + 1 if block == G else 0}
        for p, q in route:
            t, used = at[p], busy.setdefault((p, q), [])
            while any(t < e and s < t + n for s, e in used):
                t += 1
            used.append((t, t + n))
            at[q] = t + LAG
            hops.append((block, p, q, first, last, t))
    slots = {chip: {} for chip in chips}
    needs = {chip: set() for chip in chips}
    for chip, m in pairs:
        z, c = chip
        slots[chip][m, c] = m
        needs[chip].add((m, c))
        if c != z:
            slots[chip][m, z] = 4 + m
            needs[chip].add((m, z))
    for block, p, q, first, last, t in hops:
        for chip in (p, q):
            if block[0] != "u" and block not in slots[chip] and block != chip:
                slots[chip][block] = min(set(range(8)) - set(slots[chip].values()))
    steps = max([t + last - first + LAG for block, p, q, first, last, t in hops] + [d + pieces // 4 for d in due.values()] + [final + 1])
    return hops, slots, needs, due, steps, final


def ready_steps(pieces, hops, pairs):
    due, group = {}, pieces // 8
    for chip, m in pairs:
        z, c = chip
        ready = {(z, c): [1] * pieces}
        for block, p, q, first, last, t in hops:
            if q == chip:
                for j in range(first, last):
                    ready.setdefault(block, [None] * pieces)[j] = t + LAG + j - first
        both = [ready[m, c], ready[m, z]]
        for part in range(4):
            begin = part * (pieces // 4)
            due[chip, m, part] = 1 + max(b[begin + j] - j // group * group for b in both for j in range(pieces // 4))
    return due


def stream_kernel(pieces, coupling_pieces, f_ref, u_ref, x_ref, ub_ref, g_ref, send, send_u, near, near_u, recv,
                  recv_u, recv_near, recv_near_u, turn, blank, local, acc, a_buf, b_buf, stage, stage_u, zeros, flipped):
    hops, slots, needs, due, steps, final = plan(pieces, coupling_pieces)
    rows, width = f_ref.shape
    depth, narrow = u_ref.shape
    h, hu, quarter = rows // pieces, depth // coupling_pieces, width // 4
    tall = acc.shape[0]
    r, c = lax.axis_index("row"), lax.axis_index("col")
    k, z = lax.rem(r, 2), r // 2
    chip = z * 4 + c
    owner = z >= c

    def at_rows(slot, core, j):
        return pl.ds(pl.multiple_of((slot * 2 + core) * rows + j * h, h), h)

    def remote(src, dst, send_sem, recv_sem, row, col):
        return pltpu.make_async_remote_copy(
            src_ref=src, dst_ref=dst, send_sem=send_sem, recv_sem=recv_sem,
            device_id=(row, col), device_id_type=MESH,
        )

    def shapes(block, j):
        if block[0] != block[1]:
            return [(None, width)]
        part = (k * pieces + j) // (pieces // 2)
        return [(part == q, (q + 1) * quarter) for q in range(4)]

    def each(block, j, act):
        if block[0] == "u":
            act(None)
            return
        for condition, columns in shapes(block, j):
            if condition is None:
                act(columns)
            else:
                pl.when(condition)(functools.partial(act, columns))

    def hop_copy(hop, number, j, columns):
        block, p, q, first, last, t = hop
        if block[0] == "u":
            at = pl.ds(pl.multiple_of(j * hu, hu), hu)
            src = u_ref.at[at, :] if p == block[1:] else ub_ref.at[block[1] * 2 + k, at, :]
            return remote(src, ub_ref.at[block[1] * 2 + k, at, :], send_u.at[number, j], recv_u.at[block[1], j],
                          q[0] * 2 + k, q[1])
        cols = pl.ds(0, columns)
        if p == block:
            src = f_ref.at[pl.ds(pl.multiple_of(j * h, h), h), cols]
        else:
            src = x_ref.at[at_rows(slots[p][block], k, j), cols]
        slot = slots[q][block]
        return remote(src, x_ref.at[at_rows(slot, k, j), cols], send.at[number, j], recv.at[slot, j],
                      q[0] * 2 + k, q[1])

    def near_copy(slot, j, src=None):
        at = at_rows(slot, k, j)
        return remote(x_ref.at[at, :] if src is None else src, x_ref.at[at, :], near.at[slot, j],
                      recv_near.at[slot, j], z * 2 + 1 - k, c)

    def near_arrival(slot, j):
        ref = x_ref.at[at_rows(slot, 1 - k, j), :]
        return remote(ref, ref, near.at[slot, j], recv_near.at[slot, j], r, c)

    def near_copy_u(level, j, src=None):
        at = pl.ds(pl.multiple_of(j * hu, hu), hu)
        ref = ub_ref.at[level * 2 + k, at, :]
        return remote(ref if src is None else src, ref, near_u.at[level, j], recv_near_u.at[level, j],
                      z * 2 + 1 - k, c)

    def own_rows(j):
        return f_ref.at[pl.ds(pl.multiple_of(j * h, h), h), :]

    def own_rows_u(j):
        return u_ref.at[pl.ds(pl.multiple_of(j * hu, hu), hu), :]

    chips = [(a, b) for a in range(4) for b in range(4)]
    incoming = {chip_: [hop for hop in hops if hop[2] == chip_] for chip_ in chips}
    outgoing = {chip_: [] for chip_ in chips}
    count, count_u = {}, {}
    for hop in hops:
        counts = count_u if hop[0][0] == "u" else count
        number = counts.get(hop[1], 0)
        counts[hop[1]] = number + 1
        outgoing[hop[1]].append((hop, number))

    zeros[...] = jnp.zeros_like(zeros)

    def fill(slot, act):
        def one(j, carry):
            for condition, columns in shapes((0, 0), j):
                if columns < width:
                    @pl.when(condition)
                    def _():
                        act(pltpu.make_async_copy(
                            zeros.at[:, pl.ds(0, width - columns)],
                            x_ref.at[at_rows(slot, k, j), pl.ds(columns, width - columns)], blank.at[j]))
            return carry
        lax.fori_loop(0, pieces, one, 0)

    def fill_all(act):
        for place in chips:
            for block in needs[place]:
                if block[0] == block[1] and block != place:
                    pl.when(chip == place[0] * 4 + place[1])(functools.partial(fill, slots[place][block], act))

    def spread(j, carry):
        @pl.when(owner)
        def _():
            near_copy(z, j, own_rows(j)).start()
        return carry

    def spread_u(j, carry):
        near_copy_u(z, j, own_rows_u(j)).start()
        return carry

    def loads(m, slot_b, ago, into):
        cols = pl.ds(pl.multiple_of(k * tall, tall), tall)
        found = []
        for core in range(2):
            at_a = pl.ds(pl.multiple_of((m * 2 + core) * rows + ago * h, 2 * h), 2 * h)
            at_b = pl.ds(pl.multiple_of((slot_b * 2 + core) * rows + ago * h, 2 * h), 2 * h)
            half = pl.ds(core * 2 * h, 2 * h)
            found.append(pltpu.make_async_copy(x_ref.at[at_a, :], a_buf.at[into, half, :], local.at[2 + into * 4 + core]))
            found.append(pltpu.make_async_copy(x_ref.at[at_b, cols], b_buf.at[into, half, :], local.at[4 + into * 4 + core]))
        return found

    def multiply(into):
        for copy in loads(0, 0, 0, into):
            copy.wait()
        tile = min(256, tall)

        def rows_of(i, carry):
            at = pl.ds(pl.multiple_of(i * tile, tile), tile)
            acc[at, :] += lax.dot_general(
                b_buf[into, :, at], a_buf[into], (((0,), (0,)), ((), ())), preferred_element_type=jnp.float32)
            return carry
        lax.fori_loop(0, tall // tile, rows_of, 0)

    def flip():
        slot = slots[1, 0][G]
        tile = min(256, width)

        def turned(i, carry):
            at = pl.ds(pl.multiple_of(i * tile, tile), tile)
            flipped[at, :] = acc[:, at].T.astype(flipped.dtype)
            return carry
        lax.fori_loop(0, width // tile, turned, 0)
        cols = pl.ds(pl.multiple_of(k * tall, tall), tall)
        kept = []
        for half in range(2):
            at = pl.ds((slot * 2 + half) * rows, rows)
            kept.append(pltpu.make_async_copy(flipped.at[pl.ds(half * rows, rows), :], x_ref.at[at, cols],
                                              local.at[half]))
        for copy in kept:
            copy.start()
        for copy in kept:
            copy.wait()
        at = pl.ds(pl.multiple_of((slot * 2 + 1 - k) * rows, rows), rows)
        pass_on = remote(x_ref.at[at, cols], x_ref.at[at, cols], turn.at[0], turn.at[1], z * 2 + 1 - k, c)
        pass_on.start()
        pass_on.wait_send()
        at = pl.ds(pl.multiple_of((slot * 2 + k) * rows, rows), rows)
        cols = pl.ds(pl.multiple_of((1 - k) * tall, tall), tall)
        remote(x_ref.at[at, cols], x_ref.at[at, cols], turn.at[0], turn.at[1], r, c).wait_recv()

    def step(t, carry):
        for place in chips:
            @pl.when(chip == place[0] * 4 + place[1])
            def _():
                for hop in incoming[place]:
                    block, p, q, first, last, t0 = hop

                    @pl.when((t >= t0 + LAG) & (t < t0 + LAG + last - first))
                    def _():
                        j = t - (t0 + LAG) + first
                        each(block, j, lambda columns: hop_copy(hop, 0, j, columns).wait_recv())
                        if block[0] == "u":
                            near_copy_u(block[1], j).start()
                        elif block in needs[place]:
                            near_copy(slots[place][block], j).start()
                for hop, number in outgoing[place]:
                    block, p, q, first, last, t0 = hop

                    @pl.when((t >= t0) & (t < t0 + last - first))
                    def _():
                        j = t - t0 + first
                        each(block, j, lambda columns: hop_copy(hop, number, j, columns).start())

        def consume(entry, carry):
            pending, into = carry
            begin = jnp.int32(-1000)
            for index in range(16):
                begin = jnp.where(entry == index, begins[index], begin)
            m, part = entry // 4, lax.rem(entry, 4)
            past = t - begin
            ready = (past >= 0) & (past < pieces // 4) & (lax.rem(past, 2) == 0)

            @pl.when(ready)
            def _():
                ago = past + part * (pieces // 4)
                slot_b = jnp.where(c == z, m, 4 + m)
                for i in range(2):
                    near_arrival(m, ago + i).wait_recv()

                    @pl.when(c != z)
                    def _():
                        near_arrival(slot_b, ago + i).wait_recv()
                for copy in loads(m, slot_b, ago, 1 - into):
                    copy.start()
                pl.when(pending == 1)(functools.partial(multiply, into))
            return jnp.where(ready, 1, pending), jnp.where(ready, 1 - into, into)
        pending, into = lax.fori_loop(0, 16, consume, carry)
        last = (chip == 4) & (t == final)

        @pl.when(last)
        def _():
            pl.when(pending == 1)(functools.partial(multiply, into))
            flip()
        return jnp.where(last, 0, pending), into

    begins = []
    for index in range(16):
        begin = jnp.int32(-1000)
        for place in chips:
            if (place, index // 4, index % 4) in due:
                begin = jnp.where(chip == place[0] * 4 + place[1], due[place, index // 4, index % 4], begin)
        begins.append(begin)

    own = pltpu.make_async_copy(f_ref, stage, local.at[0])
    keep = pltpu.make_async_copy(stage, x_ref.at[pl.ds(pl.multiple_of((z * 2 + k) * rows, rows), rows), :], local.at[0])
    own_u = pltpu.make_async_copy(u_ref, stage_u, local.at[1])
    keep_u = pltpu.make_async_copy(stage_u, ub_ref.at[r], local.at[1])
    pl.when(owner)(own.start)
    own_u.start()
    lax.fori_loop(0, pieces, spread, 0)
    lax.fori_loop(0, coupling_pieces, spread_u, 0)
    fill_all(lambda copy: copy.start())
    acc[...] = jnp.zeros_like(acc)

    @pl.when(owner)
    def _():
        own.wait()
        keep.start()
    own_u.wait()
    keep_u.start()
    fill_all(lambda copy: copy.wait())
    pl.when(owner)(keep.wait)
    keep_u.wait()
    pending, turned_to = lax.fori_loop(0, steps, step, (jnp.int32(0), jnp.int32(0)))
    pl.when(pending == 1)(functools.partial(multiply, turned_to))

    @pl.when(chip == 1)
    def _():
        at = pl.ds(pl.multiple_of((slots[0, 1][G] * 2 + k) * rows, rows), rows)
        load = pltpu.make_async_copy(x_ref.at[at, :], stage, local.at[0])
        load.start()
        load.wait()
        tile = min(128, tall)

        def widen(i, carry):
            at = pl.ds(pl.multiple_of(i * tile, tile), tile)
            acc[at, :] = stage[at, :].astype(jnp.float32)
            return carry
        lax.fori_loop(0, tall // tile, widen, 0)
    out = pltpu.make_async_copy(acc, g_ref, local.at[0])
    out.start()

    def settle(j, carry):
        @pl.when(owner)
        def _():
            near_copy(z, j, own_rows(j)).wait_send()
        return carry
    lax.fori_loop(0, pieces, settle, 0)

    def settle_u(j, carry):
        for level in range(4):
            near_copy_u(level, j).wait_send()
            at = pl.ds(pl.multiple_of(j * hu, hu), hu)
            ref = ub_ref.at[level * 2 + 1 - k, at, :]
            remote(ref, ref, near_u.at[level, j], recv_near_u.at[level, j], r, c).wait_recv()
        return carry
    lax.fori_loop(0, coupling_pieces, settle_u, 0)
    for place in chips:
        @pl.when(chip == place[0] * 4 + place[1])
        def _():
            for hop, number in outgoing[place]:
                def sent(j, carry):
                    each(hop[0], j, lambda columns: hop_copy(hop, number, j, columns).wait_send())
                    return carry
                lax.fori_loop(hop[3], hop[4], sent, 0)
            for hop in incoming[place]:
                if hop[0][0] != "u" and hop[0] in needs[place]:
                    def passed(j, carry):
                        near_copy(slots[place][hop[0]], j).wait_send()
                        return carry
                    lax.fori_loop(hop[3], hop[4], passed, 0)
    out.wait()


def stream(factor, coupling, n_row, n_col):
    rows, width = factor.shape
    depth, narrow = coupling.shape
    pieces, coupling_pieces = 16, 4
    hops = plan(pieces, coupling_pieces)[0]
    out_count = max(sum(hop[1] == chip and hop[0][0] != "u" for hop in hops) for chip in {h[1] for h in hops})
    out_count_u = max(sum(hop[1] == chip and hop[0][0] == "u" for hop in hops) for chip in {h[1] for h in hops})
    tall = width // 2
    h = rows // pieces
    dma = pltpu.SemaphoreType.DMA
    return pl.pallas_call(
        functools.partial(stream_kernel, pieces, coupling_pieces),
        out_shape=(
            jax.ShapeDtypeStruct((8 * 2 * rows, width), factor.dtype),
            jax.ShapeDtypeStruct((n_row, depth, narrow), coupling.dtype),
            jax.ShapeDtypeStruct((tall, width), jnp.float32),
        ),
        in_specs=[pl.BlockSpec(memory_space=pl.ANY)] * 2,
        out_specs=[pl.BlockSpec(memory_space=pl.ANY)] * 3,
        scratch_shapes=[
            dma((out_count, pieces)),
            dma((out_count_u, coupling_pieces)),
            dma((8, pieces)),
            dma((4, coupling_pieces)),
            dma((8, pieces)),
            dma((4, coupling_pieces)),
            dma((8, pieces)),
            dma((4, coupling_pieces)),
            dma((2,)),
            dma((pieces,)),
            dma((12,)),
            pltpu.VMEM((tall, width), jnp.float32),
            pltpu.VMEM((2, 4 * h, width), factor.dtype),
            pltpu.VMEM((2, 4 * h, tall), factor.dtype),
            pltpu.VMEM((rows, width), factor.dtype),
            pltpu.VMEM((depth, narrow), coupling.dtype),
            pltpu.VMEM((h, width), factor.dtype),
            pltpu.VMEM((width, tall), factor.dtype),
        ],
        compiler_params=pltpu.CompilerParams(has_side_effects=True, vmem_limit_bytes=63 * 1024 * 1024),
        cost_estimate=pl.CostEstimate(flops=0, bytes_accessed=rows * width * 64, transcendentals=0),
    )(factor, coupling)


def finish_kernel(g_ref, u_ref, gram_ref, part_ref):
    gram_ref[...] = g_ref[...]
    rounded = g_ref[...].astype(u_ref.dtype)
    narrow = u_ref.shape[2]

    def one(i, carry):
        product = jnp.dot(rounded, u_ref[i], preferred_element_type=jnp.float32)
        part_ref[pl.ds(pl.multiple_of(i * narrow, narrow), narrow), :] = product.T.astype(part_ref.dtype)
        return carry
    lax.fori_loop(0, u_ref.shape[0], one, 0)


def finish(gram, coupling):
    tall, width = gram.shape
    count, depth, narrow = coupling.shape
    tile = min(256, tall)
    return pl.pallas_call(
        finish_kernel,
        grid=(tall // tile,),
        out_shape=(
            jax.ShapeDtypeStruct((tall, width), jnp.float32),
            jax.ShapeDtypeStruct((count * narrow, tall), coupling.dtype),
        ),
        in_specs=[
            pl.BlockSpec((tile, width), lambda i: (i, 0)),
            pl.BlockSpec((count, depth, narrow), lambda i: (0, 0, 0)),
        ],
        out_specs=(
            pl.BlockSpec((tile, width), lambda i: (i, 0)),
            pl.BlockSpec((count * narrow, tile), lambda i: (0, i)),
        ),
        compiler_params=pltpu.CompilerParams(vmem_limit_bytes=63 * 1024 * 1024),
        cost_estimate=pl.CostEstimate(
            flops=2 * tall * width * count * narrow, bytes_accessed=tall * width * 16, transcendentals=0),
    )(gram, coupling)


def exchange_kernel(n_col, part_ref, out_ref, send, recv):
    r, c = lax.axis_index("row"), lax.axis_index("col")
    depth = out_ref.shape[1]
    started = []
    for d in range(1, n_col):
        ct = lax.rem(c + d, n_col)
        copy = pltpu.make_async_remote_copy(
            src_ref=part_ref.at[pl.ds(pl.multiple_of(ct * depth, depth), depth), :],
            dst_ref=out_ref.at[d - 1],
            send_sem=send.at[d - 1],
            recv_sem=recv.at[d - 1],
            device_id=(r, ct),
            device_id_type=MESH,
        )
        copy.start()
        started.append(copy)
    for copy in started:
        copy.wait()


def exchange(part, n_col):
    total, width = part.shape
    dma = pltpu.SemaphoreType.DMA
    return pl.pallas_call(
        functools.partial(exchange_kernel, n_col),
        out_shape=jax.ShapeDtypeStruct((n_col - 1, total // n_col, width), part.dtype),
        in_specs=[pl.BlockSpec(memory_space=pl.ANY)],
        out_specs=pl.BlockSpec(memory_space=pl.ANY),
        scratch_shapes=[dma((n_col - 1,)), dma((n_col - 1,))],
        compiler_params=pltpu.CompilerParams(has_side_effects=True),
    )(part)


def general(n_row, n_col, factor, coupling):
    rows_here = factor.shape[0]
    row_index, col_index = lax.axis_index("row"), lax.axis_index("col")
    cores = n_row // n_col
    below, partner = gather(factor, n_row, n_col)
    coupling_full = lax.all_gather(coupling, "row", axis=1, tiled=True)

    def product(level, below, partner):
        first = level * rows_here * cores
        return lax.dot_general(
            partner[first:], below[first:], (((0,), (0,)), ((), ())), preferred_element_type=jnp.float32
        )

    gram = lax.switch(
        jnp.maximum(row_index // cores, col_index),
        [functools.partial(product, level) for level in range(n_col)],
        below,
        partner,
    )
    rounded = gram.astype(jnp.bfloat16)
    part = lax.dot_general(
        coupling_full, rounded, (((0,), (1,)), ((), ())), preferred_element_type=jnp.float32
    ).astype(jnp.bfloat16)
    return gram, part


def body(n_row, n_col, factor, sel_tiles, coupling):
    rows_here = factor.shape[0]
    row_index, col_index = lax.axis_index("row"), lax.axis_index("col")
    cores = n_row // n_col
    if (n_row, n_col) == (8, 4):
        _, pieces, gram = stream(factor, coupling, n_row, n_col)
        gram, part = finish(gram, pieces)
    else:
        gram, part = general(n_row, n_col, factor, coupling)
    global_rows = row_index * rows_here + jnp.arange(rows_here, dtype=jnp.int32)
    member = jnp.any((global_rows // TILE)[:, None] == sel_tiles[None, :], axis=1)
    depth = part.shape[0] // n_col
    arrived = exchange(part, n_col)
    summed = lax.dynamic_slice_in_dim(part, col_index * depth, depth, 0).astype(jnp.float32)
    for d in range(n_col - 1):
        summed = summed + arrived[d].astype(jnp.float32)
    child = jnp.where(member[None, :], -summed, jnp.float32(0.0))
    return (gram, child)


def solution(mesh):
    placed = (P("row", "col"), P(), P("col", "row"))
    return jax.shard_map(
        functools.partial(body, mesh.shape["row"], mesh.shape["col"]),
        mesh=mesh,
        in_specs=placed,
        out_specs=(P("row", "col"), P("col", "row")),
        check_vma=False,
    )
```

```python
import functools
import math

import jax
import jax.numpy as jnp
from jax import lax
from jax.experimental import pallas as pl
from jax.experimental.pallas import tpu as pltpu
from jax.sharding import PartitionSpec as P

TILE = 128
MESH = pl.DeviceIdType.MESH
SKEW = 2


def gather_kernel(dims, f_ref, a_ref, b_ref, recv_a, recv_b, send_z, send_p, send_b, send_f, local_a, stage):
    levels, wide, high, cores, chunks = dims
    rows, width = f_ref.shape
    narrow = width // cores
    h = rows // chunks
    r, c = lax.axis_index("row"), lax.axis_index("col")
    k, z = lax.rem(r, cores), r // cores
    x, y = lax.rem(c, wide), c // wide
    x0, y0 = lax.rem(z, wide), z // wide
    source = c == z

    def chunk_rows(block, j):
        return pl.ds(pl.multiple_of(block * rows + j * h, h), h)

    def remote(src, dst, send, recv, row, col):
        return pltpu.make_async_remote_copy(
            src_ref=src, dst_ref=dst, send_sem=send, recv_sem=recv,
            device_id=(row, col), device_id_type=MESH,
        )

    def copies(t, j):
        m = z + t
        inside = m < levels
        has = inside & (m >= c)
        block = m * cores + k
        at = chunk_rows(block, j)
        if t == 0:
            def src(cols):
                return f_ref.at[pl.ds(j * h, h), cols]
        else:
            def src(cols):
                return a_ref.at[at, cols]
        everything = pl.ds(0, width)
        found = []
        for kk in range(cores):
            piece = src(pl.ds(kk * narrow, narrow))
            into = b_ref.at[at, :]
            for dx in range(1, wide):
                xt = lax.rem(x + dx, wide)
                found.append((
                    source & inside & (m >= y * wide + xt),
                    remote(piece, into, send_b.at[kk, dx, t, j], recv_b.at[block, j],
                           z * cores + kk, y * wide + xt),
                    False,
                ))
            for dy in range(1, high):
                yt = lax.rem(y + dy, high)
                found.append((
                    source & inside & (m >= yt * wide),
                    remote(piece, into, send_b.at[kk, wide - 1 + dy, t, j], recv_b.at[block, j],
                           z * cores + kk, yt * wide + x),
                    False,
                ))
        found.append((
            has & (z > 0),
            remote(src(everything), a_ref.at[at, :], send_z.at[t, j], recv_a.at[block, j],
                   r - cores, c),
            False,
        ))
        for dk in range(1, cores):
            other = z * cores + lax.rem(k + dk, cores)
            found.append((
                has,
                remote(src(everything), a_ref.at[at, :], send_p.at[dk, t, j], recv_a.at[block, j], other, c),
                False,
            ))
        for kk in range(cores):
            piece = src(pl.ds(kk * narrow, narrow))
            into = b_ref.at[at, :]
            found.append((
                source & inside & (k != kk),
                remote(piece, into, send_b.at[kk, 0, t, j], recv_b.at[block, j], z * cores + kk, c),
                False,
            ))
        return found

    def keep(t, j):
        m = z + t
        at = chunk_rows(m * cores + k, j)
        here = f_ref.at[pl.ds(j * h, h), :] if t == 0 else a_ref.at[at, :]
        inside = (m < levels) & (m >= c)

        @pl.when(inside if t == 0 else inside & source)
        def _():
            load = pltpu.make_async_copy(here, stage, local_a.at[0])
            load.start()
            load.wait()
            if t == 0:
                pltpu.make_async_copy(stage, a_ref.at[at, :], local_a.at[1]).start()
            for kk in range(cores):
                @pl.when(source & (k == kk))
                def _():
                    store = pltpu.make_async_copy(
                        stage.at[:, pl.ds(kk * narrow, narrow)], b_ref.at[at, :], local_a.at[2]
                    )
                    store.start()
                    store.wait()
            if t == 0:
                pltpu.make_async_copy(stage, a_ref.at[at, :], local_a.at[1]).wait()

    def forwards(t, j, p):
        m = z + t
        block = m * cores + p
        part = b_ref.at[chunk_rows(block, j), :]
        mine = (x == x0) & (y != y0) & (m < levels)
        found = []
        for dx in range(1, wide):
            xt = lax.rem(x + dx, wide)
            found.append((
                mine & (m >= y * wide + xt),
                remote(part, part, send_f.at[dx, p, t, j], recv_b.at[block, j], r, y * wide + xt),
            ))
        return mine & (m >= y * wide), found

    def arrived(ref, sem):
        remote(ref, ref, send_z.at[0, 0], sem, r, c).wait_recv()

    def step(t, j):
        m = z + t
        block = m * cores + k
        if t > 0:
            @pl.when((m < levels) & (m >= c))
            def _():
                arrived(a_ref.at[chunk_rows(block, j), :], recv_a.at[block, j])
        for condition, copy, _ in copies(t, j):
            pl.when(condition)(copy.start)
        keep(t, j)

    def forward(t, j):
        for p in range(cores):
            due, found = forwards(t, j, p)
            block = (z + t) * cores + p

            @pl.when(due)
            def _():
                arrived(b_ref.at[chunk_rows(block, j), :], recv_b.at[block, j])
            for condition, copy in found:
                pl.when(condition)(copy.start)

    order = [(t, j) for t in range(levels) for j in range(chunks)]
    for n, (t, j) in enumerate(order):
        step(t, j)
        if n >= SKEW:
            forward(*order[n - SKEW])
    for t, j in order[len(order) - SKEW:]:
        forward(t, j)

    for t, j in order:
        m = z + t
        inside = m < levels
        for dk in range(1, cores):
            block = m * cores + lax.rem(k + dk, cores)

            @pl.when(inside & (m >= c))
            def _():
                arrived(a_ref.at[chunk_rows(block, j), :], recv_a.at[block, j])

            @pl.when(inside & source)
            def _():
                arrived(b_ref.at[chunk_rows(block, j), :], recv_b.at[block, j])
        for p in range(cores):
            block = m * cores + p

            @pl.when(inside & (x != x0) & (m >= c))
            def _():
                arrived(b_ref.at[chunk_rows(block, j), :], recv_b.at[block, j])
        for condition, copy, local in copies(t, j):
            pl.when(condition)(copy.wait if local else copy.wait_send)
        for p in range(cores):
            for condition, copy in forwards(t, j, p)[1]:
                pl.when(condition)(copy.wait_send)


def gather(factor, n_row, n_col):
    rows, width = factor.shape
    cores = n_row // n_col
    wide = next(w for w in range(math.isqrt(n_col), 0, -1) if n_col % w == 0)
    high = n_col // wide
    levels = n_col
    chunks = max(1, 32 // n_row)
    dma = pltpu.SemaphoreType.DMA
    whole = rows * n_row
    return pl.pallas_call(
        functools.partial(gather_kernel, (levels, wide, high, cores, chunks)),
        out_shape=(
            jax.ShapeDtypeStruct((whole, width), factor.dtype),
            jax.ShapeDtypeStruct((whole, width // cores), factor.dtype),
        ),
        in_specs=[pl.BlockSpec(memory_space=pl.ANY)],
        out_specs=(pl.BlockSpec(memory_space=pl.ANY), pl.BlockSpec(memory_space=pl.ANY)),
        scratch_shapes=[
            dma((n_row, chunks)),
            dma((n_row, chunks)),
            dma((levels, chunks)),
            dma((cores, levels, chunks)),
            dma((cores, wide + high, levels, chunks)),
            dma((wide, cores, levels, chunks)),
            dma((3,)),
            pltpu.VMEM((rows // chunks, width), factor.dtype),
        ],
        compiler_params=pltpu.CompilerParams(has_side_effects=True),
        cost_estimate=pl.CostEstimate(flops=0, bytes_accessed=whole * width * 32, transcendentals=0),
    )(factor)


LAG = 2
G = ("g", 1, 0)


def block_flows(pieces):
    half = pieces // 2
    found = []

    def add(block, source, hops, first=0, last=pieces):
        found.append((block, source, hops, first, last))

    add((3, 3), (3, 3), [((3, 3), (2, 3)), ((2, 3), (1, 3)), ((1, 3), (0, 3)), ((3, 3), (3, 1)), ((3, 3), (3, 2)),
                         ((3, 2), (3, 0))])
    add((3, 2), (3, 2), [((3, 2), (2, 2)), ((2, 2), (2, 3)), ((2, 3), (2, 1)), ((2, 2), (2, 0)), ((2, 2), (1, 2)),
                         ((1, 2), (0, 2))])
    add((3, 1), (3, 1), [((3, 1), (2, 1)), ((2, 1), (2, 0)), ((2, 0), (1, 0)), ((1, 0), (1, 1)), ((1, 1), (1, 3)),
                         ((1, 3), (1, 2))], 0, half)
    add((3, 1), (3, 1), [((3, 1), (2, 1)), ((2, 1), (1, 1)), ((1, 1), (1, 3)), ((1, 3), (1, 2)), ((1, 2), (1, 0))],
        half, pieces)
    add((3, 0), (3, 0), [((3, 0), (2, 0)), ((2, 0), (2, 1)), ((2, 1), (2, 3)), ((2, 3), (1, 3)), ((1, 3), (1, 2)),
                         ((1, 2), (1, 0)), ((1, 3), (0, 3)), ((0, 3), (0, 2)), ((0, 2), (0, 0))])
    add((2, 0), (2, 0), [((2, 0), (1, 0)), ((1, 0), (1, 1)), ((1, 1), (0, 1)), ((0, 1), (0, 0)), ((0, 0), (0, 2))])
    add((1, 0), (1, 0), [((1, 0), (0, 0))])
    add((2, 1), (2, 1), [((2, 1), (1, 1)), ((1, 1), (1, 0)), ((1, 0), (1, 2))])
    add((1, 1), (1, 1), [((1, 1), (1, 0))])
    add((2, 2), (2, 2), [((2, 2), (2, 3)), ((2, 3), (2, 1)), ((2, 2), (2, 0)), ((2, 2), (1, 2)), ((1, 2), (0, 2))])
    add(G, (1, 0), [((1, 0), (0, 0)), ((0, 0), (0, 1))], 0, half)
    add(G, (1, 0), [((1, 0), (1, 1)), ((1, 1), (0, 1))], half, pieces)
    return found


def coupling_flows(pieces):
    found = []
    for c in range(4):
        for z in range(4):
            hops = [((a, c), (a - 1, c)) for a in range(z, 0, -1)] + [((a, c), (a + 1, c)) for a in range(z, 3)]
            found.append((("u", z, c), (z, c), hops, 0, pieces))
    return found


def paced(block, s, pieces):
    if block[0] != block[1]:
        return s, False
    unit = pieces // 4
    late = s - unit
    if isinstance(s, int):
        turn = late % 3
        slow = pieces // 2 + late // 3 * 4 + turn + (turn > 0)
        return (2 * s, True) if s < unit else (slow, turn == 0)
    turn = lax.rem(late, 3)
    slow = pieces // 2 + late // 3 * 4 + turn + jnp.where(turn > 0, 1, 0)
    return jnp.where(s < unit, 2 * s, slow), (s < unit) | (turn == 0)


def span(block, first, last):
    count = last - first
    return count // 4 + count // 8 * 3 if block[0] == block[1] else count


ORDER = [14, 23, 20, 13, 6, 27, 25, 22, 3, 4, 7, 19, 21, 24, 1, 16, 5, 26, 12, 9, 2, 8, 17, 0, 15, 10, 11, 18]


@functools.cache
def plan(pieces, coupling_pieces):
    flows = block_flows(pieces) + coupling_flows(coupling_pieces)
    chips = [(z, c) for z in range(4) for c in range(4)]
    pairs = [(chip, m) for chip in chips if chip != (0, 1) for m in range(max(chip), 4)]
    busy, hops, due = {}, [], {}
    final = None
    for index in ORDER:
        block, source, route, first, last = flows[index]
        if block == G and final is None:
            due = ready_steps(pieces, hops, pairs)
            final = max(d for key, d in due.items() if key[0] == (1, 0)) + pieces // 4
        n, at = span(block, first, last), {source: final + 1 if block == G else 0}
        for p, q in route:
            t, used = at[p], busy.setdefault((p, q), [])
            while any(t < e and s < t + n for s, e in used):
                t += 1
            used.append((t, t + n))
            at[q] = t + LAG
            hops.append((block, p, q, first, last, t))
    slots = {chip: {} for chip in chips}
    needs = {chip: set() for chip in chips}
    for chip, m in pairs:
        z, c = chip
        slots[chip][m, c] = m
        needs[chip].add((m, c))
        if c != z:
            slots[chip][m, z] = 4 + m
            needs[chip].add((m, z))
    for block, p, q, first, last, t in hops:
        for chip in (p, q):
            if block[0] != "u" and block not in slots[chip] and block != chip:
                slots[chip][block] = min(set(range(8)) - set(slots[chip].values()))
    steps = max([t + span(block, first, last) + LAG for block, p, q, first, last, t in hops] + [d + pieces // 4 for d in due.values()] + [final + 1])
    return hops, slots, needs, due, steps, final


def ready_steps(pieces, hops, pairs):
    due, group = {}, pieces // 8
    for chip, m in pairs:
        z, c = chip
        ready = {(z, c): [1] * pieces}
        for block, p, q, first, last, t in hops:
            if q == chip:
                for s in range(span(block, first, last)):
                    j, more = paced(block, s, pieces)
                    for i in range(1 + more):
                        ready.setdefault(block, [None] * pieces)[first + j + i] = t + LAG + s
        both = [ready[m, c], ready[m, z]]
        for part in range(4):
            begin = part * (pieces // 4)
            due[chip, m, part] = 1 + max(b[begin + j] - j // group * group for b in both for j in range(pieces // 4))
    return due


def stream_kernel(pieces, coupling_pieces, f_ref, u_ref, x_ref, ub_ref, g_ref, send, send_u, near, near_u, recv,
                  recv_u, recv_near, recv_near_u, turn, blank, local, acc, a_buf, b_buf, stage, stage_u, zeros, flipped):
    hops, slots, needs, due, steps, final = plan(pieces, coupling_pieces)
    rows, width = f_ref.shape
    depth, narrow = u_ref.shape
    h, hu, quarter = rows // pieces, depth // coupling_pieces, width // 4
    tall = acc.shape[0]
    r, c = lax.axis_index("row"), lax.axis_index("col")
    k, z = lax.rem(r, 2), r // 2
    chip = z * 4 + c
    owner = z >= c

    def at_rows(slot, core, j):
        return pl.ds(pl.multiple_of((slot * 2 + core) * rows + j * h, h), h)

    def remote(src, dst, send_sem, recv_sem, row, col):
        return pltpu.make_async_remote_copy(
            src_ref=src, dst_ref=dst, send_sem=send_sem, recv_sem=recv_sem,
            device_id=(row, col), device_id_type=MESH,
        )

    def shapes(block, j):
        if block[0] != block[1]:
            return [(None, width)]
        part = (k * pieces + j) // (pieces // 2)
        return [(part == q, (q + 1) * quarter) for q in range(4)]

    def each(block, j, act):
        if block[0] == "u":
            act(None)
            return
        for condition, columns in shapes(block, j):
            if condition is None:
                act(columns)
            else:
                pl.when(condition)(functools.partial(act, columns))

    def hop_copy(hop, number, j, columns):
        block, p, q, first, last, t = hop
        if block[0] == "u":
            at = pl.ds(pl.multiple_of(j * hu, hu), hu)
            src = u_ref.at[at, :] if p == block[1:] else ub_ref.at[block[1] * 2 + k, at, :]
            return remote(src, ub_ref.at[block[1] * 2 + k, at, :], send_u.at[number, j], recv_u.at[block[1], j],
                          q[0] * 2 + k, q[1])
        cols = pl.ds(0, columns)
        if p == block:
            src = f_ref.at[pl.ds(pl.multiple_of(j * h, h), h), cols]
        else:
            src = x_ref.at[at_rows(slots[p][block], k, j), cols]
        slot = slots[q][block]
        return remote(src, x_ref.at[at_rows(slot, k, j), cols], send.at[number, j], recv.at[slot, j],
                      q[0] * 2 + k, q[1])

    def near_copy(slot, j, src=None):
        at = at_rows(slot, k, j)
        return remote(x_ref.at[at, :] if src is None else src, x_ref.at[at, :], near.at[slot, j],
                      recv_near.at[slot, j], z * 2 + 1 - k, c)

    def near_arrival(slot, j):
        ref = x_ref.at[at_rows(slot, 1 - k, j), :]
        return remote(ref, ref, near.at[slot, j], recv_near.at[slot, j], r, c)

    def near_copy_u(level, j, src=None):
        at = pl.ds(pl.multiple_of(j * hu, hu), hu)
        ref = ub_ref.at[level * 2 + k, at, :]
        return remote(ref if src is None else src, ref, near_u.at[level, j], recv_near_u.at[level, j],
                      z * 2 + 1 - k, c)

    def own_rows(j):
        return f_ref.at[pl.ds(pl.multiple_of(j * h, h), h), :]

    def own_rows_u(j):
        return u_ref.at[pl.ds(pl.multiple_of(j * hu, hu), hu), :]

    chips = [(a, b) for a in range(4) for b in range(4)]
    incoming = {chip_: [hop for hop in hops if hop[2] == chip_] for chip_ in chips}
    outgoing = {chip_: [] for chip_ in chips}
    count, count_u = {}, {}
    for hop in hops:
        counts = count_u if hop[0][0] == "u" else count
        number = counts.get(hop[1], 0)
        counts[hop[1]] = number + 1
        outgoing[hop[1]].append((hop, number))

    zeros[...] = jnp.zeros_like(zeros)

    def fill(slot, act):
        def one(j, carry):
            for condition, columns in shapes((0, 0), j):
                if columns < width:
                    @pl.when(condition)
                    def _():
                        act(pltpu.make_async_copy(
                            zeros.at[:, pl.ds(0, width - columns)],
                            x_ref.at[at_rows(slot, k, j), pl.ds(columns, width - columns)], blank.at[j]))
            return carry
        lax.fori_loop(0, pieces, one, 0)

    def fill_all(act):
        for place in chips:
            for block in needs[place]:
                if block[0] == block[1] and block != place:
                    pl.when(chip == place[0] * 4 + place[1])(functools.partial(fill, slots[place][block], act))

    def spread(j, carry):
        @pl.when(owner)
        def _():
            near_copy(z, j, own_rows(j)).start()
        return carry

    def spread_u(j, carry):
        near_copy_u(z, j, own_rows_u(j)).start()
        return carry

    def loads(m, slot_b, ago, into):
        cols = pl.ds(pl.multiple_of(k * tall, tall), tall)
        found = []
        for core in range(2):
            at_a = pl.ds(pl.multiple_of((m * 2 + core) * rows + ago * h, 2 * h), 2 * h)
            at_b = pl.ds(pl.multiple_of((slot_b * 2 + core) * rows + ago * h, 2 * h), 2 * h)
            half = pl.ds(core * 2 * h, 2 * h)
            found.append(pltpu.make_async_copy(x_ref.at[at_a, :], a_buf.at[into, half, :], local.at[2 + into * 4 + core]))
            found.append(pltpu.make_async_copy(x_ref.at[at_b, cols], b_buf.at[into, half, :], local.at[4 + into * 4 + core]))
        return found

    def multiply(into):
        for copy in loads(0, 0, 0, into):
            copy.wait()
        tile = min(256, tall)

        def rows_of(i, carry):
            at = pl.ds(pl.multiple_of(i * tile, tile), tile)
            acc[at, :] += lax.dot_general(
                b_buf[into, :, at], a_buf[into], (((0,), (0,)), ((), ())), preferred_element_type=jnp.float32)
            return carry
        lax.fori_loop(0, tall // tile, rows_of, 0)

    def flip():
        slot = slots[1, 0][G]
        tile = min(256, width)

        def turned(i, carry):
            at = pl.ds(pl.multiple_of(i * tile, tile), tile)
            flipped[at, :] = acc[:, at].T.astype(flipped.dtype)
            return carry
        lax.fori_loop(0, width // tile, turned, 0)
        cols = pl.ds(pl.multiple_of(k * tall, tall), tall)
        kept = []
        for half in range(2):
            at = pl.ds((slot * 2 + half) * rows, rows)
            kept.append(pltpu.make_async_copy(flipped.at[pl.ds(half * rows, rows), :], x_ref.at[at, cols],
                                              local.at[half]))
        for copy in kept:
            copy.start()
        for copy in kept:
            copy.wait()
        at = pl.ds(pl.multiple_of((slot * 2 + 1 - k) * rows, rows), rows)
        pass_on = remote(x_ref.at[at, cols], x_ref.at[at, cols], turn.at[0], turn.at[1], z * 2 + 1 - k, c)
        pass_on.start()
        pass_on.wait_send()
        at = pl.ds(pl.multiple_of((slot * 2 + k) * rows, rows), rows)
        cols = pl.ds(pl.multiple_of((1 - k) * tall, tall), tall)
        remote(x_ref.at[at, cols], x_ref.at[at, cols], turn.at[0], turn.at[1], r, c).wait_recv()

    def step(t, carry):
        for place in chips:
            @pl.when(chip == place[0] * 4 + place[1])
            def _():
                for hop in incoming[place]:
                    block, p, q, first, last, t0 = hop

                    def take(j):
                        each(block, j, lambda columns: hop_copy(hop, 0, j, columns).wait_recv())
                        if block[0] == "u":
                            near_copy_u(block[1], j).start()
                        elif block in needs[place]:
                            near_copy(slots[place][block], j).start()

                    @pl.when((t >= t0 + LAG) & (t < t0 + LAG + span(block, first, last)))
                    def _():
                        j, more = paced(block, t - (t0 + LAG), pieces)
                        take(first + j)
                        if more is not False:
                            pl.when(more)(functools.partial(take, first + j + 1))
                for hop, number in outgoing[place]:
                    block, p, q, first, last, t0 = hop

                    def give(j):
                        each(block, j, lambda columns: hop_copy(hop, number, j, columns).start())

                    @pl.when((t >= t0) & (t < t0 + span(block, first, last)))
                    def _():
                        j, more = paced(block, t - t0, pieces)
                        give(first + j)
                        if more is not False:
                            pl.when(more)(functools.partial(give, first + j + 1))

        def consume(entry, carry):
            pending, into = carry
            begin = jnp.int32(-1000)
            for index in range(16):
                begin = jnp.where(entry == index, begins[index], begin)
            m, part = entry // 4, lax.rem(entry, 4)
            past = t - begin
            ready = (past >= 0) & (past < pieces // 4) & (lax.rem(past, 2) == 0)

            @pl.when(ready)
            def _():
                ago = past + part * (pieces // 4)
                slot_b = jnp.where(c == z, m, 4 + m)
                for i in range(2):
                    near_arrival(m, ago + i).wait_recv()

                    @pl.when(c != z)
                    def _():
                        near_arrival(slot_b, ago + i).wait_recv()
                for copy in loads(m, slot_b, ago, 1 - into):
                    copy.start()
                pl.when(pending == 1)(functools.partial(multiply, into))
            return jnp.where(ready, 1, pending), jnp.where(ready, 1 - into, into)
        pending, into = lax.fori_loop(0, 16, consume, carry)
        last = (chip == 4) & (t == final)

        @pl.when(last)
        def _():
            pl.when(pending == 1)(functools.partial(multiply, into))
            flip()
        return jnp.where(last, 0, pending), into

    begins = []
    for index in range(16):
        begin = jnp.int32(-1000)
        for place in chips:
            if (place, index // 4, index % 4) in due:
                begin = jnp.where(chip == place[0] * 4 + place[1], due[place, index // 4, index % 4], begin)
        begins.append(begin)

    own = pltpu.make_async_copy(f_ref, stage, local.at[0])
    keep = pltpu.make_async_copy(stage, x_ref.at[pl.ds(pl.multiple_of((z * 2 + k) * rows, rows), rows), :], local.at[0])
    own_u = pltpu.make_async_copy(u_ref, stage_u, local.at[1])
    keep_u = pltpu.make_async_copy(stage_u, ub_ref.at[r], local.at[1])
    pl.when(owner)(own.start)
    own_u.start()
    lax.fori_loop(0, pieces, spread, 0)
    lax.fori_loop(0, coupling_pieces, spread_u, 0)
    fill_all(lambda copy: copy.start())
    acc[...] = jnp.zeros_like(acc)

    @pl.when(owner)
    def _():
        own.wait()
        keep.start()
    own_u.wait()
    keep_u.start()
    fill_all(lambda copy: copy.wait())
    pl.when(owner)(keep.wait)
    keep_u.wait()
    pending, turned_to = lax.fori_loop(0, steps, step, (jnp.int32(0), jnp.int32(0)))
    pl.when(pending == 1)(functools.partial(multiply, turned_to))

    @pl.when(chip == 1)
    def _():
        at = pl.ds(pl.multiple_of((slots[0, 1][G] * 2 + k) * rows, rows), rows)
        load = pltpu.make_async_copy(x_ref.at[at, :], stage, local.at[0])
        load.start()
        load.wait()
        tile = min(128, tall)

        def widen(i, carry):
            at = pl.ds(pl.multiple_of(i * tile, tile), tile)
            acc[at, :] = stage[at, :].astype(jnp.float32)
            return carry
        lax.fori_loop(0, tall // tile, widen, 0)
    out = pltpu.make_async_copy(acc, g_ref, local.at[0])
    out.start()

    def settle(j, carry):
        @pl.when(owner)
        def _():
            near_copy(z, j, own_rows(j)).wait_send()
        return carry
    lax.fori_loop(0, pieces, settle, 0)

    def settle_u(j, carry):
        for level in range(4):
            near_copy_u(level, j).wait_send()
            at = pl.ds(pl.multiple_of(j * hu, hu), hu)
            ref = ub_ref.at[level * 2 + 1 - k, at, :]
            remote(ref, ref, near_u.at[level, j], recv_near_u.at[level, j], r, c).wait_recv()
        return carry
    lax.fori_loop(0, coupling_pieces, settle_u, 0)
    for place in chips:
        @pl.when(chip == place[0] * 4 + place[1])
        def _():
            for hop, number in outgoing[place]:
                def sent(j, carry):
                    each(hop[0], j, lambda columns: hop_copy(hop, number, j, columns).wait_send())
                    return carry
                lax.fori_loop(hop[3], hop[4], sent, 0)
            for hop in incoming[place]:
                if hop[0][0] != "u" and hop[0] in needs[place]:
                    def passed(j, carry):
                        near_copy(slots[place][hop[0]], j).wait_send()
                        return carry
                    lax.fori_loop(hop[3], hop[4], passed, 0)
    out.wait()


def stream(factor, coupling, n_row, n_col):
    rows, width = factor.shape
    depth, narrow = coupling.shape
    pieces, coupling_pieces = 16, 4
    hops = plan(pieces, coupling_pieces)[0]
    out_count = max(sum(hop[1] == chip and hop[0][0] != "u" for hop in hops) for chip in {h[1] for h in hops})
    out_count_u = max(sum(hop[1] == chip and hop[0][0] == "u" for hop in hops) for chip in {h[1] for h in hops})
    tall = width // 2
    h = rows // pieces
    dma = pltpu.SemaphoreType.DMA
    return pl.pallas_call(
        functools.partial(stream_kernel, pieces, coupling_pieces),
        out_shape=(
            jax.ShapeDtypeStruct((8 * 2 * rows, width), factor.dtype),
            jax.ShapeDtypeStruct((n_row, depth, narrow), coupling.dtype),
            jax.ShapeDtypeStruct((tall, width), jnp.float32),
        ),
        in_specs=[pl.BlockSpec(memory_space=pl.ANY)] * 2,
        out_specs=[pl.BlockSpec(memory_space=pl.ANY)] * 3,
        scratch_shapes=[
            dma((out_count, pieces)),
            dma((out_count_u, coupling_pieces)),
            dma((8, pieces)),
            dma((4, coupling_pieces)),
            dma((8, pieces)),
            dma((4, coupling_pieces)),
            dma((8, pieces)),
            dma((4, coupling_pieces)),
            dma((2,)),
            dma((pieces,)),
            dma((12,)),
            pltpu.VMEM((tall, width), jnp.float32),
            pltpu.VMEM((2, 4 * h, width), factor.dtype),
            pltpu.VMEM((2, 4 * h, tall), factor.dtype),
            pltpu.VMEM((rows, width), factor.dtype),
            pltpu.VMEM((depth, narrow), coupling.dtype),
            pltpu.VMEM((h, width), factor.dtype),
            pltpu.VMEM((width, tall), factor.dtype),
        ],
        compiler_params=pltpu.CompilerParams(has_side_effects=True, vmem_limit_bytes=63 * 1024 * 1024),
        cost_estimate=pl.CostEstimate(flops=0, bytes_accessed=rows * width * 64, transcendentals=0),
    )(factor, coupling)


def child_kernel(n_col, g_ref, u_ref, part_ref, other_ref, send, recv, local, whole, held, out):
    r, c = lax.axis_index("row"), lax.axis_index("col")
    tile = held.shape[1]
    count, _, narrow = whole.shape
    cores = count // n_col
    tiles = g_ref.shape[0] // tile

    def rows(i):
        return pl.ds(pl.multiple_of(i * tile, tile), tile)

    def load(i, into):
        return pltpu.make_async_copy(g_ref.at[rows(i), :], held.at[into], local.at[into])

    def copies(i):
        found = []
        for d in range(1, n_col):
            ct = lax.rem(c + d, n_col)
            found.append(pltpu.make_async_remote_copy(
                src_ref=part_ref.at[ct, rows(i), :],
                dst_ref=other_ref.at[d - 1, rows(i), :],
                send_sem=send.at[d - 1, i],
                recv_sem=recv.at[d - 1, i],
                device_id=(r, ct),
                device_id_type=MESH,
            ))
        return found

    fetch = pltpu.make_async_copy(u_ref, whole, local.at[2])
    fetch.start()
    load(0, 0).start()
    fetch.wait()

    def one(i, carry):
        into = lax.rem(i, 2)
        load(i, into).wait()

        @pl.when(i + 1 < tiles)
        def _():
            load(i + 1, 1 - into).start()
        rounded = held[into].astype(whole.dtype)
        for q in range(count):
            product = jnp.dot(rounded, whole[q], preferred_element_type=jnp.float32)
            out[q // cores, :, pl.ds(q % cores * narrow, narrow)] = product.astype(out.dtype)
        keep = pltpu.make_async_copy(out, part_ref.at[:, rows(i), :], local.at[3])
        keep.start()
        keep.wait()
        for copy in copies(i):
            copy.start()
        return carry
    lax.fori_loop(0, tiles, one, 0)

    def settle(i, carry):
        for copy in copies(i):
            copy.wait()
        return carry
    lax.fori_loop(0, tiles, settle, 0)


def child_parts(gram, coupling, n_col):
    tall, width = gram.shape
    count, depth, narrow = coupling.shape
    tile = min(128, tall)
    wide = count * narrow // n_col
    dma = pltpu.SemaphoreType.DMA
    return pl.pallas_call(
        functools.partial(child_kernel, n_col),
        out_shape=(
            jax.ShapeDtypeStruct((n_col, tall, wide), coupling.dtype),
            jax.ShapeDtypeStruct((n_col - 1, tall, wide), coupling.dtype),
        ),
        in_specs=[pl.BlockSpec(memory_space=pl.ANY)] * 2,
        out_specs=[pl.BlockSpec(memory_space=pl.ANY)] * 2,
        scratch_shapes=[
            dma((n_col - 1, tall // tile)),
            dma((n_col - 1, tall // tile)),
            dma((4,)),
            pltpu.VMEM((count, depth, narrow), coupling.dtype),
            pltpu.VMEM((2, tile, width), gram.dtype),
            pltpu.VMEM((n_col, tile, wide), coupling.dtype),
        ],
        compiler_params=pltpu.CompilerParams(has_side_effects=True, vmem_limit_bytes=63 * 1024 * 1024),
    )(gram, coupling)


def finish_kernel(c_ref, g_ref, own_ref, other_ref, member_ref, gram_ref, child_ref):
    gram_ref[...] = g_ref[...]
    total = own_ref[0].astype(jnp.float32)
    for d in range(other_ref.shape[0]):
        total = total + other_ref[d].astype(jnp.float32)
    child_ref[...] = jnp.where(member_ref[...] != 0, -total.T, jnp.float32(0.0))


def finish(gram, own, other, member, col_index):
    tall, width = gram.shape
    wide = own.shape[2]
    tile = min(128, tall)
    return pl.pallas_call(
        finish_kernel,
        grid_spec=pltpu.PrefetchScalarGridSpec(
            num_scalar_prefetch=1,
            grid=(tall // tile,),
            in_specs=[
                pl.BlockSpec((tile, width), lambda i, c: (i, 0)),
                pl.BlockSpec((1, tile, wide), lambda i, c: (c[0], i, 0)),
                pl.BlockSpec((other.shape[0], tile, wide), lambda i, c: (0, i, 0)),
                pl.BlockSpec((1, tile), lambda i, c: (0, i)),
            ],
            out_specs=(
                pl.BlockSpec((tile, width), lambda i, c: (i, 0)),
                pl.BlockSpec((wide, tile), lambda i, c: (0, i)),
            ),
        ),
        out_shape=(
            jax.ShapeDtypeStruct((tall, width), jnp.float32),
            jax.ShapeDtypeStruct((wide, tall), jnp.float32),
        ),
        compiler_params=pltpu.CompilerParams(vmem_limit_bytes=63 * 1024 * 1024),
        cost_estimate=pl.CostEstimate(flops=0, bytes_accessed=tall * width * 12, transcendentals=0),
    )(jnp.reshape(col_index, (1,)), gram, own, other, member)


def exchange_kernel(n_col, part_ref, out_ref, send, recv):
    r, c = lax.axis_index("row"), lax.axis_index("col")
    depth = out_ref.shape[1]
    started = []
    for d in range(1, n_col):
        ct = lax.rem(c + d, n_col)
        copy = pltpu.make_async_remote_copy(
            src_ref=part_ref.at[pl.ds(pl.multiple_of(ct * depth, depth), depth), :],
            dst_ref=out_ref.at[d - 1],
            send_sem=send.at[d - 1],
            recv_sem=recv.at[d - 1],
            device_id=(r, ct),
            device_id_type=MESH,
        )
        copy.start()
        started.append(copy)
    for copy in started:
        copy.wait()


def exchange(part, n_col):
    total, width = part.shape
    dma = pltpu.SemaphoreType.DMA
    return pl.pallas_call(
        functools.partial(exchange_kernel, n_col),
        out_shape=jax.ShapeDtypeStruct((n_col - 1, total // n_col, width), part.dtype),
        in_specs=[pl.BlockSpec(memory_space=pl.ANY)],
        out_specs=pl.BlockSpec(memory_space=pl.ANY),
        scratch_shapes=[dma((n_col - 1,)), dma((n_col - 1,))],
        compiler_params=pltpu.CompilerParams(has_side_effects=True),
    )(part)


def general(n_row, n_col, factor, coupling):
    rows_here = factor.shape[0]
    row_index, col_index = lax.axis_index("row"), lax.axis_index("col")
    cores = n_row // n_col
    below, partner = gather(factor, n_row, n_col)
    coupling_full = lax.all_gather(coupling, "row", axis=1, tiled=True)

    def product(level, below, partner):
        first = level * rows_here * cores
        return lax.dot_general(
            partner[first:], below[first:], (((0,), (0,)), ((), ())), preferred_element_type=jnp.float32
        )

    gram = lax.switch(
        jnp.maximum(row_index // cores, col_index),
        [functools.partial(product, level) for level in range(n_col)],
        below,
        partner,
    )
    rounded = gram.astype(jnp.bfloat16)
    part = lax.dot_general(
        coupling_full, rounded, (((0,), (1,)), ((), ())), preferred_element_type=jnp.float32
    ).astype(jnp.bfloat16)
    return gram, part


def body(n_row, n_col, factor, sel_tiles, coupling):
    rows_here = factor.shape[0]
    row_index, col_index = lax.axis_index("row"), lax.axis_index("col")
    cores = n_row // n_col
    global_rows = row_index * rows_here + jnp.arange(rows_here, dtype=jnp.int32)
    member = jnp.any((global_rows // TILE)[:, None] == sel_tiles[None, :], axis=1)
    if (n_row, n_col) == (8, 4):
        _, pieces, gram = stream(factor, coupling, n_row, n_col)
        own, other = child_parts(gram, pieces, n_col)
        return finish(gram, own, other, member.astype(jnp.int32)[None, :], col_index)
    gram, part = general(n_row, n_col, factor, coupling)
    depth = part.shape[0] // n_col
    arrived = exchange(part, n_col)
    summed = lax.dynamic_slice_in_dim(part, col_index * depth, depth, 0).astype(jnp.float32)
    for d in range(n_col - 1):
        summed = summed + arrived[d].astype(jnp.float32)
    child = jnp.where(member[None, :], -summed, jnp.float32(0.0))
    return (gram, child)


def solution(mesh):
    placed = (P("row", "col"), P(), P("col", "row"))
    return jax.shard_map(
        functools.partial(body, mesh.shape["row"], mesh.shape["col"]),
        mesh=mesh,
        in_specs=placed,
        out_specs=(P("row", "col"), P("col", "row")),
        check_vma=False,
    )
```

```python
import functools
import math

import jax
import jax.numpy as jnp
from jax import lax
from jax.experimental import pallas as pl
from jax.experimental.pallas import tpu as pltpu
from jax.sharding import PartitionSpec as P

TILE = 128
MESH = pl.DeviceIdType.MESH
SKEW = 2


def gather_kernel(dims, f_ref, a_ref, b_ref, recv_a, recv_b, send_z, send_p, send_b, send_f, local_a, stage):
    levels, wide, high, cores, chunks = dims
    rows, width = f_ref.shape
    narrow = width // cores
    h = rows // chunks
    r, c = lax.axis_index("row"), lax.axis_index("col")
    k, z = lax.rem(r, cores), r // cores
    x, y = lax.rem(c, wide), c // wide
    x0, y0 = lax.rem(z, wide), z // wide
    source = c == z

    def chunk_rows(block, j):
        return pl.ds(pl.multiple_of(block * rows + j * h, h), h)

    def remote(src, dst, send, recv, row, col):
        return pltpu.make_async_remote_copy(
            src_ref=src, dst_ref=dst, send_sem=send, recv_sem=recv,
            device_id=(row, col), device_id_type=MESH,
        )

    def copies(t, j):
        m = z + t
        inside = m < levels
        has = inside & (m >= c)
        block = m * cores + k
        at = chunk_rows(block, j)
        if t == 0:
            def src(cols):
                return f_ref.at[pl.ds(j * h, h), cols]
        else:
            def src(cols):
                return a_ref.at[at, cols]
        everything = pl.ds(0, width)
        found = []
        for kk in range(cores):
            piece = src(pl.ds(kk * narrow, narrow))
            into = b_ref.at[at, :]
            for dx in range(1, wide):
                xt = lax.rem(x + dx, wide)
                found.append((
                    source & inside & (m >= y * wide + xt),
                    remote(piece, into, send_b.at[kk, dx, t, j], recv_b.at[block, j],
                           z * cores + kk, y * wide + xt),
                    False,
                ))
            for dy in range(1, high):
                yt = lax.rem(y + dy, high)
                found.append((
                    source & inside & (m >= yt * wide),
                    remote(piece, into, send_b.at[kk, wide - 1 + dy, t, j], recv_b.at[block, j],
                           z * cores + kk, yt * wide + x),
                    False,
                ))
        found.append((
            has & (z > 0),
            remote(src(everything), a_ref.at[at, :], send_z.at[t, j], recv_a.at[block, j],
                   r - cores, c),
            False,
        ))
        for dk in range(1, cores):
            other = z * cores + lax.rem(k + dk, cores)
            found.append((
                has,
                remote(src(everything), a_ref.at[at, :], send_p.at[dk, t, j], recv_a.at[block, j], other, c),
                False,
            ))
        for kk in range(cores):
            piece = src(pl.ds(kk * narrow, narrow))
            into = b_ref.at[at, :]
            found.append((
                source & inside & (k != kk),
                remote(piece, into, send_b.at[kk, 0, t, j], recv_b.at[block, j], z * cores + kk, c),
                False,
            ))
        return found

    def keep(t, j):
        m = z + t
        at = chunk_rows(m * cores + k, j)
        here = f_ref.at[pl.ds(j * h, h), :] if t == 0 else a_ref.at[at, :]
        inside = (m < levels) & (m >= c)

        @pl.when(inside if t == 0 else inside & source)
        def _():
            load = pltpu.make_async_copy(here, stage, local_a.at[0])
            load.start()
            load.wait()
            if t == 0:
                pltpu.make_async_copy(stage, a_ref.at[at, :], local_a.at[1]).start()
            for kk in range(cores):
                @pl.when(source & (k == kk))
                def _():
                    store = pltpu.make_async_copy(
                        stage.at[:, pl.ds(kk * narrow, narrow)], b_ref.at[at, :], local_a.at[2]
                    )
                    store.start()
                    store.wait()
            if t == 0:
                pltpu.make_async_copy(stage, a_ref.at[at, :], local_a.at[1]).wait()

    def forwards(t, j, p):
        m = z + t
        block = m * cores + p
        part = b_ref.at[chunk_rows(block, j), :]
        mine = (x == x0) & (y != y0) & (m < levels)
        found = []
        for dx in range(1, wide):
            xt = lax.rem(x + dx, wide)
            found.append((
                mine & (m >= y * wide + xt),
                remote(part, part, send_f.at[dx, p, t, j], recv_b.at[block, j], r, y * wide + xt),
            ))
        return mine & (m >= y * wide), found

    def arrived(ref, sem):
        remote(ref, ref, send_z.at[0, 0], sem, r, c).wait_recv()

    def step(t, j):
        m = z + t
        block = m * cores + k
        if t > 0:
            @pl.when((m < levels) & (m >= c))
            def _():
                arrived(a_ref.at[chunk_rows(block, j), :], recv_a.at[block, j])
        for condition, copy, _ in copies(t, j):
            pl.when(condition)(copy.start)
        keep(t, j)

    def forward(t, j):
        for p in range(cores):
            due, found = forwards(t, j, p)
            block = (z + t) * cores + p

            @pl.when(due)
            def _():
                arrived(b_ref.at[chunk_rows(block, j), :], recv_b.at[block, j])
            for condition, copy in found:
                pl.when(condition)(copy.start)

    order = [(t, j) for t in range(levels) for j in range(chunks)]
    for n, (t, j) in enumerate(order):
        step(t, j)
        if n >= SKEW:
            forward(*order[n - SKEW])
    for t, j in order[len(order) - SKEW:]:
        forward(t, j)

    for t, j in order:
        m = z + t
        inside = m < levels
        for dk in range(1, cores):
            block = m * cores + lax.rem(k + dk, cores)

            @pl.when(inside & (m >= c))
            def _():
                arrived(a_ref.at[chunk_rows(block, j), :], recv_a.at[block, j])

            @pl.when(inside & source)
            def _():
                arrived(b_ref.at[chunk_rows(block, j), :], recv_b.at[block, j])
        for p in range(cores):
            block = m * cores + p

            @pl.when(inside & (x != x0) & (m >= c))
            def _():
                arrived(b_ref.at[chunk_rows(block, j), :], recv_b.at[block, j])
        for condition, copy, local in copies(t, j):
            pl.when(condition)(copy.wait if local else copy.wait_send)
        for p in range(cores):
            for condition, copy in forwards(t, j, p)[1]:
                pl.when(condition)(copy.wait_send)


def gather(factor, n_row, n_col):
    rows, width = factor.shape
    cores = n_row // n_col
    wide = next(w for w in range(math.isqrt(n_col), 0, -1) if n_col % w == 0)
    high = n_col // wide
    levels = n_col
    chunks = max(1, 32 // n_row)
    dma = pltpu.SemaphoreType.DMA
    whole = rows * n_row
    return pl.pallas_call(
        functools.partial(gather_kernel, (levels, wide, high, cores, chunks)),
        out_shape=(
            jax.ShapeDtypeStruct((whole, width), factor.dtype),
            jax.ShapeDtypeStruct((whole, width // cores), factor.dtype),
        ),
        in_specs=[pl.BlockSpec(memory_space=pl.ANY)],
        out_specs=(pl.BlockSpec(memory_space=pl.ANY), pl.BlockSpec(memory_space=pl.ANY)),
        scratch_shapes=[
            dma((n_row, chunks)),
            dma((n_row, chunks)),
            dma((levels, chunks)),
            dma((cores, levels, chunks)),
            dma((cores, wide + high, levels, chunks)),
            dma((wide, cores, levels, chunks)),
            dma((3,)),
            pltpu.VMEM((rows // chunks, width), factor.dtype),
        ],
        compiler_params=pltpu.CompilerParams(has_side_effects=True),
        cost_estimate=pl.CostEstimate(flops=0, bytes_accessed=whole * width * 32, transcendentals=0),
    )(factor)


LAG = 2
G = ("g", 1, 0)


def block_flows(pieces):
    half, cut = pieces // 2, 5 * pieces // 8
    found = []

    def add(block, source, hops, first=0, last=pieces):
        found.append((block, source, hops, first, last))

    add((3, 3), (3, 3), [((3, 3), (2, 3)), ((2, 3), (1, 3)), ((1, 3), (0, 3)), ((3, 3), (3, 1)), ((3, 3), (3, 2)),
                         ((3, 2), (3, 0))])
    add((3, 2), (3, 2), [((3, 2), (2, 2)), ((2, 2), (2, 3)), ((2, 3), (2, 1)), ((2, 2), (2, 0)), ((2, 2), (1, 2)),
                         ((1, 2), (0, 2))])
    add((3, 1), (3, 1), [((3, 1), (2, 1)), ((2, 1), (2, 0)), ((2, 0), (1, 0)), ((1, 0), (1, 1)), ((1, 1), (1, 3)),
                         ((1, 0), (1, 2))], 0, cut)
    add((3, 1), (3, 1), [((3, 1), (2, 1)), ((2, 1), (1, 1)), ((1, 1), (1, 3)), ((1, 3), (1, 2)), ((1, 2), (1, 0))],
        cut, pieces)
    add((3, 0), (3, 0), [((3, 0), (2, 0)), ((2, 0), (2, 1)), ((2, 1), (2, 3)), ((2, 3), (1, 3)), ((1, 3), (1, 2)),
                         ((1, 2), (1, 0)), ((1, 3), (0, 3)), ((0, 3), (0, 2)), ((0, 2), (0, 0))])
    around = [((1, 0), (1, 1)), ((1, 1), (0, 1)), ((0, 1), (0, 0)), ((0, 0), (0, 2))]
    add((2, 0), (2, 0), [((2, 0), (1, 0))] + around, 0, 3 * pieces // 4)
    add((2, 0), (2, 0), [((2, 0), (2, 2)), ((2, 2), (1, 2)), ((1, 2), (1, 0))] + around, 3 * pieces // 4, pieces)
    add((1, 0), (1, 0), [((1, 0), (0, 0))])
    add((2, 1), (2, 1), [((2, 1), (1, 1)), ((1, 1), (1, 0)), ((1, 0), (1, 2))])
    add((1, 1), (1, 1), [((1, 1), (1, 0))])
    add((2, 2), (2, 2), [((2, 2), (2, 3)), ((2, 3), (2, 1)), ((2, 2), (2, 0)), ((2, 2), (1, 2)), ((1, 2), (0, 2))])
    add(G, (1, 0), [((1, 0), (0, 0)), ((0, 0), (0, 1))], 0, half)
    add(G, (1, 0), [((1, 0), (1, 1)), ((1, 1), (0, 1))], half, pieces)
    return found


def coupling_flows(pieces):
    found = []
    for c in range(4):
        for z in range(4):
            hops = [((a, c), (a - 1, c)) for a in range(z, 0, -1)] + [((a, c), (a + 1, c)) for a in range(z, 3)]
            found.append((("u", z, c), (z, c), hops, 0, pieces))
    return found


def paced(block, s, pieces):
    if block[0] != block[1]:
        return s, False
    unit = pieces // 4
    late = s - unit
    if isinstance(s, int):
        turn = late % 3
        slow = pieces // 2 + late // 3 * 4 + turn + (turn > 0)
        return (2 * s, True) if s < unit else (slow, turn == 0)
    turn = lax.rem(late, 3)
    slow = pieces // 2 + late // 3 * 4 + turn + jnp.where(turn > 0, 1, 0)
    return jnp.where(s < unit, 2 * s, slow), (s < unit) | (turn == 0)


def span(block, first, last):
    count = last - first
    return count // 4 + count // 8 * 3 if block[0] == block[1] else count


ORDER = [6, 24, 14, 15, 3, 9, 25, 13, 7, 17, 5, 4, 8, 26, 1, 2, 20, 10, 19, 0, 28, 16, 18, 21, 12, 11, 23, 22, 27]


@functools.cache
def plan(pieces, coupling_pieces):
    flows = block_flows(pieces) + coupling_flows(coupling_pieces)
    chips = [(z, c) for z in range(4) for c in range(4)]
    pairs = [(chip, m) for chip in chips if chip != (0, 1) for m in range(max(chip), 4)]
    busy, hops, due = {}, [], {}
    final = None
    for index in ORDER:
        block, source, route, first, last = flows[index]
        if block == G and final is None:
            due = ready_steps(pieces, hops, pairs)
            final = max(d for key, d in due.items() if key[0] == (1, 0)) + pieces // 4
        n, at = span(block, first, last), {source: final + 1 if block == G else 0}
        for p, q in route:
            t, used = at[p], busy.setdefault((p, q), [])
            while any(t < e and s < t + n for s, e in used):
                t += 1
            used.append((t, t + n))
            at[q] = t + LAG
            hops.append((block, p, q, first, last, t))
    slots = {chip: {} for chip in chips}
    needs = {chip: set() for chip in chips}
    for chip, m in pairs:
        z, c = chip
        slots[chip][m, c] = m
        needs[chip].add((m, c))
        if c != z:
            slots[chip][m, z] = 4 + m
            needs[chip].add((m, z))
    for block, p, q, first, last, t in hops:
        for chip in (p, q):
            if block[0] != "u" and block not in slots[chip] and block != chip:
                slots[chip][block] = min(set(range(8)) - set(slots[chip].values()))
    steps = max([t + span(block, first, last) + LAG for block, p, q, first, last, t in hops] + [d + pieces // 4 for d in due.values()] + [final + 1])
    return hops, slots, needs, due, steps, final


def ready_steps(pieces, hops, pairs):
    due, group = {}, pieces // 8
    for chip, m in pairs:
        z, c = chip
        ready = {(z, c): [1] * pieces}
        for block, p, q, first, last, t in hops:
            if q == chip:
                for s in range(span(block, first, last)):
                    j, more = paced(block, s, pieces)
                    for i in range(1 + more):
                        ready.setdefault(block, [None] * pieces)[first + j + i] = t + LAG + s
        both = [ready[m, c], ready[m, z]]
        for part in range(4):
            begin = part * (pieces // 4)
            due[chip, m, part] = 1 + max(b[begin + j] - j // group * group for b in both for j in range(pieces // 4))
    return due


def stream_kernel(pieces, coupling_pieces, f_ref, u_ref, x_ref, ub_ref, g_ref, send, send_u, near, near_u, recv,
                  recv_u, recv_near, recv_near_u, turn, blank, local, acc, a_buf, b_buf, stage, stage_u, zeros, flipped):
    hops, slots, needs, due, steps, final = plan(pieces, coupling_pieces)
    rows, width = f_ref.shape
    depth, narrow = u_ref.shape
    h, hu, quarter = rows // pieces, depth // coupling_pieces, width // 4
    tall = acc.shape[0]
    r, c = lax.axis_index("row"), lax.axis_index("col")
    k, z = lax.rem(r, 2), r // 2
    chip = z * 4 + c
    owner = z >= c

    def at_rows(slot, core, j):
        return pl.ds(pl.multiple_of((slot * 2 + core) * rows + j * h, h), h)

    def remote(src, dst, send_sem, recv_sem, row, col):
        return pltpu.make_async_remote_copy(
            src_ref=src, dst_ref=dst, send_sem=send_sem, recv_sem=recv_sem,
            device_id=(row, col), device_id_type=MESH,
        )

    def shapes(block, j):
        if block[0] != block[1]:
            return [(None, width)]
        part = (k * pieces + j) // (pieces // 2)
        return [(part == q, (q + 1) * quarter) for q in range(4)]

    def each(block, j, act):
        if block[0] == "u":
            act(None)
            return
        for condition, columns in shapes(block, j):
            if condition is None:
                act(columns)
            else:
                pl.when(condition)(functools.partial(act, columns))

    def hop_copy(hop, number, j, columns):
        block, p, q, first, last, t = hop
        if block[0] == "u":
            at = pl.ds(pl.multiple_of(j * hu, hu), hu)
            src = u_ref.at[at, :] if p == block[1:] else ub_ref.at[block[1] * 2 + k, at, :]
            return remote(src, ub_ref.at[block[1] * 2 + k, at, :], send_u.at[number, j], recv_u.at[block[1], j],
                          q[0] * 2 + k, q[1])
        cols = pl.ds(0, columns)
        if p == block:
            src = f_ref.at[pl.ds(pl.multiple_of(j * h, h), h), cols]
        else:
            src = x_ref.at[at_rows(slots[p][block], k, j), cols]
        slot = slots[q][block]
        return remote(src, x_ref.at[at_rows(slot, k, j), cols], send.at[number, j], recv.at[slot, j],
                      q[0] * 2 + k, q[1])

    def near_copy(slot, j, src=None):
        at = at_rows(slot, k, j)
        return remote(x_ref.at[at, :] if src is None else src, x_ref.at[at, :], near.at[slot, j],
                      recv_near.at[slot, j], z * 2 + 1 - k, c)

    def near_arrival(slot, j):
        ref = x_ref.at[at_rows(slot, 1 - k, j), :]
        return remote(ref, ref, near.at[slot, j], recv_near.at[slot, j], r, c)

    def near_copy_u(level, j, src=None):
        at = pl.ds(pl.multiple_of(j * hu, hu), hu)
        ref = ub_ref.at[level * 2 + k, at, :]
        return remote(ref if src is None else src, ref, near_u.at[level, j], recv_near_u.at[level, j],
                      z * 2 + 1 - k, c)

    def own_rows(j):
        return f_ref.at[pl.ds(pl.multiple_of(j * h, h), h), :]

    def own_rows_u(j):
        return u_ref.at[pl.ds(pl.multiple_of(j * hu, hu), hu), :]

    chips = [(a, b) for a in range(4) for b in range(4)]
    incoming = {chip_: [hop for hop in hops if hop[2] == chip_] for chip_ in chips}
    outgoing = {chip_: [] for chip_ in chips}
    count, count_u = {}, {}
    for hop in hops:
        counts = count_u if hop[0][0] == "u" else count
        number = counts.get(hop[1], 0)
        counts[hop[1]] = number + 1
        outgoing[hop[1]].append((hop, number))

    zeros[...] = jnp.zeros_like(zeros)

    def fill(slot, act):
        def one(j, carry):
            for condition, columns in shapes((0, 0), j):
                if columns < width:
                    @pl.when(condition)
                    def _():
                        act(pltpu.make_async_copy(
                            zeros.at[:, pl.ds(0, width - columns)],
                            x_ref.at[at_rows(slot, k, j), pl.ds(columns, width - columns)], blank.at[j]))
            return carry
        lax.fori_loop(0, pieces, one, 0)

    def fill_all(act):
        for place in chips:
            for block in needs[place]:
                if block[0] == block[1] and block != place:
                    pl.when(chip == place[0] * 4 + place[1])(functools.partial(fill, slots[place][block], act))

    def spread(j, carry):
        @pl.when(owner)
        def _():
            near_copy(z, j, own_rows(j)).start()
        return carry

    def spread_u(j, carry):
        near_copy_u(z, j, own_rows_u(j)).start()
        return carry

    def loads(m, slot_b, ago, into):
        cols = pl.ds(pl.multiple_of(k * tall, tall), tall)
        found = []
        for core in range(2):
            at_a = pl.ds(pl.multiple_of((m * 2 + core) * rows + ago * h, 2 * h), 2 * h)
            at_b = pl.ds(pl.multiple_of((slot_b * 2 + core) * rows + ago * h, 2 * h), 2 * h)
            half = pl.ds(core * 2 * h, 2 * h)
            found.append(pltpu.make_async_copy(x_ref.at[at_a, :], a_buf.at[into, half, :], local.at[2 + into * 4 + core]))
            found.append(pltpu.make_async_copy(x_ref.at[at_b, cols], b_buf.at[into, half, :], local.at[4 + into * 4 + core]))
        return found

    def multiply(into):
        for copy in loads(0, 0, 0, into):
            copy.wait()
        tile = min(256, tall)

        def rows_of(i, carry):
            at = pl.ds(pl.multiple_of(i * tile, tile), tile)
            acc[at, :] += lax.dot_general(
                b_buf[into, :, at], a_buf[into], (((0,), (0,)), ((), ())), preferred_element_type=jnp.float32)
            return carry
        lax.fori_loop(0, tall // tile, rows_of, 0)

    def flip():
        slot = slots[1, 0][G]
        tile = min(256, width)

        def turned(i, carry):
            at = pl.ds(pl.multiple_of(i * tile, tile), tile)
            flipped[at, :] = acc[:, at].T.astype(flipped.dtype)
            return carry
        lax.fori_loop(0, width // tile, turned, 0)
        cols = pl.ds(pl.multiple_of(k * tall, tall), tall)
        kept = []
        for half in range(2):
            at = pl.ds((slot * 2 + half) * rows, rows)
            kept.append(pltpu.make_async_copy(flipped.at[pl.ds(half * rows, rows), :], x_ref.at[at, cols],
                                              local.at[half]))
        for copy in kept:
            copy.start()
        for copy in kept:
            copy.wait()
        at = pl.ds(pl.multiple_of((slot * 2 + 1 - k) * rows, rows), rows)
        pass_on = remote(x_ref.at[at, cols], x_ref.at[at, cols], turn.at[0], turn.at[1], z * 2 + 1 - k, c)
        pass_on.start()
        pass_on.wait_send()
        at = pl.ds(pl.multiple_of((slot * 2 + k) * rows, rows), rows)
        cols = pl.ds(pl.multiple_of((1 - k) * tall, tall), tall)
        remote(x_ref.at[at, cols], x_ref.at[at, cols], turn.at[0], turn.at[1], r, c).wait_recv()

    def step(t, carry):
        for place in chips:
            @pl.when(chip == place[0] * 4 + place[1])
            def _():
                for hop in incoming[place]:
                    block, p, q, first, last, t0 = hop

                    def take(j):
                        each(block, j, lambda columns: hop_copy(hop, 0, j, columns).wait_recv())
                        if block[0] == "u":
                            near_copy_u(block[1], j).start()
                        elif block in needs[place]:
                            near_copy(slots[place][block], j).start()

                    @pl.when((t >= t0 + LAG) & (t < t0 + LAG + span(block, first, last)))
                    def _():
                        j, more = paced(block, t - (t0 + LAG), pieces)
                        take(first + j)
                        if more is not False:
                            pl.when(more)(functools.partial(take, first + j + 1))
                for hop, number in outgoing[place]:
                    block, p, q, first, last, t0 = hop

                    def give(j):
                        each(block, j, lambda columns: hop_copy(hop, number, j, columns).start())

                    @pl.when((t >= t0) & (t < t0 + span(block, first, last)))
                    def _():
                        j, more = paced(block, t - t0, pieces)
                        give(first + j)
                        if more is not False:
                            pl.when(more)(functools.partial(give, first + j + 1))

        def consume(entry, carry):
            pending, into = carry
            begin = jnp.int32(-1000)
            for index in range(16):
                begin = jnp.where(entry == index, begins[index], begin)
            m, part = entry // 4, lax.rem(entry, 4)
            past = t - begin
            ready = (past >= 0) & (past < pieces // 4) & (lax.rem(past, 2) == 0)

            @pl.when(ready)
            def _():
                ago = past + part * (pieces // 4)
                slot_b = jnp.where(c == z, m, 4 + m)
                for i in range(2):
                    near_arrival(m, ago + i).wait_recv()

                    @pl.when(c != z)
                    def _():
                        near_arrival(slot_b, ago + i).wait_recv()
                for copy in loads(m, slot_b, ago, 1 - into):
                    copy.start()
                pl.when(pending == 1)(functools.partial(multiply, into))
            return jnp.where(ready, 1, pending), jnp.where(ready, 1 - into, into)
        pending, into = lax.fori_loop(0, 16, consume, carry)
        last = (chip == 4) & (t == final)

        @pl.when(last)
        def _():
            pl.when(pending == 1)(functools.partial(multiply, into))
            flip()
        return jnp.where(last, 0, pending), into

    begins = []
    for index in range(16):
        begin = jnp.int32(-1000)
        for place in chips:
            if (place, index // 4, index % 4) in due:
                begin = jnp.where(chip == place[0] * 4 + place[1], due[place, index // 4, index % 4], begin)
        begins.append(begin)

    own = pltpu.make_async_copy(f_ref, stage, local.at[0])
    keep = pltpu.make_async_copy(stage, x_ref.at[pl.ds(pl.multiple_of((z * 2 + k) * rows, rows), rows), :], local.at[0])
    own_u = pltpu.make_async_copy(u_ref, stage_u, local.at[1])
    keep_u = pltpu.make_async_copy(stage_u, ub_ref.at[r], local.at[1])
    pl.when(owner)(own.start)
    own_u.start()
    lax.fori_loop(0, pieces, spread, 0)
    lax.fori_loop(0, coupling_pieces, spread_u, 0)
    fill_all(lambda copy: copy.start())
    acc[...] = jnp.zeros_like(acc)

    @pl.when(owner)
    def _():
        own.wait()
        keep.start()
    own_u.wait()
    keep_u.start()
    fill_all(lambda copy: copy.wait())
    pl.when(owner)(keep.wait)
    keep_u.wait()
    pending, turned_to = lax.fori_loop(0, steps, step, (jnp.int32(0), jnp.int32(0)))
    pl.when(pending == 1)(functools.partial(multiply, turned_to))

    @pl.when(chip == 1)
    def _():
        at = pl.ds(pl.multiple_of((slots[0, 1][G] * 2 + k) * rows, rows), rows)
        load = pltpu.make_async_copy(x_ref.at[at, :], stage, local.at[0])
        load.start()
        load.wait()
        tile = min(128, tall)

        def widen(i, carry):
            at = pl.ds(pl.multiple_of(i * tile, tile), tile)
            acc[at, :] = stage[at, :].astype(jnp.float32)
            return carry
        lax.fori_loop(0, tall // tile, widen, 0)
    out = pltpu.make_async_copy(acc, g_ref, local.at[0])
    out.start()

    def settle(j, carry):
        @pl.when(owner)
        def _():
            near_copy(z, j, own_rows(j)).wait_send()
        return carry
    lax.fori_loop(0, pieces, settle, 0)

    def settle_u(j, carry):
        for level in range(4):
            near_copy_u(level, j).wait_send()
            at = pl.ds(pl.multiple_of(j * hu, hu), hu)
            ref = ub_ref.at[level * 2 + 1 - k, at, :]
            remote(ref, ref, near_u.at[level, j], recv_near_u.at[level, j], r, c).wait_recv()
        return carry
    lax.fori_loop(0, coupling_pieces, settle_u, 0)
    for place in chips:
        @pl.when(chip == place[0] * 4 + place[1])
        def _():
            for hop, number in outgoing[place]:
                def sent(j, carry):
                    each(hop[0], j, lambda columns: hop_copy(hop, number, j, columns).wait_send())
                    return carry
                lax.fori_loop(hop[3], hop[4], sent, 0)
            for hop in incoming[place]:
                if hop[0][0] != "u" and hop[0] in needs[place]:
                    def passed(j, carry):
                        near_copy(slots[place][hop[0]], j).wait_send()
                        return carry
                    lax.fori_loop(hop[3], hop[4], passed, 0)
    out.wait()


def stream(factor, coupling, n_row, n_col):
    rows, width = factor.shape
    depth, narrow = coupling.shape
    pieces, coupling_pieces = 16, 4
    hops = plan(pieces, coupling_pieces)[0]
    out_count = max(sum(hop[1] == chip and hop[0][0] != "u" for hop in hops) for chip in {h[1] for h in hops})
    out_count_u = max(sum(hop[1] == chip and hop[0][0] == "u" for hop in hops) for chip in {h[1] for h in hops})
    tall = width // 2
    h = rows // pieces
    dma = pltpu.SemaphoreType.DMA
    return pl.pallas_call(
        functools.partial(stream_kernel, pieces, coupling_pieces),
        out_shape=(
            jax.ShapeDtypeStruct((8 * 2 * rows, width), factor.dtype),
            jax.ShapeDtypeStruct((n_row, depth, narrow), coupling.dtype),
            jax.ShapeDtypeStruct((tall, width), jnp.float32),
        ),
        in_specs=[pl.BlockSpec(memory_space=pl.ANY)] * 2,
        out_specs=[pl.BlockSpec(memory_space=pl.ANY)] * 3,
        scratch_shapes=[
            dma((out_count, pieces)),
            dma((out_count_u, coupling_pieces)),
            dma((8, pieces)),
            dma((4, coupling_pieces)),
            dma((8, pieces)),
            dma((4, coupling_pieces)),
            dma((8, pieces)),
            dma((4, coupling_pieces)),
            dma((2,)),
            dma((pieces,)),
            dma((12,)),
            pltpu.VMEM((tall, width), jnp.float32),
            pltpu.VMEM((2, 4 * h, width), factor.dtype),
            pltpu.VMEM((2, 4 * h, tall), factor.dtype),
            pltpu.VMEM((rows, width), factor.dtype),
            pltpu.VMEM((depth, narrow), coupling.dtype),
            pltpu.VMEM((h, width), factor.dtype),
            pltpu.VMEM((width, tall), factor.dtype),
        ],
        compiler_params=pltpu.CompilerParams(has_side_effects=True, vmem_limit_bytes=63 * 1024 * 1024),
        cost_estimate=pl.CostEstimate(flops=0, bytes_accessed=rows * width * 64, transcendentals=0),
    )(factor, coupling)


def child_kernel(n_col, g_ref, u_ref, part_ref, other_ref, send, recv, local, whole, held, out):
    r, c = lax.axis_index("row"), lax.axis_index("col")
    tile = held.shape[1]
    count, _, narrow = whole.shape
    cores = count // n_col
    tiles = g_ref.shape[0] // tile

    def rows(i):
        return pl.ds(pl.multiple_of(i * tile, tile), tile)

    def load(i, into):
        return pltpu.make_async_copy(g_ref.at[rows(i), :], held.at[into], local.at[into])

    def copies(i):
        found = []
        for d in range(1, n_col):
            ct = lax.rem(c + d, n_col)
            found.append(pltpu.make_async_remote_copy(
                src_ref=part_ref.at[ct, rows(i), :],
                dst_ref=other_ref.at[d - 1, rows(i), :],
                send_sem=send.at[d - 1, i],
                recv_sem=recv.at[d - 1, i],
                device_id=(r, ct),
                device_id_type=MESH,
            ))
        return found

    def fetch(q):
        return pltpu.make_async_copy(u_ref.at[q], whole.at[q], local.at[3 + q])

    load(0, 0).start()
    for q in range(count):
        fetch(q).start()

    def one(i, carry):
        into = lax.rem(i, 2)
        load(i, into).wait()

        @pl.when(i + 1 < tiles)
        def _():
            load(i + 1, 1 - into).start()
        rounded = held[into].astype(whole.dtype)
        for q in range(count):
            pl.when(i == 0)(fetch(q).wait)
            product = jnp.dot(rounded, whole[q], preferred_element_type=jnp.float32)
            out[q // cores, :, pl.ds(q % cores * narrow, narrow)] = product.astype(out.dtype)
        keep = pltpu.make_async_copy(out, part_ref.at[:, rows(i), :], local.at[2])
        keep.start()
        keep.wait()
        for copy in copies(i):
            copy.start()
        return carry
    lax.fori_loop(0, tiles, one, 0)

    def settle(i, carry):
        for copy in copies(i):
            copy.wait()
        return carry
    lax.fori_loop(0, tiles, settle, 0)


def child_parts(gram, coupling, n_col):
    tall, width = gram.shape
    count, depth, narrow = coupling.shape
    tile = min(128, tall)
    wide = count * narrow // n_col
    dma = pltpu.SemaphoreType.DMA
    return pl.pallas_call(
        functools.partial(child_kernel, n_col),
        out_shape=(
            jax.ShapeDtypeStruct((n_col, tall, wide), coupling.dtype),
            jax.ShapeDtypeStruct((n_col - 1, tall, wide), coupling.dtype),
        ),
        in_specs=[pl.BlockSpec(memory_space=pl.ANY)] * 2,
        out_specs=[pl.BlockSpec(memory_space=pl.ANY)] * 2,
        scratch_shapes=[
            dma((n_col - 1, tall // tile)),
            dma((n_col - 1, tall // tile)),
            dma((3 + count,)),
            pltpu.VMEM((count, depth, narrow), coupling.dtype),
            pltpu.VMEM((2, tile, width), gram.dtype),
            pltpu.VMEM((n_col, tile, wide), coupling.dtype),
        ],
        compiler_params=pltpu.CompilerParams(has_side_effects=True, vmem_limit_bytes=63 * 1024 * 1024),
    )(gram, coupling)


def finish_kernel(c_ref, g_ref, own_ref, other_ref, member_ref, gram_ref, child_ref):
    gram_ref[...] = g_ref[...]
    total = own_ref[0].astype(jnp.float32)
    for d in range(other_ref.shape[0]):
        total = total + other_ref[d].astype(jnp.float32)
    child_ref[...] = jnp.where(member_ref[...] != 0, -total.T, jnp.float32(0.0))


def finish(gram, own, other, member, col_index):
    tall, width = gram.shape
    wide = own.shape[2]
    tile = min(256, tall)
    return pl.pallas_call(
        finish_kernel,
        grid_spec=pltpu.PrefetchScalarGridSpec(
            num_scalar_prefetch=1,
            grid=(tall // tile,),
            in_specs=[
                pl.BlockSpec((tile, width), lambda i, c: (i, 0)),
                pl.BlockSpec((1, tile, wide), lambda i, c: (c[0], i, 0)),
                pl.BlockSpec((other.shape[0], tile, wide), lambda i, c: (0, i, 0)),
                pl.BlockSpec((1, tile), lambda i, c: (0, i)),
            ],
            out_specs=(
                pl.BlockSpec((tile, width), lambda i, c: (i, 0)),
                pl.BlockSpec((wide, tile), lambda i, c: (0, i)),
            ),
        ),
        out_shape=(
            jax.ShapeDtypeStruct((tall, width), jnp.float32),
            jax.ShapeDtypeStruct((wide, tall), jnp.float32),
        ),
        compiler_params=pltpu.CompilerParams(vmem_limit_bytes=63 * 1024 * 1024),
        cost_estimate=pl.CostEstimate(flops=0, bytes_accessed=tall * width * 12, transcendentals=0),
    )(jnp.reshape(col_index, (1,)), gram, own, other, member)


def exchange_kernel(n_col, part_ref, out_ref, send, recv):
    r, c = lax.axis_index("row"), lax.axis_index("col")
    depth = out_ref.shape[1]
    started = []
    for d in range(1, n_col):
        ct = lax.rem(c + d, n_col)
        copy = pltpu.make_async_remote_copy(
            src_ref=part_ref.at[pl.ds(pl.multiple_of(ct * depth, depth), depth), :],
            dst_ref=out_ref.at[d - 1],
            send_sem=send.at[d - 1],
            recv_sem=recv.at[d - 1],
            device_id=(r, ct),
            device_id_type=MESH,
        )
        copy.start()
        started.append(copy)
    for copy in started:
        copy.wait()


def exchange(part, n_col):
    total, width = part.shape
    dma = pltpu.SemaphoreType.DMA
    return pl.pallas_call(
        functools.partial(exchange_kernel, n_col),
        out_shape=jax.ShapeDtypeStruct((n_col - 1, total // n_col, width), part.dtype),
        in_specs=[pl.BlockSpec(memory_space=pl.ANY)],
        out_specs=pl.BlockSpec(memory_space=pl.ANY),
        scratch_shapes=[dma((n_col - 1,)), dma((n_col - 1,))],
        compiler_params=pltpu.CompilerParams(has_side_effects=True),
    )(part)


def general(n_row, n_col, factor, coupling):
    rows_here = factor.shape[0]
    row_index, col_index = lax.axis_index("row"), lax.axis_index("col")
    cores = n_row // n_col
    below, partner = gather(factor, n_row, n_col)
    coupling_full = lax.all_gather(coupling, "row", axis=1, tiled=True)

    def product(level, below, partner):
        first = level * rows_here * cores
        return lax.dot_general(
            partner[first:], below[first:], (((0,), (0,)), ((), ())), preferred_element_type=jnp.float32
        )

    gram = lax.switch(
        jnp.maximum(row_index // cores, col_index),
        [functools.partial(product, level) for level in range(n_col)],
        below,
        partner,
    )
    rounded = gram.astype(jnp.bfloat16)
    part = lax.dot_general(
        coupling_full, rounded, (((0,), (1,)), ((), ())), preferred_element_type=jnp.float32
    ).astype(jnp.bfloat16)
    return gram, part


def body(n_row, n_col, factor, sel_tiles, coupling):
    rows_here = factor.shape[0]
    row_index, col_index = lax.axis_index("row"), lax.axis_index("col")
    cores = n_row // n_col
    global_rows = row_index * rows_here + jnp.arange(rows_here, dtype=jnp.int32)
    member = jnp.any((global_rows // TILE)[:, None] == sel_tiles[None, :], axis=1)
    if (n_row, n_col) == (8, 4):
        _, pieces, gram = stream(factor, coupling, n_row, n_col)
        own, other = child_parts(gram, pieces, n_col)
        return finish(gram, own, other, member.astype(jnp.int32)[None, :], col_index)
    gram, part = general(n_row, n_col, factor, coupling)
    depth = part.shape[0] // n_col
    arrived = exchange(part, n_col)
    summed = lax.dynamic_slice_in_dim(part, col_index * depth, depth, 0).astype(jnp.float32)
    for d in range(n_col - 1):
        summed = summed + arrived[d].astype(jnp.float32)
    child = jnp.where(member[None, :], -summed, jnp.float32(0.0))
    return (gram, child)


def solution(mesh):
    placed = (P("row", "col"), P(), P("col", "row"))
    return jax.shard_map(
        functools.partial(body, mesh.shape["row"], mesh.shape["col"]),
        mesh=mesh,
        in_specs=placed,
        out_specs=(P("row", "col"), P("col", "row")),
        check_vma=False,
    )
```

```python
import functools
import math

import jax
import jax.numpy as jnp
from jax import lax
from jax.experimental import pallas as pl
from jax.experimental.pallas import tpu as pltpu
from jax.sharding import PartitionSpec as P

TILE = 128
MESH = pl.DeviceIdType.MESH
SKEW = 2


def gather_kernel(dims, f_ref, a_ref, b_ref, recv_a, recv_b, send_z, send_p, send_b, send_f, local_a, stage):
    levels, wide, high, cores, chunks = dims
    rows, width = f_ref.shape
    narrow = width // cores
    h = rows // chunks
    r, c = lax.axis_index("row"), lax.axis_index("col")
    k, z = lax.rem(r, cores), r // cores
    x, y = lax.rem(c, wide), c // wide
    x0, y0 = lax.rem(z, wide), z // wide
    source = c == z

    def chunk_rows(block, j):
        return pl.ds(pl.multiple_of(block * rows + j * h, h), h)

    def remote(src, dst, send, recv, row, col):
        return pltpu.make_async_remote_copy(
            src_ref=src, dst_ref=dst, send_sem=send, recv_sem=recv,
            device_id=(row, col), device_id_type=MESH,
        )

    def copies(t, j):
        m = z + t
        inside = m < levels
        has = inside & (m >= c)
        block = m * cores + k
        at = chunk_rows(block, j)
        if t == 0:
            def src(cols):
                return f_ref.at[pl.ds(j * h, h), cols]
        else:
            def src(cols):
                return a_ref.at[at, cols]
        everything = pl.ds(0, width)
        found = []
        for kk in range(cores):
            piece = src(pl.ds(kk * narrow, narrow))
            into = b_ref.at[at, :]
            for dx in range(1, wide):
                xt = lax.rem(x + dx, wide)
                found.append((
                    source & inside & (m >= y * wide + xt),
                    remote(piece, into, send_b.at[kk, dx, t, j], recv_b.at[block, j],
                           z * cores + kk, y * wide + xt),
                    False,
                ))
            for dy in range(1, high):
                yt = lax.rem(y + dy, high)
                found.append((
                    source & inside & (m >= yt * wide),
                    remote(piece, into, send_b.at[kk, wide - 1 + dy, t, j], recv_b.at[block, j],
                           z * cores + kk, yt * wide + x),
                    False,
                ))
        found.append((
            has & (z > 0),
            remote(src(everything), a_ref.at[at, :], send_z.at[t, j], recv_a.at[block, j],
                   r - cores, c),
            False,
        ))
        for dk in range(1, cores):
            other = z * cores + lax.rem(k + dk, cores)
            found.append((
                has,
                remote(src(everything), a_ref.at[at, :], send_p.at[dk, t, j], recv_a.at[block, j], other, c),
                False,
            ))
        for kk in range(cores):
            piece = src(pl.ds(kk * narrow, narrow))
            into = b_ref.at[at, :]
            found.append((
                source & inside & (k != kk),
                remote(piece, into, send_b.at[kk, 0, t, j], recv_b.at[block, j], z * cores + kk, c),
                False,
            ))
        return found

    def keep(t, j):
        m = z + t
        at = chunk_rows(m * cores + k, j)
        here = f_ref.at[pl.ds(j * h, h), :] if t == 0 else a_ref.at[at, :]
        inside = (m < levels) & (m >= c)

        @pl.when(inside if t == 0 else inside & source)
        def _():
            load = pltpu.make_async_copy(here, stage, local_a.at[0])
            load.start()
            load.wait()
            if t == 0:
                pltpu.make_async_copy(stage, a_ref.at[at, :], local_a.at[1]).start()
            for kk in range(cores):
                @pl.when(source & (k == kk))
                def _():
                    store = pltpu.make_async_copy(
                        stage.at[:, pl.ds(kk * narrow, narrow)], b_ref.at[at, :], local_a.at[2]
                    )
                    store.start()
                    store.wait()
            if t == 0:
                pltpu.make_async_copy(stage, a_ref.at[at, :], local_a.at[1]).wait()

    def forwards(t, j, p):
        m = z + t
        block = m * cores + p
        part = b_ref.at[chunk_rows(block, j), :]
        mine = (x == x0) & (y != y0) & (m < levels)
        found = []
        for dx in range(1, wide):
            xt = lax.rem(x + dx, wide)
            found.append((
                mine & (m >= y * wide + xt),
                remote(part, part, send_f.at[dx, p, t, j], recv_b.at[block, j], r, y * wide + xt),
            ))
        return mine & (m >= y * wide), found

    def arrived(ref, sem):
        remote(ref, ref, send_z.at[0, 0], sem, r, c).wait_recv()

    def step(t, j):
        m = z + t
        block = m * cores + k
        if t > 0:
            @pl.when((m < levels) & (m >= c))
            def _():
                arrived(a_ref.at[chunk_rows(block, j), :], recv_a.at[block, j])
        for condition, copy, _ in copies(t, j):
            pl.when(condition)(copy.start)
        keep(t, j)

    def forward(t, j):
        for p in range(cores):
            due, found = forwards(t, j, p)
            block = (z + t) * cores + p

            @pl.when(due)
            def _():
                arrived(b_ref.at[chunk_rows(block, j), :], recv_b.at[block, j])
            for condition, copy in found:
                pl.when(condition)(copy.start)

    order = [(t, j) for t in range(levels) for j in range(chunks)]
    for n, (t, j) in enumerate(order):
        step(t, j)
        if n >= SKEW:
            forward(*order[n - SKEW])
    for t, j in order[len(order) - SKEW:]:
        forward(t, j)

    for t, j in order:
        m = z + t
        inside = m < levels
        for dk in range(1, cores):
            block = m * cores + lax.rem(k + dk, cores)

            @pl.when(inside & (m >= c))
            def _():
                arrived(a_ref.at[chunk_rows(block, j), :], recv_a.at[block, j])

            @pl.when(inside & source)
            def _():
                arrived(b_ref.at[chunk_rows(block, j), :], recv_b.at[block, j])
        for p in range(cores):
            block = m * cores + p

            @pl.when(inside & (x != x0) & (m >= c))
            def _():
                arrived(b_ref.at[chunk_rows(block, j), :], recv_b.at[block, j])
        for condition, copy, local in copies(t, j):
            pl.when(condition)(copy.wait if local else copy.wait_send)
        for p in range(cores):
            for condition, copy in forwards(t, j, p)[1]:
                pl.when(condition)(copy.wait_send)


def gather(factor, n_row, n_col):
    rows, width = factor.shape
    cores = n_row // n_col
    wide = next(w for w in range(math.isqrt(n_col), 0, -1) if n_col % w == 0)
    high = n_col // wide
    levels = n_col
    chunks = max(1, 32 // n_row)
    dma = pltpu.SemaphoreType.DMA
    whole = rows * n_row
    return pl.pallas_call(
        functools.partial(gather_kernel, (levels, wide, high, cores, chunks)),
        out_shape=(
            jax.ShapeDtypeStruct((whole, width), factor.dtype),
            jax.ShapeDtypeStruct((whole, width // cores), factor.dtype),
        ),
        in_specs=[pl.BlockSpec(memory_space=pl.ANY)],
        out_specs=(pl.BlockSpec(memory_space=pl.ANY), pl.BlockSpec(memory_space=pl.ANY)),
        scratch_shapes=[
            dma((n_row, chunks)),
            dma((n_row, chunks)),
            dma((levels, chunks)),
            dma((cores, levels, chunks)),
            dma((cores, wide + high, levels, chunks)),
            dma((wide, cores, levels, chunks)),
            dma((3,)),
            pltpu.VMEM((rows // chunks, width), factor.dtype),
        ],
        compiler_params=pltpu.CompilerParams(has_side_effects=True),
        cost_estimate=pl.CostEstimate(flops=0, bytes_accessed=whole * width * 32, transcendentals=0),
    )(factor)


LAG = 2
G = ("g", 1, 0)


def block_flows(pieces):
    half, cut = pieces // 2, 5 * pieces // 8
    found = []

    def add(block, source, hops, first=0, last=pieces):
        found.append((block, source, hops, first, last))

    add((3, 3), (3, 3), [((3, 3), (2, 3)), ((2, 3), (1, 3)), ((1, 3), (0, 3)), ((3, 3), (3, 1)), ((3, 3), (3, 2)),
                         ((3, 2), (3, 0))])
    add((3, 2), (3, 2), [((3, 2), (2, 2)), ((2, 2), (2, 3)), ((2, 3), (2, 1)), ((2, 2), (2, 0)), ((2, 2), (1, 2)),
                         ((1, 2), (0, 2))])
    add((3, 1), (3, 1), [((3, 1), (2, 1)), ((2, 1), (2, 0)), ((2, 0), (1, 0)), ((1, 0), (1, 1)), ((1, 1), (1, 3)),
                         ((1, 0), (1, 2))], 0, cut)
    add((3, 1), (3, 1), [((3, 1), (2, 1)), ((2, 1), (1, 1)), ((1, 1), (1, 3)), ((1, 3), (1, 2)), ((1, 2), (1, 0))],
        cut, pieces)
    add((3, 0), (3, 0), [((3, 0), (2, 0)), ((2, 0), (2, 1)), ((2, 1), (2, 3)), ((2, 3), (1, 3)), ((1, 3), (1, 2)),
                         ((1, 2), (1, 0)), ((1, 3), (0, 3)), ((0, 3), (0, 2)), ((0, 2), (0, 0))])
    around = [((1, 0), (1, 1)), ((1, 1), (0, 1)), ((0, 1), (0, 0)), ((0, 0), (0, 2))]
    add((2, 0), (2, 0), [((2, 0), (1, 0))] + around, 0, 3 * pieces // 4)
    add((2, 0), (2, 0), [((2, 0), (2, 2)), ((2, 2), (1, 2)), ((1, 2), (1, 0))] + around, 3 * pieces // 4, pieces)
    add((1, 0), (1, 0), [((1, 0), (0, 0))])
    add((2, 1), (2, 1), [((2, 1), (1, 1)), ((1, 1), (1, 0)), ((1, 0), (1, 2))])
    add((1, 1), (1, 1), [((1, 1), (1, 0))])
    add((2, 2), (2, 2), [((2, 2), (2, 3)), ((2, 3), (2, 1)), ((2, 2), (2, 0)), ((2, 2), (1, 2)), ((1, 2), (0, 2))])
    add(G, (1, 0), [((1, 0), (0, 0)), ((0, 0), (0, 1))], 0, half)
    add(G, (1, 0), [((1, 0), (1, 1)), ((1, 1), (0, 1))], half, pieces)
    return found


def coupling_flows(pieces):
    found = []
    for c in range(4):
        for z in range(4):
            hops = [((a, c), (a - 1, c)) for a in range(z, 0, -1)] + [((a, c), (a + 1, c)) for a in range(z, 3)]
            found.append((("u", z, c), (z, c), hops, 0, pieces))
    return found


def paced(block, s, pieces):
    if block[0] != block[1]:
        return s, False
    unit = pieces // 4
    late = s - unit
    if isinstance(s, int):
        turn = late % 3
        slow = pieces // 2 + late // 3 * 4 + turn + (turn > 0)
        return (2 * s, True) if s < unit else (slow, turn == 0)
    turn = lax.rem(late, 3)
    slow = pieces // 2 + late // 3 * 4 + turn + jnp.where(turn > 0, 1, 0)
    return jnp.where(s < unit, 2 * s, slow), (s < unit) | (turn == 0)


def span(block, first, last):
    count = last - first
    return count // 4 + count // 8 * 3 if block[0] == block[1] else count


ORDER = [6, 24, 14, 15, 3, 9, 25, 13, 7, 17, 5, 4, 8, 26, 1, 2, 20, 10, 19, 0, 28, 16, 18, 21, 12, 11, 23, 22, 27]


@functools.cache
def plan(pieces, coupling_pieces):
    flows = block_flows(pieces) + coupling_flows(coupling_pieces)
    chips = [(z, c) for z in range(4) for c in range(4)]
    pairs = [(chip, m) for chip in chips if chip != (0, 1) for m in range(max(chip), 4)]
    busy, hops, due = {}, [], {}
    final = None
    for index in ORDER:
        block, source, route, first, last = flows[index]
        if block == G and final is None:
            due = ready_steps(pieces, hops, pairs)
            final = max(d for key, d in due.items() if key[0] == (1, 0)) + pieces // 4
        n, at = span(block, first, last), {source: final + 1 if block == G else 0}
        for p, q in route:
            t, used = at[p], busy.setdefault((p, q), [])
            while any(t < e and s < t + n for s, e in used):
                t += 1
            used.append((t, t + n))
            at[q] = t + LAG
            hops.append((block, p, q, first, last, t))
    slots = {chip: {} for chip in chips}
    needs = {chip: set() for chip in chips}
    for chip, m in pairs:
        z, c = chip
        slots[chip][m, c] = m
        needs[chip].add((m, c))
        if c != z:
            slots[chip][m, z] = 4 + m
            needs[chip].add((m, z))
    for block, p, q, first, last, t in hops:
        for chip in (p, q):
            if block[0] != "u" and block not in slots[chip] and block != chip:
                slots[chip][block] = min(set(range(8)) - set(slots[chip].values()))
    steps = max([t + span(block, first, last) + LAG for block, p, q, first, last, t in hops] + [d + pieces // 4 for d in due.values()] + [final + 1])
    return hops, slots, needs, due, steps, final


def ready_steps(pieces, hops, pairs):
    due, group = {}, pieces // 8
    for chip, m in pairs:
        z, c = chip
        ready = {(z, c): [1] * pieces}
        for block, p, q, first, last, t in hops:
            if q == chip:
                for s in range(span(block, first, last)):
                    j, more = paced(block, s, pieces)
                    for i in range(1 + more):
                        ready.setdefault(block, [None] * pieces)[first + j + i] = t + LAG + s
        both = [ready[m, c], ready[m, z]]
        for part in range(4):
            begin = part * (pieces // 4)
            due[chip, m, part] = 1 + max(b[begin + j] - j // group * group for b in both for j in range(pieces // 4))
    return due


def stream_kernel(pieces, coupling_pieces, f_ref, u_ref, x_ref, ub_ref, g_ref, send, send_u, near, near_u, recv,
                  recv_u, recv_near, recv_near_u, turn, blank, local, acc, a_buf, b_buf, stage, stage_u, zeros, flipped):
    hops, slots, needs, due, steps, final = plan(pieces, coupling_pieces)
    rows, width = f_ref.shape
    depth, narrow = u_ref.shape
    h, hu, quarter = rows // pieces, depth // coupling_pieces, width // 4
    tall = acc.shape[0]
    r, c = lax.axis_index("row"), lax.axis_index("col")
    k, z = lax.rem(r, 2), r // 2
    chip = z * 4 + c
    owner = z >= c

    def at_rows(slot, core, j):
        return pl.ds(pl.multiple_of((slot * 2 + core) * rows + j * h, h), h)

    def remote(src, dst, send_sem, recv_sem, row, col):
        return pltpu.make_async_remote_copy(
            src_ref=src, dst_ref=dst, send_sem=send_sem, recv_sem=recv_sem,
            device_id=(row, col), device_id_type=MESH,
        )

    def shapes(block, j):
        if block[0] != block[1]:
            return [(None, width)]
        part = (k * pieces + j) // (pieces // 2)
        return [(part == q, (q + 1) * quarter) for q in range(4)]

    def each(block, j, act):
        if block[0] == "u":
            act(None)
            return
        for condition, columns in shapes(block, j):
            if condition is None:
                act(columns)
            else:
                pl.when(condition)(functools.partial(act, columns))

    def hop_copy(hop, number, j, columns):
        block, p, q, first, last, t = hop
        if block[0] == "u":
            at = pl.ds(pl.multiple_of(j * hu, hu), hu)
            src = u_ref.at[at, :] if p == block[1:] else ub_ref.at[block[1] * 2 + k, at, :]
            return remote(src, ub_ref.at[block[1] * 2 + k, at, :], send_u.at[number, j], recv_u.at[block[1], j],
                          q[0] * 2 + k, q[1])
        cols = pl.ds(0, columns)
        if p == block:
            src = f_ref.at[pl.ds(pl.multiple_of(j * h, h), h), cols]
        else:
            src = x_ref.at[at_rows(slots[p][block], k, j), cols]
        slot = slots[q][block]
        return remote(src, x_ref.at[at_rows(slot, k, j), cols], send.at[number, j], recv.at[slot, j],
                      q[0] * 2 + k, q[1])

    def near_copy(slot, j, src=None):
        at = at_rows(slot, k, j)
        return remote(x_ref.at[at, :] if src is None else src, x_ref.at[at, :], near.at[slot, j],
                      recv_near.at[slot, j], z * 2 + 1 - k, c)

    def near_arrival(slot, j):
        ref = x_ref.at[at_rows(slot, 1 - k, j), :]
        return remote(ref, ref, near.at[slot, j], recv_near.at[slot, j], r, c)

    def near_copy_u(level, j, src=None):
        at = pl.ds(pl.multiple_of(j * hu, hu), hu)
        ref = ub_ref.at[level * 2 + k, at, :]
        return remote(ref if src is None else src, ref, near_u.at[level, j], recv_near_u.at[level, j],
                      z * 2 + 1 - k, c)

    def own_rows(j):
        return f_ref.at[pl.ds(pl.multiple_of(j * h, h), h), :]

    def own_rows_u(j):
        return u_ref.at[pl.ds(pl.multiple_of(j * hu, hu), hu), :]

    chips = [(a, b) for a in range(4) for b in range(4)]
    incoming = {chip_: [hop for hop in hops if hop[2] == chip_] for chip_ in chips}
    outgoing = {chip_: [] for chip_ in chips}
    count, count_u = {}, {}
    for hop in hops:
        counts = count_u if hop[0][0] == "u" else count
        number = counts.get(hop[1], 0)
        counts[hop[1]] = number + 1
        outgoing[hop[1]].append((hop, number))

    zeros[...] = jnp.zeros_like(zeros)

    def fill(slot, act):
        def one(j, carry):
            for condition, columns in shapes((0, 0), j):
                if columns < width:
                    @pl.when(condition)
                    def _():
                        act(pltpu.make_async_copy(
                            zeros.at[:, pl.ds(0, width - columns)],
                            x_ref.at[at_rows(slot, k, j), pl.ds(columns, width - columns)], blank.at[j]))
            return carry
        lax.fori_loop(0, pieces, one, 0)

    def fill_all(act):
        for place in chips:
            for block in needs[place]:
                if block[0] == block[1] and block != place:
                    pl.when(chip == place[0] * 4 + place[1])(functools.partial(fill, slots[place][block], act))

    def spread(j, carry):
        @pl.when(owner)
        def _():
            near_copy(z, j, own_rows(j)).start()
        return carry

    def spread_u(j, carry):
        near_copy_u(z, j, own_rows_u(j)).start()
        return carry

    def loads(m, slot_b, ago, into):
        cols = pl.ds(pl.multiple_of(k * tall, tall), tall)
        found = []
        for core in range(2):
            at_a = pl.ds(pl.multiple_of((m * 2 + core) * rows + ago * h, 2 * h), 2 * h)
            at_b = pl.ds(pl.multiple_of((slot_b * 2 + core) * rows + ago * h, 2 * h), 2 * h)
            half = pl.ds(core * 2 * h, 2 * h)
            found.append(pltpu.make_async_copy(x_ref.at[at_a, :], a_buf.at[into, half, :], local.at[2 + into * 4 + core]))
            found.append(pltpu.make_async_copy(x_ref.at[at_b, cols], b_buf.at[into, half, :], local.at[4 + into * 4 + core]))
        return found

    def multiply(into):
        for copy in loads(0, 0, 0, into):
            copy.wait()
        tile = min(256, tall)

        def rows_of(i, carry):
            at = pl.ds(pl.multiple_of(i * tile, tile), tile)
            acc[at, :] += lax.dot_general(
                b_buf[into, :, at], a_buf[into], (((0,), (0,)), ((), ())), preferred_element_type=jnp.float32)
            return carry
        lax.fori_loop(0, tall // tile, rows_of, 0)

    def flip():
        slot = slots[1, 0][G]
        tile = min(256, width)

        def turned(i, carry):
            at = pl.ds(pl.multiple_of(i * tile, tile), tile)
            flipped[at, :] = acc[:, at].T.astype(flipped.dtype)
            return carry
        lax.fori_loop(0, width // tile, turned, 0)
        cols = pl.ds(pl.multiple_of(k * tall, tall), tall)
        kept = []
        for half in range(2):
            at = pl.ds((slot * 2 + half) * rows, rows)
            kept.append(pltpu.make_async_copy(flipped.at[pl.ds(half * rows, rows), :], x_ref.at[at, cols],
                                              local.at[half]))
        for copy in kept:
            copy.start()
        for copy in kept:
            copy.wait()
        at = pl.ds(pl.multiple_of((slot * 2 + 1 - k) * rows, rows), rows)
        pass_on = remote(x_ref.at[at, cols], x_ref.at[at, cols], turn.at[0], turn.at[1], z * 2 + 1 - k, c)
        pass_on.start()
        pass_on.wait_send()
        at = pl.ds(pl.multiple_of((slot * 2 + k) * rows, rows), rows)
        cols = pl.ds(pl.multiple_of((1 - k) * tall, tall), tall)
        remote(x_ref.at[at, cols], x_ref.at[at, cols], turn.at[0], turn.at[1], r, c).wait_recv()

    def step(t, carry):
        for place in chips:
            @pl.when(chip == place[0] * 4 + place[1])
            def _():
                for hop in incoming[place]:
                    block, p, q, first, last, t0 = hop

                    def take(j):
                        each(block, j, lambda columns: hop_copy(hop, 0, j, columns).wait_recv())
                        if block[0] == "u":
                            near_copy_u(block[1], j).start()
                        elif block in needs[place]:
                            near_copy(slots[place][block], j).start()

                    @pl.when((t >= t0 + LAG) & (t < t0 + LAG + span(block, first, last)))
                    def _():
                        j, more = paced(block, t - (t0 + LAG), pieces)
                        take(first + j)
                        if more is not False:
                            pl.when(more)(functools.partial(take, first + j + 1))
                for hop, number in outgoing[place]:
                    block, p, q, first, last, t0 = hop

                    def give(j):
                        each(block, j, lambda columns: hop_copy(hop, number, j, columns).start())

                    @pl.when((t >= t0) & (t < t0 + span(block, first, last)))
                    def _():
                        j, more = paced(block, t - t0, pieces)
                        give(first + j)
                        if more is not False:
                            pl.when(more)(functools.partial(give, first + j + 1))

        def consume(entry, carry):
            pending, into = carry
            begin = jnp.int32(-1000)
            for index in range(16):
                begin = jnp.where(entry == index, begins[index], begin)
            m, part = entry // 4, lax.rem(entry, 4)
            past = t - begin
            ready = (past >= 0) & (past < pieces // 4) & (lax.rem(past, 2) == 0)

            @pl.when(ready)
            def _():
                ago = past + part * (pieces // 4)
                slot_b = jnp.where(c == z, m, 4 + m)
                for i in range(2):
                    near_arrival(m, ago + i).wait_recv()

                    @pl.when(c != z)
                    def _():
                        near_arrival(slot_b, ago + i).wait_recv()
                for copy in loads(m, slot_b, ago, 1 - into):
                    copy.start()
                pl.when(pending == 1)(functools.partial(multiply, into))
            return jnp.where(ready, 1, pending), jnp.where(ready, 1 - into, into)
        pending, into = lax.fori_loop(0, 16, consume, carry)
        last = (chip == 4) & (t == final)

        @pl.when(last)
        def _():
            pl.when(pending == 1)(functools.partial(multiply, into))
            flip()
        return jnp.where(last, 0, pending), into

    begins = []
    for index in range(16):
        begin = jnp.int32(-1000)
        for place in chips:
            if (place, index // 4, index % 4) in due:
                begin = jnp.where(chip == place[0] * 4 + place[1], due[place, index // 4, index % 4], begin)
        begins.append(begin)

    own = pltpu.make_async_copy(f_ref, stage, local.at[0])
    keep = pltpu.make_async_copy(stage, x_ref.at[pl.ds(pl.multiple_of((z * 2 + k) * rows, rows), rows), :], local.at[0])
    own_u = pltpu.make_async_copy(u_ref, stage_u, local.at[1])
    keep_u = pltpu.make_async_copy(stage_u, ub_ref.at[r], local.at[1])
    pl.when(owner)(own.start)
    own_u.start()
    lax.fori_loop(0, pieces, spread, 0)
    lax.fori_loop(0, coupling_pieces, spread_u, 0)
    fill_all(lambda copy: copy.start())
    acc[...] = jnp.zeros_like(acc)

    @pl.when(owner)
    def _():
        own.wait()
        keep.start()
    own_u.wait()
    keep_u.start()
    fill_all(lambda copy: copy.wait())
    pl.when(owner)(keep.wait)
    keep_u.wait()
    pending, turned_to = lax.fori_loop(0, steps, step, (jnp.int32(0), jnp.int32(0)))
    pl.when(pending == 1)(functools.partial(multiply, turned_to))

    @pl.when(chip == 1)
    def _():
        at = pl.ds(pl.multiple_of((slots[0, 1][G] * 2 + k) * rows, rows), rows)
        load = pltpu.make_async_copy(x_ref.at[at, :], stage, local.at[0])
        load.start()
        load.wait()
        tile = min(128, tall)

        def widen(i, carry):
            at = pl.ds(pl.multiple_of(i * tile, tile), tile)
            acc[at, :] = stage[at, :].astype(jnp.float32)
            return carry
        lax.fori_loop(0, tall // tile, widen, 0)
    out = pltpu.make_async_copy(acc, g_ref, local.at[0])
    out.start()

    def settle(j, carry):
        @pl.when(owner)
        def _():
            near_copy(z, j, own_rows(j)).wait_send()
        return carry
    lax.fori_loop(0, pieces, settle, 0)

    def settle_u(j, carry):
        for level in range(4):
            near_copy_u(level, j).wait_send()
            at = pl.ds(pl.multiple_of(j * hu, hu), hu)
            ref = ub_ref.at[level * 2 + 1 - k, at, :]
            remote(ref, ref, near_u.at[level, j], recv_near_u.at[level, j], r, c).wait_recv()
        return carry
    lax.fori_loop(0, coupling_pieces, settle_u, 0)
    for place in chips:
        @pl.when(chip == place[0] * 4 + place[1])
        def _():
            for hop, number in outgoing[place]:
                def sent(j, carry):
                    each(hop[0], j, lambda columns: hop_copy(hop, number, j, columns).wait_send())
                    return carry
                lax.fori_loop(hop[3], hop[4], sent, 0)
            for hop in incoming[place]:
                if hop[0][0] != "u" and hop[0] in needs[place]:
                    def passed(j, carry):
                        near_copy(slots[place][hop[0]], j).wait_send()
                        return carry
                    lax.fori_loop(hop[3], hop[4], passed, 0)
    out.wait()


def stream(factor, coupling, n_row, n_col):
    rows, width = factor.shape
    depth, narrow = coupling.shape
    pieces, coupling_pieces = 16, 4
    hops = plan(pieces, coupling_pieces)[0]
    out_count = max(sum(hop[1] == chip and hop[0][0] != "u" for hop in hops) for chip in {h[1] for h in hops})
    out_count_u = max(sum(hop[1] == chip and hop[0][0] == "u" for hop in hops) for chip in {h[1] for h in hops})
    tall = width // 2
    h = rows // pieces
    dma = pltpu.SemaphoreType.DMA
    return pl.pallas_call(
        functools.partial(stream_kernel, pieces, coupling_pieces),
        out_shape=(
            jax.ShapeDtypeStruct((8 * 2 * rows, width), factor.dtype),
            jax.ShapeDtypeStruct((n_row, depth, narrow), coupling.dtype),
            jax.ShapeDtypeStruct((tall, width), jnp.float32),
        ),
        in_specs=[pl.BlockSpec(memory_space=pl.ANY)] * 2,
        out_specs=[pl.BlockSpec(memory_space=pl.ANY)] * 3,
        scratch_shapes=[
            dma((out_count, pieces)),
            dma((out_count_u, coupling_pieces)),
            dma((8, pieces)),
            dma((4, coupling_pieces)),
            dma((8, pieces)),
            dma((4, coupling_pieces)),
            dma((8, pieces)),
            dma((4, coupling_pieces)),
            dma((2,)),
            dma((pieces,)),
            dma((12,)),
            pltpu.VMEM((tall, width), jnp.float32),
            pltpu.VMEM((2, 4 * h, width), factor.dtype),
            pltpu.VMEM((2, 4 * h, tall), factor.dtype),
            pltpu.VMEM((rows, width), factor.dtype),
            pltpu.VMEM((depth, narrow), coupling.dtype),
            pltpu.VMEM((h, width), factor.dtype),
            pltpu.VMEM((width, tall), factor.dtype),
        ],
        compiler_params=pltpu.CompilerParams(has_side_effects=True, vmem_limit_bytes=63 * 1024 * 1024),
        cost_estimate=pl.CostEstimate(flops=0, bytes_accessed=rows * width * 64, transcendentals=0),
    )(factor, coupling)


DELAY = 4


def child_kernel(n_col, g_ref, u_ref, part_ref, first_ref, second_ref, sum_ref, send, recv, send_sum, recv_sum, local,
                 whole, held, out, came, mine, both):
    r, c = lax.axis_index("row"), lax.axis_index("col")
    x, y = lax.rem(c, 2), c // 2
    beside, above, across = y * 2 + 1 - x, (1 - y) * 2 + x, (1 - y) * 2 + 1 - x
    tile = held.shape[1]
    count, _, narrow = whole.shape
    cores = count // n_col
    tiles = g_ref.shape[0] // tile

    def rows(i):
        return pl.ds(pl.multiple_of(i * tile, tile), tile)

    def pair(i):
        even = lax.rem(i, 2) == 0
        return jnp.where(even, beside, above), jnp.where(even, above, beside)

    def remote(src, dst, send_sem, recv_sem, col):
        return pltpu.make_async_remote_copy(
            src_ref=src, dst_ref=dst, send_sem=send_sem, recv_sem=recv_sem,
            device_id=(r, col), device_id_type=MESH,
        )

    def load(i, into):
        return pltpu.make_async_copy(g_ref.at[rows(i), :], held.at[into], local.at[into])

    def fetch(q):
        return pltpu.make_async_copy(u_ref.at[q], whole.at[q], local.at[7 + q])

    def keep(i):
        return pltpu.make_async_copy(out, part_ref.at[:, rows(i), :], local.at[2])

    def firsts(i):
        near = pair(i)[0]
        return [
            remote(part_ref.at[ct, rows(i), :], first_ref.at[n, rows(i), :], send.at[n, i], recv.at[n, i], near)
            for n, ct in enumerate((near, across))
        ]

    def seconds(i):
        return remote(sum_ref.at[rows(i), :], second_ref.at[rows(i), :], send_sum.at[i], recv_sum.at[i], pair(i)[1])

    def reads(i):
        return (
            pltpu.make_async_copy(first_ref.at[1, rows(i), :], came, local.at[3]),
            pltpu.make_async_copy(part_ref.at[pair(i)[1], rows(i), :], mine, local.at[4]),
        )

    def store(i):
        into = lax.rem(i, 2)
        return pltpu.make_async_copy(both.at[into], sum_ref.at[rows(i), :], local.at[5 + into])

    load(0, 0).start()
    for q in range(count):
        fetch(q).start()

    def one(i, carry):
        @pl.when((i > DELAY) & (i <= tiles + DELAY))
        def _():
            store(i - DELAY - 1).wait()
            seconds(i - DELAY - 1).start()

        @pl.when((i >= DELAY) & (i < tiles + DELAY))
        def _():
            for copy in firsts(i - DELAY):
                copy.wait_recv()
            for copy in reads(i - DELAY):
                copy.start()

        @pl.when(i < tiles)
        def _():
            into = lax.rem(i, 2)
            load(i, into).wait()

            @pl.when(i + 1 < tiles)
            def _():
                load(i + 1, 1 - into).start()
            rounded = held[into].astype(whole.dtype)
            for q in range(count):
                pl.when(i == 0)(fetch(q).wait)
                product = jnp.dot(rounded, whole[q], preferred_element_type=jnp.float32)
                out[q // cores, :, pl.ds(q % cores * narrow, narrow)] = product.astype(out.dtype)
            keep(i).start()

        @pl.when((i >= DELAY) & (i < tiles + DELAY))
        def _():
            for copy in reads(i - DELAY):
                copy.wait()
            total = came[...].astype(jnp.float32) + mine[...].astype(jnp.float32)
            both[lax.rem(i - DELAY, 2)] = total.astype(both.dtype)
            store(i - DELAY).start()

        @pl.when(i < tiles)
        def _():
            keep(i).wait()
            for copy in firsts(i):
                copy.start()
        return carry
    lax.fori_loop(0, tiles + DELAY + 1, one, 0)

    def settle(i, carry):
        for copy in firsts(i):
            copy.wait_send()
        seconds(i).wait()
        return carry
    lax.fori_loop(0, tiles, settle, 0)


def child_parts(gram, coupling, n_col):
    tall, width = gram.shape
    count, depth, narrow = coupling.shape
    tile = min(128, tall)
    wide = count * narrow // n_col
    tiles = tall // tile
    dma = pltpu.SemaphoreType.DMA
    own, first, second, _ = pl.pallas_call(
        functools.partial(child_kernel, n_col),
        out_shape=(
            jax.ShapeDtypeStruct((n_col, tall, wide), coupling.dtype),
            jax.ShapeDtypeStruct((2, tall, wide), coupling.dtype),
            jax.ShapeDtypeStruct((tall, wide), coupling.dtype),
            jax.ShapeDtypeStruct((tall, wide), coupling.dtype),
        ),
        in_specs=[pl.BlockSpec(memory_space=pl.ANY)] * 2,
        out_specs=[pl.BlockSpec(memory_space=pl.ANY)] * 4,
        scratch_shapes=[
            dma((2, tiles)),
            dma((2, tiles)),
            dma((tiles,)),
            dma((tiles,)),
            dma((7 + count,)),
            pltpu.VMEM((count, depth, narrow), coupling.dtype),
            pltpu.VMEM((2, tile, width), gram.dtype),
            pltpu.VMEM((n_col, tile, wide), coupling.dtype),
            pltpu.VMEM((tile, wide), coupling.dtype),
            pltpu.VMEM((tile, wide), coupling.dtype),
            pltpu.VMEM((2, tile, wide), coupling.dtype),
        ],
        compiler_params=pltpu.CompilerParams(has_side_effects=True, vmem_limit_bytes=63 * 1024 * 1024),
    )(gram, coupling)
    return own, first, second


def finish_kernel(c_ref, g_ref, own_ref, first_ref, second_ref, member_ref, gram_ref, child_ref):
    gram_ref[...] = g_ref[...]
    total = own_ref[0].astype(jnp.float32) + first_ref[0].astype(jnp.float32) + second_ref[...].astype(jnp.float32)
    child_ref[...] = jnp.where(member_ref[...] != 0, -total.T, jnp.float32(0.0))


def finish(gram, own, first, second, member, col_index):
    tall, width = gram.shape
    wide = own.shape[2]
    tile = min(256, tall)
    return pl.pallas_call(
        finish_kernel,
        grid_spec=pltpu.PrefetchScalarGridSpec(
            num_scalar_prefetch=1,
            grid=(tall // tile,),
            in_specs=[
                pl.BlockSpec((tile, width), lambda i, c: (i, 0)),
                pl.BlockSpec((1, tile, wide), lambda i, c: (c[0], i, 0)),
                pl.BlockSpec((1, tile, wide), lambda i, c: (0, i, 0)),
                pl.BlockSpec((tile, wide), lambda i, c: (i, 0)),
                pl.BlockSpec((1, tile), lambda i, c: (0, i)),
            ],
            out_specs=(
                pl.BlockSpec((tile, width), lambda i, c: (i, 0)),
                pl.BlockSpec((wide, tile), lambda i, c: (0, i)),
            ),
        ),
        out_shape=(
            jax.ShapeDtypeStruct((tall, width), jnp.float32),
            jax.ShapeDtypeStruct((wide, tall), jnp.float32),
        ),
        compiler_params=pltpu.CompilerParams(vmem_limit_bytes=63 * 1024 * 1024),
        cost_estimate=pl.CostEstimate(flops=0, bytes_accessed=tall * width * 12, transcendentals=0),
    )(jnp.reshape(col_index, (1,)), gram, own, first, second, member)


def exchange_kernel(n_col, part_ref, out_ref, send, recv):
    r, c = lax.axis_index("row"), lax.axis_index("col")
    depth = out_ref.shape[1]
    started = []
    for d in range(1, n_col):
        ct = lax.rem(c + d, n_col)
        copy = pltpu.make_async_remote_copy(
            src_ref=part_ref.at[pl.ds(pl.multiple_of(ct * depth, depth), depth), :],
            dst_ref=out_ref.at[d - 1],
            send_sem=send.at[d - 1],
            recv_sem=recv.at[d - 1],
            device_id=(r, ct),
            device_id_type=MESH,
        )
        copy.start()
        started.append(copy)
    for copy in started:
        copy.wait()


def exchange(part, n_col):
    total, width = part.shape
    dma = pltpu.SemaphoreType.DMA
    return pl.pallas_call(
        functools.partial(exchange_kernel, n_col),
        out_shape=jax.ShapeDtypeStruct((n_col - 1, total // n_col, width), part.dtype),
        in_specs=[pl.BlockSpec(memory_space=pl.ANY)],
        out_specs=pl.BlockSpec(memory_space=pl.ANY),
        scratch_shapes=[dma((n_col - 1,)), dma((n_col - 1,))],
        compiler_params=pltpu.CompilerParams(has_side_effects=True),
    )(part)


def general(n_row, n_col, factor, coupling):
    rows_here = factor.shape[0]
    row_index, col_index = lax.axis_index("row"), lax.axis_index("col")
    cores = n_row // n_col
    below, partner = gather(factor, n_row, n_col)
    coupling_full = lax.all_gather(coupling, "row", axis=1, tiled=True)

    def product(level, below, partner):
        first = level * rows_here * cores
        return lax.dot_general(
            partner[first:], below[first:], (((0,), (0,)), ((), ())), preferred_element_type=jnp.float32
        )

    gram = lax.switch(
        jnp.maximum(row_index // cores, col_index),
        [functools.partial(product, level) for level in range(n_col)],
        below,
        partner,
    )
    rounded = gram.astype(jnp.bfloat16)
    part = lax.dot_general(
        coupling_full, rounded, (((0,), (1,)), ((), ())), preferred_element_type=jnp.float32
    ).astype(jnp.bfloat16)
    return gram, part


def body(n_row, n_col, factor, sel_tiles, coupling):
    rows_here = factor.shape[0]
    row_index, col_index = lax.axis_index("row"), lax.axis_index("col")
    cores = n_row // n_col
    global_rows = row_index * rows_here + jnp.arange(rows_here, dtype=jnp.int32)
    member = jnp.any((global_rows // TILE)[:, None] == sel_tiles[None, :], axis=1)
    if (n_row, n_col) == (8, 4):
        _, pieces, gram = stream(factor, coupling, n_row, n_col)
        own, first, second = child_parts(gram, pieces, n_col)
        return finish(gram, own, first, second, member.astype(jnp.int32)[None, :], col_index)
    gram, part = general(n_row, n_col, factor, coupling)
    depth = part.shape[0] // n_col
    arrived = exchange(part, n_col)
    summed = lax.dynamic_slice_in_dim(part, col_index * depth, depth, 0).astype(jnp.float32)
    for d in range(n_col - 1):
        summed = summed + arrived[d].astype(jnp.float32)
    child = jnp.where(member[None, :], -summed, jnp.float32(0.0))
    return (gram, child)


def solution(mesh):
    placed = (P("row", "col"), P(), P("col", "row"))
    return jax.shard_map(
        functools.partial(body, mesh.shape["row"], mesh.shape["col"]),
        mesh=mesh,
        in_specs=placed,
        out_specs=(P("row", "col"), P("col", "row")),
        check_vma=False,
    )
```

```python
import functools
import math

import jax
import jax.numpy as jnp
from jax import lax
from jax.experimental import pallas as pl
from jax.experimental.pallas import tpu as pltpu
from jax.sharding import PartitionSpec as P

TILE = 128
MESH = pl.DeviceIdType.MESH
SKEW = 2


def gather_kernel(dims, f_ref, a_ref, b_ref, recv_a, recv_b, send_z, send_p, send_b, send_f, local_a, stage):
    levels, wide, high, cores, chunks = dims
    rows, width = f_ref.shape
    narrow = width // cores
    h = rows // chunks
    r, c = lax.axis_index("row"), lax.axis_index("col")
    k, z = lax.rem(r, cores), r // cores
    x, y = lax.rem(c, wide), c // wide
    x0, y0 = lax.rem(z, wide), z // wide
    source = c == z

    def chunk_rows(block, j):
        return pl.ds(pl.multiple_of(block * rows + j * h, h), h)

    def remote(src, dst, send, recv, row, col):
        return pltpu.make_async_remote_copy(
            src_ref=src, dst_ref=dst, send_sem=send, recv_sem=recv,
            device_id=(row, col), device_id_type=MESH,
        )

    def copies(t, j):
        m = z + t
        inside = m < levels
        has = inside & (m >= c)
        block = m * cores + k
        at = chunk_rows(block, j)
        if t == 0:
            def src(cols):
                return f_ref.at[pl.ds(j * h, h), cols]
        else:
            def src(cols):
                return a_ref.at[at, cols]
        everything = pl.ds(0, width)
        found = []
        for kk in range(cores):
            piece = src(pl.ds(kk * narrow, narrow))
            into = b_ref.at[at, :]
            for dx in range(1, wide):
                xt = lax.rem(x + dx, wide)
                found.append((
                    source & inside & (m >= y * wide + xt),
                    remote(piece, into, send_b.at[kk, dx, t, j], recv_b.at[block, j],
                           z * cores + kk, y * wide + xt),
                    False,
                ))
            for dy in range(1, high):
                yt = lax.rem(y + dy, high)
                found.append((
                    source & inside & (m >= yt * wide),
                    remote(piece, into, send_b.at[kk, wide - 1 + dy, t, j], recv_b.at[block, j],
                           z * cores + kk, yt * wide + x),
                    False,
                ))
        found.append((
            has & (z > 0),
            remote(src(everything), a_ref.at[at, :], send_z.at[t, j], recv_a.at[block, j],
                   r - cores, c),
            False,
        ))
        for dk in range(1, cores):
            other = z * cores + lax.rem(k + dk, cores)
            found.append((
                has,
                remote(src(everything), a_ref.at[at, :], send_p.at[dk, t, j], recv_a.at[block, j], other, c),
                False,
            ))
        for kk in range(cores):
            piece = src(pl.ds(kk * narrow, narrow))
            into = b_ref.at[at, :]
            found.append((
                source & inside & (k != kk),
                remote(piece, into, send_b.at[kk, 0, t, j], recv_b.at[block, j], z * cores + kk, c),
                False,
            ))
        return found

    def keep(t, j):
        m = z + t
        at = chunk_rows(m * cores + k, j)
        here = f_ref.at[pl.ds(j * h, h), :] if t == 0 else a_ref.at[at, :]
        inside = (m < levels) & (m >= c)

        @pl.when(inside if t == 0 else inside & source)
        def _():
            load = pltpu.make_async_copy(here, stage, local_a.at[0])
            load.start()
            load.wait()
            if t == 0:
                pltpu.make_async_copy(stage, a_ref.at[at, :], local_a.at[1]).start()
            for kk in range(cores):
                @pl.when(source & (k == kk))
                def _():
                    store = pltpu.make_async_copy(
                        stage.at[:, pl.ds(kk * narrow, narrow)], b_ref.at[at, :], local_a.at[2]
                    )
                    store.start()
                    store.wait()
            if t == 0:
                pltpu.make_async_copy(stage, a_ref.at[at, :], local_a.at[1]).wait()

    def forwards(t, j, p):
        m = z + t
        block = m * cores + p
        part = b_ref.at[chunk_rows(block, j), :]
        mine = (x == x0) & (y != y0) & (m < levels)
        found = []
        for dx in range(1, wide):
            xt = lax.rem(x + dx, wide)
            found.append((
                mine & (m >= y * wide + xt),
                remote(part, part, send_f.at[dx, p, t, j], recv_b.at[block, j], r, y * wide + xt),
            ))
        return mine & (m >= y * wide), found

    def arrived(ref, sem):
        remote(ref, ref, send_z.at[0, 0], sem, r, c).wait_recv()

    def step(t, j):
        m = z + t
        block = m * cores + k
        if t > 0:
            @pl.when((m < levels) & (m >= c))
            def _():
                arrived(a_ref.at[chunk_rows(block, j), :], recv_a.at[block, j])
        for condition, copy, _ in copies(t, j):
            pl.when(condition)(copy.start)
        keep(t, j)

    def forward(t, j):
        for p in range(cores):
            due, found = forwards(t, j, p)
            block = (z + t) * cores + p

            @pl.when(due)
            def _():
                arrived(b_ref.at[chunk_rows(block, j), :], recv_b.at[block, j])
            for condition, copy in found:
                pl.when(condition)(copy.start)

    order = [(t, j) for t in range(levels) for j in range(chunks)]
    for n, (t, j) in enumerate(order):
        step(t, j)
        if n >= SKEW:
            forward(*order[n - SKEW])
    for t, j in order[len(order) - SKEW:]:
        forward(t, j)

    for t, j in order:
        m = z + t
        inside = m < levels
        for dk in range(1, cores):
            block = m * cores + lax.rem(k + dk, cores)

            @pl.when(inside & (m >= c))
            def _():
                arrived(a_ref.at[chunk_rows(block, j), :], recv_a.at[block, j])

            @pl.when(inside & source)
            def _():
                arrived(b_ref.at[chunk_rows(block, j), :], recv_b.at[block, j])
        for p in range(cores):
            block = m * cores + p

            @pl.when(inside & (x != x0) & (m >= c))
            def _():
                arrived(b_ref.at[chunk_rows(block, j), :], recv_b.at[block, j])
        for condition, copy, local in copies(t, j):
            pl.when(condition)(copy.wait if local else copy.wait_send)
        for p in range(cores):
            for condition, copy in forwards(t, j, p)[1]:
                pl.when(condition)(copy.wait_send)


def gather(factor, n_row, n_col):
    rows, width = factor.shape
    cores = n_row // n_col
    wide = next(w for w in range(math.isqrt(n_col), 0, -1) if n_col % w == 0)
    high = n_col // wide
    levels = n_col
    chunks = max(1, 32 // n_row)
    dma = pltpu.SemaphoreType.DMA
    whole = rows * n_row
    return pl.pallas_call(
        functools.partial(gather_kernel, (levels, wide, high, cores, chunks)),
        out_shape=(
            jax.ShapeDtypeStruct((whole, width), factor.dtype),
            jax.ShapeDtypeStruct((whole, width // cores), factor.dtype),
        ),
        in_specs=[pl.BlockSpec(memory_space=pl.ANY)],
        out_specs=(pl.BlockSpec(memory_space=pl.ANY), pl.BlockSpec(memory_space=pl.ANY)),
        scratch_shapes=[
            dma((n_row, chunks)),
            dma((n_row, chunks)),
            dma((levels, chunks)),
            dma((cores, levels, chunks)),
            dma((cores, wide + high, levels, chunks)),
            dma((wide, cores, levels, chunks)),
            dma((3,)),
            pltpu.VMEM((rows // chunks, width), factor.dtype),
        ],
        compiler_params=pltpu.CompilerParams(has_side_effects=True),
        cost_estimate=pl.CostEstimate(flops=0, bytes_accessed=whole * width * 32, transcendentals=0),
    )(factor)


LAG = 2
G = ("g", 1, 0)


def block_flows(pieces):
    half, cut = pieces // 2, 5 * pieces // 8
    found = []

    def add(block, source, hops, first=0, last=pieces):
        found.append((block, source, hops, first, last))

    add((3, 3), (3, 3), [((3, 3), (2, 3)), ((2, 3), (1, 3)), ((1, 3), (0, 3)), ((3, 3), (3, 1)), ((3, 3), (3, 2)),
                         ((3, 2), (3, 0))])
    add((3, 2), (3, 2), [((3, 2), (2, 2)), ((2, 2), (2, 3)), ((2, 3), (2, 1)), ((2, 2), (2, 0)), ((2, 2), (1, 2)),
                         ((1, 2), (0, 2))])
    add((3, 1), (3, 1), [((3, 1), (2, 1)), ((2, 1), (2, 0)), ((2, 0), (1, 0)), ((1, 0), (1, 1)), ((1, 1), (1, 3)),
                         ((1, 0), (1, 2))], 0, cut)
    add((3, 1), (3, 1), [((3, 1), (2, 1)), ((2, 1), (1, 1)), ((1, 1), (1, 3)), ((1, 3), (1, 2)), ((1, 2), (1, 0))],
        cut, pieces)
    add((3, 0), (3, 0), [((3, 0), (2, 0)), ((2, 0), (2, 1)), ((2, 1), (2, 3)), ((2, 3), (1, 3)), ((1, 3), (1, 2)),
                         ((1, 2), (1, 0)), ((1, 3), (0, 3)), ((0, 3), (0, 2)), ((0, 2), (0, 0))])
    around = [((1, 0), (1, 1)), ((1, 1), (0, 1)), ((0, 1), (0, 0)), ((0, 0), (0, 2))]
    add((2, 0), (2, 0), [((2, 0), (1, 0))] + around, 0, 3 * pieces // 4)
    add((2, 0), (2, 0), [((2, 0), (2, 2)), ((2, 2), (1, 2)), ((1, 2), (1, 0))] + around, 3 * pieces // 4, pieces)
    add((1, 0), (1, 0), [((1, 0), (0, 0))])
    add((2, 1), (2, 1), [((2, 1), (1, 1)), ((1, 1), (1, 0)), ((1, 0), (1, 2))])
    add((1, 1), (1, 1), [((1, 1), (1, 0))])
    add((2, 2), (2, 2), [((2, 2), (2, 3)), ((2, 3), (2, 1)), ((2, 2), (2, 0)), ((2, 2), (1, 2)), ((1, 2), (0, 2))])
    add(G, (1, 0), [((1, 0), (0, 0)), ((0, 0), (0, 1))], 0, half)
    add(G, (1, 0), [((1, 0), (1, 1)), ((1, 1), (0, 1))], half, pieces)
    return found


def coupling_flows(pieces):
    found = []
    for c in range(4):
        for z in range(4):
            hops = [((a, c), (a - 1, c)) for a in range(z, 0, -1)] + [((a, c), (a + 1, c)) for a in range(z, 3)]
            found.append((("u", z, c), (z, c), hops, 0, pieces))
    return found


def paced(block, s, pieces):
    if block[0] != block[1]:
        return s, False
    unit = pieces // 4
    late = s - unit
    if isinstance(s, int):
        turn = late % 3
        slow = pieces // 2 + late // 3 * 4 + turn + (turn > 0)
        return (2 * s, True) if s < unit else (slow, turn == 0)
    turn = lax.rem(late, 3)
    slow = pieces // 2 + late // 3 * 4 + turn + jnp.where(turn > 0, 1, 0)
    return jnp.where(s < unit, 2 * s, slow), (s < unit) | (turn == 0)


def span(block, first, last):
    count = last - first
    return count // 4 + count // 8 * 3 if block[0] == block[1] else count


ORDER = [6, 24, 14, 15, 3, 9, 25, 13, 7, 17, 5, 4, 8, 26, 1, 2, 20, 10, 19, 0, 28, 16, 18, 21, 12, 11, 23, 22, 27]


@functools.cache
def plan(pieces, coupling_pieces):
    flows = block_flows(pieces) + coupling_flows(coupling_pieces)
    chips = [(z, c) for z in range(4) for c in range(4)]
    pairs = [(chip, m) for chip in chips if chip != (0, 1) for m in range(max(chip), 4)]
    busy, hops, due = {}, [], {}
    final = None
    for index in ORDER:
        block, source, route, first, last = flows[index]
        if block == G and final is None:
            due = ready_steps(pieces, hops, pairs)
            final = max(d for key, d in due.items() if key[0] == (1, 0)) + pieces // 4
        n, at = span(block, first, last), {source: final + 1 if block == G else 0}
        for p, q in route:
            t, used = at[p], busy.setdefault((p, q), [])
            while any(t < e and s < t + n for s, e in used):
                t += 1
            used.append((t, t + n))
            at[q] = t + LAG
            hops.append((block, p, q, first, last, t))
    slots = {chip: {} for chip in chips}
    needs = {chip: set() for chip in chips}
    for chip, m in pairs:
        z, c = chip
        slots[chip][m, c] = m
        needs[chip].add((m, c))
        if c != z:
            slots[chip][m, z] = 4 + m
            needs[chip].add((m, z))
    for block, p, q, first, last, t in hops:
        for chip in (p, q):
            if block[0] != "u" and block not in slots[chip] and block != chip:
                slots[chip][block] = min(set(range(8)) - set(slots[chip].values()))
    steps = max([t + span(block, first, last) + LAG for block, p, q, first, last, t in hops] + [d + pieces // 4 for d in due.values()] + [final + 1])
    return hops, slots, needs, due, steps, final


def ready_steps(pieces, hops, pairs):
    due, group = {}, pieces // 8
    for chip, m in pairs:
        z, c = chip
        ready = {(z, c): [1] * pieces}
        for block, p, q, first, last, t in hops:
            if q == chip:
                for s in range(span(block, first, last)):
                    j, more = paced(block, s, pieces)
                    for i in range(1 + more):
                        ready.setdefault(block, [None] * pieces)[first + j + i] = t + LAG + s
        both = [ready[m, c], ready[m, z]]
        for part in range(4):
            begin = part * (pieces // 4)
            due[chip, m, part] = 1 + max(b[begin + j] - j // group * group for b in both for j in range(pieces // 4))
    return due


def stream_kernel(pieces, coupling_pieces, f_ref, u_ref, x_ref, ub_ref, g_ref, send, send_u, near, near_u, recv,
                  recv_u, recv_near, recv_near_u, turn, blank, local, acc, a_buf, b_buf, stage, stage_u, zeros, flipped):
    hops, slots, needs, due, steps, final = plan(pieces, coupling_pieces)
    rows, width = f_ref.shape
    depth, narrow = u_ref.shape
    h, hu, quarter = rows // pieces, depth // coupling_pieces, width // 4
    tall = acc.shape[0]
    r, c = lax.axis_index("row"), lax.axis_index("col")
    k, z = lax.rem(r, 2), r // 2
    chip = z * 4 + c
    owner = z >= c

    def at_rows(slot, core, j):
        return pl.ds(pl.multiple_of((slot * 2 + core) * rows + j * h, h), h)

    def remote(src, dst, send_sem, recv_sem, row, col):
        return pltpu.make_async_remote_copy(
            src_ref=src, dst_ref=dst, send_sem=send_sem, recv_sem=recv_sem,
            device_id=(row, col), device_id_type=MESH,
        )

    def shapes(block, j):
        if block[0] != block[1]:
            return [(None, width)]
        part = (k * pieces + j) // (pieces // 2)
        return [(part == q, (q + 1) * quarter) for q in range(4)]

    def each(block, j, act):
        if block[0] == "u":
            act(None)
            return
        for condition, columns in shapes(block, j):
            if condition is None:
                act(columns)
            else:
                pl.when(condition)(functools.partial(act, columns))

    def hop_copy(hop, number, j, columns):
        block, p, q, first, last, t = hop
        if block[0] == "u":
            at = pl.ds(pl.multiple_of(j * hu, hu), hu)
            src = u_ref.at[at, :] if p == block[1:] else ub_ref.at[block[1] * 2 + k, at, :]
            return remote(src, ub_ref.at[block[1] * 2 + k, at, :], send_u.at[number, j], recv_u.at[block[1], j],
                          q[0] * 2 + k, q[1])
        cols = pl.ds(0, columns)
        if p == block:
            src = f_ref.at[pl.ds(pl.multiple_of(j * h, h), h), cols]
        else:
            src = x_ref.at[at_rows(slots[p][block], k, j), cols]
        slot = slots[q][block]
        return remote(src, x_ref.at[at_rows(slot, k, j), cols], send.at[number, j], recv.at[slot, j],
                      q[0] * 2 + k, q[1])

    def near_copy(slot, j, src=None):
        at = at_rows(slot, k, j)
        return remote(x_ref.at[at, :] if src is None else src, x_ref.at[at, :], near.at[slot, j],
                      recv_near.at[slot, j], z * 2 + 1 - k, c)

    def near_arrival(slot, j):
        ref = x_ref.at[at_rows(slot, 1 - k, j), :]
        return remote(ref, ref, near.at[slot, j], recv_near.at[slot, j], r, c)

    def near_copy_u(level, j, src=None):
        at = pl.ds(pl.multiple_of(j * hu, hu), hu)
        ref = ub_ref.at[level * 2 + k, at, :]
        return remote(ref if src is None else src, ref, near_u.at[level, j], recv_near_u.at[level, j],
                      z * 2 + 1 - k, c)

    def own_rows(j):
        return f_ref.at[pl.ds(pl.multiple_of(j * h, h), h), :]

    def own_rows_u(j):
        return u_ref.at[pl.ds(pl.multiple_of(j * hu, hu), hu), :]

    chips = [(a, b) for a in range(4) for b in range(4)]
    incoming = {chip_: [hop for hop in hops if hop[2] == chip_] for chip_ in chips}
    outgoing = {chip_: [] for chip_ in chips}
    count, count_u = {}, {}
    for hop in hops:
        counts = count_u if hop[0][0] == "u" else count
        number = counts.get(hop[1], 0)
        counts[hop[1]] = number + 1
        outgoing[hop[1]].append((hop, number))

    zeros[...] = jnp.zeros_like(zeros)

    def fill(slot, act):
        def one(j, carry):
            for condition, columns in shapes((0, 0), j):
                if columns < width:
                    @pl.when(condition)
                    def _():
                        act(pltpu.make_async_copy(
                            zeros.at[:, pl.ds(0, width - columns)],
                            x_ref.at[at_rows(slot, k, j), pl.ds(columns, width - columns)], blank.at[j]))
            return carry
        lax.fori_loop(0, pieces, one, 0)

    def fill_all(act):
        for place in chips:
            for block in needs[place]:
                if block[0] == block[1] and block != place:
                    pl.when(chip == place[0] * 4 + place[1])(functools.partial(fill, slots[place][block], act))

    def spread(j, carry):
        @pl.when(owner)
        def _():
            near_copy(z, j, own_rows(j)).start()
        return carry

    def spread_u(j, carry):
        near_copy_u(z, j, own_rows_u(j)).start()
        return carry

    def loads(m, slot_b, ago, into):
        cols = pl.ds(pl.multiple_of(k * tall, tall), tall)
        found = []
        for core in range(2):
            at_a = pl.ds(pl.multiple_of((m * 2 + core) * rows + ago * h, 2 * h), 2 * h)
            at_b = pl.ds(pl.multiple_of((slot_b * 2 + core) * rows + ago * h, 2 * h), 2 * h)
            half = pl.ds(core * 2 * h, 2 * h)
            found.append(pltpu.make_async_copy(x_ref.at[at_a, :], a_buf.at[into, half, :], local.at[2 + into * 4 + core]))
            found.append(pltpu.make_async_copy(x_ref.at[at_b, cols], b_buf.at[into, half, :], local.at[4 + into * 4 + core]))
        return found

    def multiply(into):
        for copy in loads(0, 0, 0, into):
            copy.wait()
        tile = min(256, tall)

        def rows_of(i, carry):
            at = pl.ds(pl.multiple_of(i * tile, tile), tile)
            acc[at, :] += lax.dot_general(
                b_buf[into, :, at], a_buf[into], (((0,), (0,)), ((), ())), preferred_element_type=jnp.float32)
            return carry
        lax.fori_loop(0, tall // tile, rows_of, 0)

    def flip():
        slot = slots[1, 0][G]
        tile = min(256, width)

        def turned(i, carry):
            at = pl.ds(pl.multiple_of(i * tile, tile), tile)
            flipped[at, :] = acc[:, at].T.astype(flipped.dtype)
            return carry
        lax.fori_loop(0, width // tile, turned, 0)
        cols = pl.ds(pl.multiple_of(k * tall, tall), tall)
        kept = []
        for half in range(2):
            at = pl.ds((slot * 2 + half) * rows, rows)
            kept.append(pltpu.make_async_copy(flipped.at[pl.ds(half * rows, rows), :], x_ref.at[at, cols],
                                              local.at[half]))
        for copy in kept:
            copy.start()
        for copy in kept:
            copy.wait()
        at = pl.ds(pl.multiple_of((slot * 2 + 1 - k) * rows, rows), rows)
        pass_on = remote(x_ref.at[at, cols], x_ref.at[at, cols], turn.at[0], turn.at[1], z * 2 + 1 - k, c)
        pass_on.start()
        pass_on.wait_send()
        at = pl.ds(pl.multiple_of((slot * 2 + k) * rows, rows), rows)
        cols = pl.ds(pl.multiple_of((1 - k) * tall, tall), tall)
        remote(x_ref.at[at, cols], x_ref.at[at, cols], turn.at[0], turn.at[1], r, c).wait_recv()

    def step(t, carry):
        for place in chips:
            @pl.when(chip == place[0] * 4 + place[1])
            def _():
                for hop in incoming[place]:
                    block, p, q, first, last, t0 = hop

                    def take(j):
                        each(block, j, lambda columns: hop_copy(hop, 0, j, columns).wait_recv())
                        if block[0] == "u":
                            near_copy_u(block[1], j).start()
                        elif block in needs[place]:
                            near_copy(slots[place][block], j).start()

                    @pl.when((t >= t0 + LAG) & (t < t0 + LAG + span(block, first, last)))
                    def _():
                        j, more = paced(block, t - (t0 + LAG), pieces)
                        take(first + j)
                        if more is not False:
                            pl.when(more)(functools.partial(take, first + j + 1))
                for hop, number in outgoing[place]:
                    block, p, q, first, last, t0 = hop

                    def give(j):
                        each(block, j, lambda columns: hop_copy(hop, number, j, columns).start())

                    @pl.when((t >= t0) & (t < t0 + span(block, first, last)))
                    def _():
                        j, more = paced(block, t - t0, pieces)
                        give(first + j)
                        if more is not False:
                            pl.when(more)(functools.partial(give, first + j + 1))

        def consume(entry, carry):
            pending, into = carry
            begin = jnp.int32(-1000)
            for index in range(16):
                begin = jnp.where(entry == index, begins[index], begin)
            m, part = entry // 4, lax.rem(entry, 4)
            past = t - begin
            ready = (past >= 0) & (past < pieces // 4) & (lax.rem(past, 2) == 0)

            @pl.when(ready)
            def _():
                ago = past + part * (pieces // 4)
                slot_b = jnp.where(c == z, m, 4 + m)
                for i in range(2):
                    near_arrival(m, ago + i).wait_recv()

                    @pl.when(c != z)
                    def _():
                        near_arrival(slot_b, ago + i).wait_recv()
                for copy in loads(m, slot_b, ago, 1 - into):
                    copy.start()
                pl.when(pending == 1)(functools.partial(multiply, into))
            return jnp.where(ready, 1, pending), jnp.where(ready, 1 - into, into)
        pending, into = lax.fori_loop(0, 16, consume, carry)
        last = (chip == 4) & (t == final)

        @pl.when(last)
        def _():
            pl.when(pending == 1)(functools.partial(multiply, into))
            flip()
        return jnp.where(last, 0, pending), into

    begins = []
    for index in range(16):
        begin = jnp.int32(-1000)
        for place in chips:
            if (place, index // 4, index % 4) in due:
                begin = jnp.where(chip == place[0] * 4 + place[1], due[place, index // 4, index % 4], begin)
        begins.append(begin)

    own = pltpu.make_async_copy(f_ref, stage, local.at[0])
    keep = pltpu.make_async_copy(stage, x_ref.at[pl.ds(pl.multiple_of((z * 2 + k) * rows, rows), rows), :], local.at[0])
    own_u = pltpu.make_async_copy(u_ref, stage_u, local.at[1])
    keep_u = pltpu.make_async_copy(stage_u, ub_ref.at[r], local.at[1])
    pl.when(owner)(own.start)
    own_u.start()
    lax.fori_loop(0, pieces, spread, 0)
    lax.fori_loop(0, coupling_pieces, spread_u, 0)
    fill_all(lambda copy: copy.start())
    acc[...] = jnp.zeros_like(acc)

    @pl.when(owner)
    def _():
        own.wait()
        keep.start()
    own_u.wait()
    keep_u.start()
    fill_all(lambda copy: copy.wait())
    pl.when(owner)(keep.wait)
    keep_u.wait()
    pending, turned_to = lax.fori_loop(0, steps, step, (jnp.int32(0), jnp.int32(0)))
    pl.when(pending == 1)(functools.partial(multiply, turned_to))

    @pl.when(chip == 1)
    def _():
        at = pl.ds(pl.multiple_of((slots[0, 1][G] * 2 + k) * rows, rows), rows)
        load = pltpu.make_async_copy(x_ref.at[at, :], stage, local.at[0])
        load.start()
        load.wait()
        tile = min(128, tall)

        def widen(i, carry):
            at = pl.ds(pl.multiple_of(i * tile, tile), tile)
            acc[at, :] = stage[at, :].astype(jnp.float32)
            return carry
        lax.fori_loop(0, tall // tile, widen, 0)
    out = pltpu.make_async_copy(acc, g_ref, local.at[0])
    out.start()

    def settle(j, carry):
        @pl.when(owner)
        def _():
            near_copy(z, j, own_rows(j)).wait_send()
        return carry
    lax.fori_loop(0, pieces, settle, 0)

    def settle_u(j, carry):
        for level in range(4):
            near_copy_u(level, j).wait_send()
            at = pl.ds(pl.multiple_of(j * hu, hu), hu)
            ref = ub_ref.at[level * 2 + 1 - k, at, :]
            remote(ref, ref, near_u.at[level, j], recv_near_u.at[level, j], r, c).wait_recv()
        return carry
    lax.fori_loop(0, coupling_pieces, settle_u, 0)
    for place in chips:
        @pl.when(chip == place[0] * 4 + place[1])
        def _():
            for hop, number in outgoing[place]:
                def sent(j, carry):
                    each(hop[0], j, lambda columns: hop_copy(hop, number, j, columns).wait_send())
                    return carry
                lax.fori_loop(hop[3], hop[4], sent, 0)
            for hop in incoming[place]:
                if hop[0][0] != "u" and hop[0] in needs[place]:
                    def passed(j, carry):
                        near_copy(slots[place][hop[0]], j).wait_send()
                        return carry
                    lax.fori_loop(hop[3], hop[4], passed, 0)
    out.wait()


def stream(factor, coupling, n_row, n_col):
    rows, width = factor.shape
    depth, narrow = coupling.shape
    pieces, coupling_pieces = 16, 4
    hops = plan(pieces, coupling_pieces)[0]
    out_count = max(sum(hop[1] == chip and hop[0][0] != "u" for hop in hops) for chip in {h[1] for h in hops})
    out_count_u = max(sum(hop[1] == chip and hop[0][0] == "u" for hop in hops) for chip in {h[1] for h in hops})
    tall = width // 2
    h = rows // pieces
    dma = pltpu.SemaphoreType.DMA
    return pl.pallas_call(
        functools.partial(stream_kernel, pieces, coupling_pieces),
        out_shape=(
            jax.ShapeDtypeStruct((8 * 2 * rows, width), factor.dtype),
            jax.ShapeDtypeStruct((n_row, depth, narrow), coupling.dtype),
            jax.ShapeDtypeStruct((tall, width), jnp.float32),
        ),
        in_specs=[pl.BlockSpec(memory_space=pl.ANY)] * 2,
        out_specs=[pl.BlockSpec(memory_space=pl.ANY)] * 3,
        scratch_shapes=[
            dma((out_count, pieces)),
            dma((out_count_u, coupling_pieces)),
            dma((8, pieces)),
            dma((4, coupling_pieces)),
            dma((8, pieces)),
            dma((4, coupling_pieces)),
            dma((8, pieces)),
            dma((4, coupling_pieces)),
            dma((2,)),
            dma((pieces,)),
            dma((12,)),
            pltpu.VMEM((tall, width), jnp.float32),
            pltpu.VMEM((2, 4 * h, width), factor.dtype),
            pltpu.VMEM((2, 4 * h, tall), factor.dtype),
            pltpu.VMEM((rows, width), factor.dtype),
            pltpu.VMEM((depth, narrow), coupling.dtype),
            pltpu.VMEM((h, width), factor.dtype),
            pltpu.VMEM((width, tall), factor.dtype),
        ],
        compiler_params=pltpu.CompilerParams(has_side_effects=True, vmem_limit_bytes=63 * 1024 * 1024),
        cost_estimate=pl.CostEstimate(flops=0, bytes_accessed=rows * width * 64, transcendentals=0),
    )(factor, coupling)


DELAY = 3


def child_kernel(n_col, g_ref, u_ref, part_ref, first_ref, second_ref, sum_ref, send, recv, send_sum, recv_sum, local,
                 whole, held, out, came, mine, both):
    r, c = lax.axis_index("row"), lax.axis_index("col")
    x, y = lax.rem(c, 2), c // 2
    beside, above, across = y * 2 + 1 - x, (1 - y) * 2 + x, (1 - y) * 2 + 1 - x
    tile = held.shape[1]
    count, _, narrow = whole.shape
    cores = count // n_col
    tiles = g_ref.shape[0] // tile

    def rows(i):
        return pl.ds(pl.multiple_of(i * tile, tile), tile)

    def pair(i):
        even = lax.rem(i, 2) == 0
        return jnp.where(even, beside, above), jnp.where(even, above, beside)

    def remote(src, dst, send_sem, recv_sem, col):
        return pltpu.make_async_remote_copy(
            src_ref=src, dst_ref=dst, send_sem=send_sem, recv_sem=recv_sem,
            device_id=(r, col), device_id_type=MESH,
        )

    def load(i, into):
        return pltpu.make_async_copy(g_ref.at[rows(i), :], held.at[into], local.at[into])

    def fetch(q):
        return pltpu.make_async_copy(u_ref.at[q], whole.at[q], local.at[7 + q])

    def keep(i):
        return pltpu.make_async_copy(out, part_ref.at[:, rows(i), :], local.at[2])

    def firsts(i):
        near = pair(i)[0]
        return [
            remote(part_ref.at[ct, rows(i), :], first_ref.at[n, rows(i), :], send.at[n, i], recv.at[n, i], near)
            for n, ct in enumerate((near, across))
        ]

    def seconds(i):
        return remote(sum_ref.at[rows(i), :], second_ref.at[rows(i), :], send_sum.at[i], recv_sum.at[i], pair(i)[1])

    def reads(i):
        return (
            pltpu.make_async_copy(first_ref.at[1, rows(i), :], came, local.at[3]),
            pltpu.make_async_copy(part_ref.at[pair(i)[1], rows(i), :], mine, local.at[4]),
        )

    def store(i):
        into = lax.rem(i, 2)
        return pltpu.make_async_copy(both.at[into], sum_ref.at[rows(i), :], local.at[5 + into])

    load(0, 0).start()
    for q in range(count):
        fetch(q).start()

    def one(i, carry):
        @pl.when((i > DELAY) & (i <= tiles + DELAY))
        def _():
            store(i - DELAY - 1).wait()
            seconds(i - DELAY - 1).start()

        @pl.when((i >= DELAY) & (i < tiles + DELAY))
        def _():
            for copy in firsts(i - DELAY):
                copy.wait_recv()
            for copy in reads(i - DELAY):
                copy.start()

        @pl.when(i < tiles)
        def _():
            into = lax.rem(i, 2)
            load(i, into).wait()

            @pl.when(i + 1 < tiles)
            def _():
                load(i + 1, 1 - into).start()
            rounded = held[into].astype(whole.dtype)
            for q in range(count):
                pl.when(i == 0)(fetch(q).wait)
                product = jnp.dot(rounded, whole[q], preferred_element_type=jnp.float32)
                out[q // cores, :, pl.ds(q % cores * narrow, narrow)] = product.astype(out.dtype)
            keep(i).start()

        @pl.when((i >= DELAY) & (i < tiles + DELAY))
        def _():
            for copy in reads(i - DELAY):
                copy.wait()
            total = came[...].astype(jnp.float32) + mine[...].astype(jnp.float32)
            both[lax.rem(i - DELAY, 2)] = total.astype(both.dtype)
            store(i - DELAY).start()

        @pl.when(i < tiles)
        def _():
            keep(i).wait()
            for copy in firsts(i):
                copy.start()
        return carry
    lax.fori_loop(0, tiles + DELAY + 1, one, 0)

    def settle(i, carry):
        for copy in firsts(i):
            copy.wait_send()
        seconds(i).wait()
        return carry
    lax.fori_loop(0, tiles, settle, 0)


def child_parts(gram, coupling, n_col):
    tall, width = gram.shape
    count, depth, narrow = coupling.shape
    tile = min(128, tall)
    wide = count * narrow // n_col
    tiles = tall // tile
    dma = pltpu.SemaphoreType.DMA
    own, first, second, _ = pl.pallas_call(
        functools.partial(child_kernel, n_col),
        out_shape=(
            jax.ShapeDtypeStruct((n_col, tall, wide), coupling.dtype),
            jax.ShapeDtypeStruct((2, tall, wide), coupling.dtype),
            jax.ShapeDtypeStruct((tall, wide), coupling.dtype),
            jax.ShapeDtypeStruct((tall, wide), coupling.dtype),
        ),
        in_specs=[pl.BlockSpec(memory_space=pl.ANY)] * 2,
        out_specs=[pl.BlockSpec(memory_space=pl.ANY)] * 4,
        scratch_shapes=[
            dma((2, tiles)),
            dma((2, tiles)),
            dma((tiles,)),
            dma((tiles,)),
            dma((7 + count,)),
            pltpu.VMEM((count, depth, narrow), coupling.dtype),
            pltpu.VMEM((2, tile, width), gram.dtype),
            pltpu.VMEM((n_col, tile, wide), coupling.dtype),
            pltpu.VMEM((tile, wide), coupling.dtype),
            pltpu.VMEM((tile, wide), coupling.dtype),
            pltpu.VMEM((2, tile, wide), coupling.dtype),
        ],
        compiler_params=pltpu.CompilerParams(has_side_effects=True, vmem_limit_bytes=63 * 1024 * 1024),
    )(gram, coupling)
    return own, first, second


def finish_kernel(c_ref, g_ref, own_ref, first_ref, second_ref, member_ref, gram_ref, child_ref):
    gram_ref[...] = g_ref[...]
    total = own_ref[0].astype(jnp.float32) + first_ref[0].astype(jnp.float32) + second_ref[...].astype(jnp.float32)
    child_ref[...] = jnp.where(member_ref[...] != 0, -total.T, jnp.float32(0.0))


def finish(gram, own, first, second, member, col_index):
    tall, width = gram.shape
    wide = own.shape[2]
    tile = min(256, tall)
    return pl.pallas_call(
        finish_kernel,
        grid_spec=pltpu.PrefetchScalarGridSpec(
            num_scalar_prefetch=1,
            grid=(tall // tile,),
            in_specs=[
                pl.BlockSpec((tile, width), lambda i, c: (i, 0)),
                pl.BlockSpec((1, tile, wide), lambda i, c: (c[0], i, 0)),
                pl.BlockSpec((1, tile, wide), lambda i, c: (0, i, 0)),
                pl.BlockSpec((tile, wide), lambda i, c: (i, 0)),
                pl.BlockSpec((1, tile), lambda i, c: (0, i)),
            ],
            out_specs=(
                pl.BlockSpec((tile, width), lambda i, c: (i, 0)),
                pl.BlockSpec((wide, tile), lambda i, c: (0, i)),
            ),
        ),
        out_shape=(
            jax.ShapeDtypeStruct((tall, width), jnp.float32),
            jax.ShapeDtypeStruct((wide, tall), jnp.float32),
        ),
        compiler_params=pltpu.CompilerParams(vmem_limit_bytes=63 * 1024 * 1024),
        cost_estimate=pl.CostEstimate(flops=0, bytes_accessed=tall * width * 12, transcendentals=0),
    )(jnp.reshape(col_index, (1,)), gram, own, first, second, member)


def exchange_kernel(n_col, part_ref, out_ref, send, recv):
    r, c = lax.axis_index("row"), lax.axis_index("col")
    depth = out_ref.shape[1]
    started = []
    for d in range(1, n_col):
        ct = lax.rem(c + d, n_col)
        copy = pltpu.make_async_remote_copy(
            src_ref=part_ref.at[pl.ds(pl.multiple_of(ct * depth, depth), depth), :],
            dst_ref=out_ref.at[d - 1],
            send_sem=send.at[d - 1],
            recv_sem=recv.at[d - 1],
            device_id=(r, ct),
            device_id_type=MESH,
        )
        copy.start()
        started.append(copy)
    for copy in started:
        copy.wait()


def exchange(part, n_col):
    total, width = part.shape
    dma = pltpu.SemaphoreType.DMA
    return pl.pallas_call(
        functools.partial(exchange_kernel, n_col),
        out_shape=jax.ShapeDtypeStruct((n_col - 1, total // n_col, width), part.dtype),
        in_specs=[pl.BlockSpec(memory_space=pl.ANY)],
        out_specs=pl.BlockSpec(memory_space=pl.ANY),
        scratch_shapes=[dma((n_col - 1,)), dma((n_col - 1,))],
        compiler_params=pltpu.CompilerParams(has_side_effects=True),
    )(part)


def general(n_row, n_col, factor, coupling):
    rows_here = factor.shape[0]
    row_index, col_index = lax.axis_index("row"), lax.axis_index("col")
    cores = n_row // n_col
    below, partner = gather(factor, n_row, n_col)
    coupling_full = lax.all_gather(coupling, "row", axis=1, tiled=True)

    def product(level, below, partner):
        first = level * rows_here * cores
        return lax.dot_general(
            partner[first:], below[first:], (((0,), (0,)), ((), ())), preferred_element_type=jnp.float32
        )

    gram = lax.switch(
        jnp.maximum(row_index // cores, col_index),
        [functools.partial(product, level) for level in range(n_col)],
        below,
        partner,
    )
    rounded = gram.astype(jnp.bfloat16)
    part = lax.dot_general(
        coupling_full, rounded, (((0,), (1,)), ((), ())), preferred_element_type=jnp.float32
    ).astype(jnp.bfloat16)
    return gram, part


def body(n_row, n_col, factor, sel_tiles, coupling):
    rows_here = factor.shape[0]
    row_index, col_index = lax.axis_index("row"), lax.axis_index("col")
    cores = n_row // n_col
    global_rows = row_index * rows_here + jnp.arange(rows_here, dtype=jnp.int32)
    member = jnp.any((global_rows // TILE)[:, None] == sel_tiles[None, :], axis=1)
    if (n_row, n_col) == (8, 4):
        _, pieces, gram = stream(factor, coupling, n_row, n_col)
        own, first, second = child_parts(gram, pieces, n_col)
        return finish(gram, own, first, second, member.astype(jnp.int32)[None, :], col_index)
    gram, part = general(n_row, n_col, factor, coupling)
    depth = part.shape[0] // n_col
    arrived = exchange(part, n_col)
    summed = lax.dynamic_slice_in_dim(part, col_index * depth, depth, 0).astype(jnp.float32)
    for d in range(n_col - 1):
        summed = summed + arrived[d].astype(jnp.float32)
    child = jnp.where(member[None, :], -summed, jnp.float32(0.0))
    return (gram, child)


def solution(mesh):
    placed = (P("row", "col"), P(), P("col", "row"))
    return jax.shard_map(
        functools.partial(body, mesh.shape["row"], mesh.shape["col"]),
        mesh=mesh,
        in_specs=placed,
        out_specs=(P("row", "col"), P("col", "row")),
        check_vma=False,
    )
```
